256 devices in a mesh: gx: 8 (over z_lo, core), gy: 4 (over x), gz: 8 (over y, z_hi).
Axes of the slice: x: 4, y: 4, z: 8 (z_hi: 2, z_lo: 4; z = z_hi * 4 + z_lo), core: 2. Of those that a mesh axis runs over, the one named last changes fastest.
Arguments:
- displacement: float32 [3, 48, 24, 3072], P(None, 'gx', 'gy', 'gz'), may hold values from -0.18 to 0.18
- size_field_modes: float32 [27, 16, 8, 1024], P(None, 'gx', 'gy', 'gz'), may hold values from -6 to 6
- velocity: float32 [3, 16, 8, 1024], P(None, 'gx', 'gy', 'gz'), may hold values from -1 to 1
Outputs:
- advected_field: float32 [27, 16, 8, 1024], P(None, 'gx', 'gy', 'gz')
- gradient: float32 [3, 48, 24, 3072], P(None, 'gx', 'gy', 'gz')
- checks: float32 [3], replicated
The draws below stay inside these ranges and needn't reach their ends.
All inputs are finite; a program needn't handle non-finite values. Where the reference program divides by a largest or mean magnitude, that divisor is 1e-20 or more.
Results may differ from the reference program's by a relative error of at most 0.0001.
Values sent between devices are 32-bit elements; how exact they have to be, the bound alone decides.
No kernel may reach another device: no remote copies, remote signals or barrier semaphores. Data moves between devices by JAX's collectives and lax.ppermute only.
A program may use at most 64 MiB of HBM per device.

```python
import math
import jax
import jax.numpy as jnp
import numpy as np
from jax import lax

LOCAL_ELEMS_X = 2
LOCAL_ELEMS_Y = 2
LOCAL_ELEMS_Z = 128
SUBSTEPS = 4
GLOBAL_ELEMS_X = 16
GLOBAL_ELEMS_Y = 8
GLOBAL_ELEMS_Z = 1024
ELEMENTS = 131072


def draw_size_field_modes(key, part):
    random_key_noise, random_key_blocks = jax.random.split(key)
    noise_component = jnp.clip(0.5 * jax.random.normal(random_key_noise, (27, GLOBAL_ELEMS_X, GLOBAL_ELEMS_Y, GLOBAL_ELEMS_Z), jnp.float32), -3.0, 3.0)
    block_list = jax.random.uniform(random_key_blocks, (GLOBAL_ELEMS_X // LOCAL_ELEMS_X, GLOBAL_ELEMS_Y // LOCAL_ELEMS_Y, GLOBAL_ELEMS_Z // LOCAL_ELEMS_Z), jnp.float32, -3.0, 3.0)
    offset = jnp.repeat(jnp.repeat(jnp.repeat(block_list, LOCAL_ELEMS_X, axis=0), LOCAL_ELEMS_Y, axis=1), LOCAL_ELEMS_Z, axis=2)
    return noise_component.at[0].add(offset)


def draw_velocity(key, part):
    random_key_heading, random_key_scale = jax.random.split(key)
    heading_text = jax.random.uniform(random_key_heading, (3, GLOBAL_ELEMS_X, GLOBAL_ELEMS_Y, GLOBAL_ELEMS_Z), jnp.float32, -1.0, 1.0)
    scale_factors = jnp.exp(jax.random.uniform(random_key_scale, (GLOBAL_ELEMS_X // LOCAL_ELEMS_X, GLOBAL_ELEMS_Y // LOCAL_ELEMS_Y, GLOBAL_ELEMS_Z // LOCAL_ELEMS_Z), jnp.float32, math.log(0.15), 0.0))
    expanded = jnp.repeat(jnp.repeat(jnp.repeat(scale_factors, LOCAL_ELEMS_X, axis=0), LOCAL_ELEMS_Y, axis=1), LOCAL_ELEMS_Z, axis=2)
    return heading_text * expanded[None]


def block_levels(rng, shape, shards, low, largest):
    gain = 1.0
    for axis_at, blocks in shards:
        draws = jax.random.uniform(jax.random.fold_in(jax.random.fold_in(rng, 6), axis_at), (blocks,), jnp.float32, low / len(shards), largest / len(shards))
        gain = gain * jnp.repeat(jnp.exp(draws), shape[axis_at] // blocks).reshape((-1,) + (1,) * (len(shape) - 1 - axis_at))
    return gain


def normal_values(own_key, shape, scale, most, cuts=(), kind=jnp.bfloat16):
    drawn = jax.random.normal(own_key, shape, jnp.float32) * scale
    if len(cuts) > 0:
        drawn = block_levels(own_key, shape, cuts, -0.22, 0.18) * drawn
    return jnp.clip(drawn, min=-most, max=most).astype(kind)


def setup_inputs(seed: int = 0) -> dict:
    key_list = jax.random.split(jax.random.key(seed), 4)
    displacement = normal_values(key_list[0], (3, 3 * GLOBAL_ELEMS_X, 3 * GLOBAL_ELEMS_Y, 3 * GLOBAL_ELEMS_Z), 0.03, 0.18, ((1, 8), (2, 4), (3, 8)), jnp.float32)
    size_field_modes = draw_size_field_modes(jax.random.fold_in(key_list[3], 71), 0)
    velocity = draw_velocity(jax.random.fold_in(key_list[3], 71), 0)
    return {"displacement": displacement, "size_field_modes": size_field_modes, "velocity": velocity}


root_half = 0.7071067811865476
root_three_half = 1.224744871391589
root_five_half = 1.5811388300841898
plus_values = (0.7071067811865476, 1.224744871391589, 1.5811388300841898)
minus_values = (0.7071067811865476, -1.224744871391589, 1.5811388300841898)
stiffness = ((0.0, 0.0, 0.0), (1.7320508075688772, 0.0, 0.0), (0.0, 3.872983346207417, 0.0))
courant = 0.1
theta_size = 0.3
trial_step = 0.05

def build_tables():
    points = np.array([-0.8611363115940526, -0.3399810435848563, 0.3399810435848563, 0.8611363115940526])
    weights = np.array([0.3478548451374538, 0.6521451548625461, 0.6521451548625461, 0.3478548451374538])
    points = 0.5 * (points + 1.0)
    weights = 0.5 * weights
    node_points = np.array([0.0, 1.0 / 3.0, 2.0 / 3.0, 1.0])
    value_table = np.zeros((4, 4))
    slope_table = np.zeros((4, 4))
    for column in range(4):
        others = [node_points[member] for member in range(4) if member != column]
        denominator = np.prod([node_points[column] - member for member in others])
        for quad_row in range(4):
            gauss_point = points[quad_row]
            value_table[quad_row, column] = np.prod([gauss_point - member for member in others]) / denominator
            slope_table[quad_row, column] = sum((np.prod([gauss_point - others[position] for position in range(3) if position != skipped]) for skipped in range(3))) / denominator
    centred = 2.0 * points - 1.0
    legendre_table = np.stack([np.full(4, root_half), root_three_half * centred, root_five_half * 0.5 * (3.0 * centred ** 2 - 1.0)], axis=1)
    cube_table = (weights[:, None, None] * weights[None, :, None] * weights[None, None, :]).reshape(4, 4, 4, 1, 1, 1)
    return (value_table, slope_table, legendre_table, cube_table)

def as_table(operand):
    return jnp.asarray(np.asarray(operand), jnp.float32)

def contract(weights_table, operand, along):
    product = jnp.tensordot(as_table(weights_table), operand, axes=([1], [along]), precision=lax.Precision.HIGHEST)
    return jnp.moveaxis(product, 0, along)

def trace_along(modal_coefficients, vector, direction):
    return jnp.tensordot(as_table(vector), modal_coefficients, axes=([0], [direction]), precision=lax.Precision.HIGHEST)

def spread_shape(vector, direction):
    broadcast_shape = [1] * 6
    broadcast_shape[direction] = 3
    return as_table(vector).reshape(broadcast_shape)

def boundary_terms(modal_coefficients, local_speed, right_ext, left_ext, speed_ext, direction):
    extent = modal_coefficients.shape[3 + direction]
    face_speed = 0.5 * (lax.slice_in_dim(speed_ext, 0, extent + 1, axis=direction) + lax.slice_in_dim(speed_ext, 1, extent + 2, axis=direction))
    flux = jnp.maximum(face_speed, 0.0)[None, None] * right_ext + jnp.minimum(face_speed, 0.0)[None, None] * left_ext
    flux_left = lax.slice_in_dim(flux, 0, extent, axis=2 + direction)
    flux_right = lax.slice_in_dim(flux, 1, extent + 1, axis=2 + direction)
    lifted = contract(stiffness, modal_coefficients, direction)
    faces = spread_shape(plus_values, direction) * jnp.expand_dims(flux_right, direction) - spread_shape(minus_values, direction) * jnp.expand_dims(flux_left, direction)
    return local_speed[None, None, None] * lifted - faces

def element_energy(corners, modal_coefficients):
    lagrange_values, lagrange_slopes, legendre_values, cube_weights = build_tables()
    along_value = contract(lagrange_values, corners, 1)
    along_slope = contract(lagrange_slopes, corners, 1)
    value_value = contract(lagrange_values, along_value, 2)
    jac_first = contract(lagrange_values, contract(lagrange_values, along_slope, 2), 3)
    jac_second = contract(lagrange_values, contract(lagrange_slopes, along_value, 2), 3)
    jac_third = contract(lagrange_slopes, value_value, 3)
    columns = (jac_first, jac_second, jac_third)
    sample = contract(legendre_values, contract(legendre_values, contract(legendre_values, modal_coefficients, 0), 1), 2)
    target_size = jnp.exp(theta_size * sample)
    inverse = 1.0 / target_size
    mapped = [[((1.0 if component == column else 0.0) + columns[column][component]) * inverse for column in range(3)] for component in range(3)]
    metric = jnp.zeros_like(sample)
    for first_column in range(3):
        for second_column in range(3):
            gram_entry = mapped[0][first_column] * mapped[0][second_column] + mapped[1][first_column] * mapped[1][second_column] + mapped[2][first_column] * mapped[2][second_column]
            deviation = gram_entry - (1.0 if first_column == second_column else 0.0)
            metric = metric + deviation * deviation
    return jnp.sum(as_table(cube_weights) * target_size ** 3 * metric)

def element_corners(padded):
    gathered = padded
    for along, stack_axis in ((1, 1), (3, 2), (5, 3)):
        extent = (gathered.shape[along] - 1) // 3
        gathered = jnp.stack([lax.slice_in_dim(gathered, node_offset, node_offset + 3 * extent - 2, stride=3, axis=along) for node_offset in range(4)], axis=stack_axis)
    return gathered

def pad_one(operand, node_offset, along):
    config = [(0, 0, 0)] * operand.ndim
    config[along] = (node_offset, 3 - node_offset, 2)
    return lax.pad(operand, jnp.zeros((), operand.dtype), config)

def spread_corners(corner_grad):
    spread = corner_grad
    for stack_axis, along in ((3, 5), (2, 3), (1, 1)):
        pieces = [pad_one(lax.index_in_dim(spread, node_offset, axis=stack_axis, keepdims=False), node_offset, along) for node_offset in range(4)]
        spread = pieces[0] + pieces[1] + pieces[2] + pieces[3]
    return spread

def advection_rate(modal_coefficients, velocity):
    accumulated = jnp.zeros_like(modal_coefficients)
    for direction in range(3):
        element_axis = 2 + direction
        extent = modal_coefficients.shape[3 + direction]
        local_speed = velocity[direction]
        speed_ext = jnp.concatenate([lax.slice_in_dim(local_speed, extent - 1, extent, axis=direction), local_speed, lax.slice_in_dim(local_speed, 0, 1, axis=direction)], axis=direction)
        right_trace = trace_along(modal_coefficients, plus_values, direction)
        left_trace = trace_along(modal_coefficients, minus_values, direction)
        right_ext = jnp.concatenate([lax.slice_in_dim(right_trace, extent - 1, extent, axis=element_axis), right_trace], axis=element_axis)
        left_ext = jnp.concatenate([left_trace, lax.slice_in_dim(left_trace, 0, 1, axis=element_axis)], axis=element_axis)
        accumulated = accumulated + boundary_terms(modal_coefficients, local_speed, right_ext, left_ext, speed_ext, direction)
    return 2.0 * accumulated

def periodic_pad(nodal):
    for along in (1, 2, 3):
        nodal = jnp.concatenate([nodal, lax.slice_in_dim(nodal, 0, 1, axis=along)], axis=along)
    return nodal

def periodic_fold(gradient_pad):
    for along in (1, 2, 3):
        extent = gradient_pad.shape[along] - 1
        gradient_pad = jnp.concatenate([lax.slice_in_dim(gradient_pad, 0, 1, axis=along) + lax.slice_in_dim(gradient_pad, extent, extent + 1, axis=along), lax.slice_in_dim(gradient_pad, 1, extent, axis=along)], axis=along)
    return gradient_pad

def gradient_scan(padded, modal_coefficients):

    def advance(running, slab_start):
        energy_sum, gradient_pad = running
        nodes_slab = lax.dynamic_slice_in_dim(padded, 3 * slab_start, 4, axis=1)
        field_slab = lax.dynamic_slice_in_dim(modal_coefficients, slab_start, 1, axis=3)
        energy_here, corner_grad = jax.value_and_grad(element_energy)(element_corners(nodes_slab), field_slab)
        contribution = spread_corners(corner_grad)
        current = lax.dynamic_slice_in_dim(gradient_pad, 3 * slab_start, 4, axis=1)
        gradient_pad = lax.dynamic_update_slice_in_dim(gradient_pad, current + contribution, 3 * slab_start, axis=1)
        return ((energy_sum + energy_here, gradient_pad), None)
    start_value = (jnp.zeros((), jnp.float32), jnp.zeros_like(padded))
    finished, unused = lax.scan(advance, start_value, jnp.arange(GLOBAL_ELEMS_X, dtype=jnp.int32))
    return finished

def energy_scan(padded, modal_coefficients):

    def advance(energy_sum, slab_start):
        nodes_slab = lax.dynamic_slice_in_dim(padded, 3 * slab_start, 4, axis=1)
        field_slab = lax.dynamic_slice_in_dim(modal_coefficients, slab_start, 1, axis=3)
        return (energy_sum + element_energy(element_corners(nodes_slab), field_slab), None)
    finished, unused = lax.scan(advance, jnp.zeros((), jnp.float32), jnp.arange(GLOBAL_ELEMS_X, dtype=jnp.int32))
    return finished

def reference(displacement, size_field_modes, velocity):
    modal_coefficients = size_field_modes.reshape(3, 3, 3, GLOBAL_ELEMS_X, GLOBAL_ELEMS_Y, GLOBAL_ELEMS_Z)
    fastest = jnp.max(lax.optimization_barrier(jnp.sum(jnp.abs(velocity), axis=0)))
    time_step = courant / jnp.maximum(fastest, 0.25)
    for substep in range(SUBSTEPS):
        midway = modal_coefficients + time_step * advection_rate(modal_coefficients, velocity)
        modal_coefficients = 0.5 * modal_coefficients + 0.5 * (midway + time_step * advection_rate(midway, velocity))
    energy_total, gradient_pad = gradient_scan(periodic_pad(displacement), modal_coefficients)
    gradient = periodic_fold(gradient_pad)
    elements = 1.0 * ELEMENTS
    entries = 81.0 * ELEMENTS
    square_total = jnp.sum(gradient * gradient)
    step_length = trial_step / jnp.sqrt(1.0 + square_total / entries)
    trial_nodes = displacement - step_length * gradient
    trial_total = energy_scan(periodic_pad(trial_nodes), modal_coefficients)
    checks = jnp.stack([energy_total / elements, square_total / entries, trial_total / elements])
    return (modal_coefficients.reshape(27, GLOBAL_ELEMS_X, GLOBAL_ELEMS_Y, GLOBAL_ELEMS_Z), gradient, checks)
```

```python
import jax
import jax.numpy as jnp
import numpy as np
from jax import lax
from jax.experimental import pallas as pl
from jax.experimental.pallas import tpu as pltpu
from jax.sharding import Mesh
from jax.sharding import PartitionSpec as P

SUBSTEPS = 4
GX = ("gx_0", "gx_1")
GZ = ("gz_0", "gz_1")
XY = ("gx_0", "gx_1", "gy")

NZ = 8
NXY = 32
HALO_ROWS = 16
IN_ROWS = 48
X_ROW = 24
MAX_ROW = 47
OUT_ROWS = 16

p0 = 0.7071067811865476
p1 = 1.224744871391589
p2 = 1.5811388300841898
root3 = 1.7320508075688772
root15 = 3.872983346207417
courant = 0.1
theta_size = 0.3
trial_step = 0.05


def build_tables():
    points = np.array(
        [-0.8611363115940526, -0.3399810435848563, 0.3399810435848563, 0.8611363115940526]
    )
    weights = np.array(
        [0.3478548451374538, 0.6521451548625461, 0.6521451548625461, 0.3478548451374538]
    )
    points = 0.5 * (points + 1.0)
    weights = 0.5 * weights
    node_points = np.array([0.0, 1.0 / 3.0, 2.0 / 3.0, 1.0])
    value_table = np.zeros((4, 4))
    slope_table = np.zeros((4, 4))
    for column in range(4):
        others = [node_points[member] for member in range(4) if member != column]
        denominator = np.prod([node_points[column] - member for member in others])
        for quad_row in range(4):
            gauss_point = points[quad_row]
            value_table[quad_row, column] = (
                np.prod([gauss_point - member for member in others]) / denominator
            )
            slope_table[quad_row, column] = (
                sum(
                    np.prod(
                        [gauss_point - others[position] for position in range(3) if position != skipped]
                    )
                    for skipped in range(3)
                )
                / denominator
            )
    centred = 2.0 * points - 1.0
    legendre_table = np.stack(
        [
            np.full(4, p0),
            p1 * centred,
            p2 * 0.5 * (3.0 * centred**2 - 1.0),
        ],
        axis=1,
    )
    return value_table, slope_table, legendre_table, weights


VALUES, SLOPES, LEGENDRE, WEIGHTS = build_tables()


def iota(shape, dim):
    return lax.broadcasted_iota(jnp.int32, shape, dim)


def lanes(x, by):
    return pltpu.roll(x, (-by) % 128, x.ndim - 1)


def rows(x, by):
    return pltpu.roll(x, (-by) % 8, x.ndim - 2)


class Shifts:
    def __init__(self, *lead):
        r, l = iota((*lead, 8, 128), len(lead)), iota((*lead, 8, 128), len(lead) + 1)
        self.a0 = ((r >> 1) & 1) == 0
        self.b0 = (r & 1) == 0
        self.low = r < 4
        self.j = l & 3
        self.i = (l >> 2) & 7
        self.z = l >> 5

    def swap_x(self, x):
        return jnp.where(self.a0, rows(x, 2), rows(x, -2))

    def swap_y(self, x):
        return jnp.where(self.b0, rows(x, 1), rows(x, -1))

    def next(self, x, d):
        if d == 0:
            s = self.swap_x(x)
            return jnp.where(self.a0, s, jnp.where(self.i < 7, lanes(s, 4), lanes(s, -28)))
        if d == 1:
            s = self.swap_y(x)
            return jnp.where(self.b0, s, jnp.where(self.j < 3, lanes(s, 1), lanes(s, -3)))
        s = lanes(x, 32)
        t = rows(s, 4)
        if x.ndim == 3:
            t = jnp.where(self.low, t, jnp.concatenate([t[1:], t[:1]], axis=0))
        return jnp.where(self.z < 3, s, t)

    def prev(self, x, d):
        if d == 0:
            s = self.swap_x(x)
            return jnp.where(self.a0, jnp.where(self.i > 0, lanes(s, -4), lanes(s, 28)), s)
        if d == 1:
            s = self.swap_y(x)
            return jnp.where(self.b0, jnp.where(self.j > 0, lanes(s, -1), lanes(s, 3)), s)
        s = lanes(x, -32)
        t = rows(s, 4)
        if x.ndim == 3:
            t = jnp.where(self.low, jnp.concatenate([t[-1:], t[:-1]], axis=0), t)
        return jnp.where(self.z > 0, s, t)


def halves(x):
    return (x[0] + x[3], x[1] + x[2], x[0] - x[3], x[1] - x[2])


def apply_table(table, sign, half):
    ea, eb, oa, ob = half
    out = [None] * 4
    for p in range(2):
        even = float(0.5 * (table[p, 0] + table[p, 3])) * ea + float(0.5 * (table[p, 1] + table[p, 2])) * eb
        odd = float(0.5 * (table[p, 0] - table[p, 3])) * oa + float(0.5 * (table[p, 1] - table[p, 2])) * ob
        out[p] = even + odd
        out[3 - p] = even - odd if sign > 0 else odd - even
    return out


def transpose_kernel(g_ref, u_ref, v_ref, x_ref, tuv_ref, tx_ref, halo_ref, uv_s, x_s):
    zero = jnp.zeros((24, 384), jnp.float32)
    uv_s[0:108, :] = u_ref[...]
    uv_s[108:120, :] = v_ref[...]
    uv_s[120:128, :] = zero[0:8, 0:128]
    x_s[0:108, :] = x_ref[...]
    x_s[108:128, :] = zero[0:20]
    tuv_ref[...] = uv_s[...].T
    for n in range(3):
        tx_ref[128 * n : 128 * n + 128, :] = x_s[:, 128 * n : 128 * n + 128].T
    speed = jnp.abs(v_ref[0:4, :]) + jnp.abs(v_ref[4:8, :]) + jnp.abs(v_ref[8:12, :])
    fastest = jnp.broadcast_to(jnp.max(speed, axis=(0, 1), keepdims=True), (1, 128))
    for n in range(NZ):
        halo_ref[n, :, :] = zero[0:16, 0:128]
        halo_ref[n, 13:14, :] = fastest
    up = lax.rem(g_ref[0] + 1, NZ)
    down = lax.rem(g_ref[0] + NZ - 1, NZ)
    halo_ref[up, 0:9, :] = tuv_ref[119:128, :]
    halo_ref[up, 9:12, :] = tx_ref[381:384, :]
    halo_ref[down, 0:9, :] = tuv_ref[0:9, :]
    halo_ref[down, 9:13, :] = tx_ref[0:4, :]


def pack_kernel(g_ref, tuv_ref, tx_ref, halo_ref, out_ref, uv_s, x_s):
    below = lax.rem(g_ref[0] + NZ - 1, NZ)
    above = lax.rem(g_ref[0] + 1, NZ)
    uv_s[0:16, :] = jnp.zeros((16, 128), jnp.float32)
    uv_s[144:160, :] = jnp.zeros((16, 128), jnp.float32)
    x_s[0:8, :] = jnp.zeros((8, 128), jnp.float32)
    x_s[392:408, :] = jnp.zeros((16, 128), jnp.float32)
    uv_s[16:144, :] = tuv_ref[...]
    x_s[8:392, :] = tx_ref[...]
    uv_s[7:16, :] = halo_ref[below, 0:9, :]
    uv_s[144:153, :] = halo_ref[above, 0:9, :]
    x_s[5:8, :] = halo_ref[below, 9:12, :]
    x_s[392:396, :] = halo_ref[above, 9:13, :]
    fastest = halo_ref[0, 13:14, :]
    for n in range(1, NZ):
        fastest = jnp.maximum(fastest, halo_ref[n, 13:14, :])
    for k in range(NXY):
        at = IN_ROWS * k
        out_ref[at : at + 24, :] = uv_s[4 * k + 7 : 4 * k + 31, :]
        out_ref[at + 24 : at + 48, :] = x_s[12 * k + 5 : 12 * k + 29, :]
        out_ref[at + MAX_ROW : at + MAX_ROW + 1, :] = fastest


def corner_fill(ref, sh):
    def one(c, carry):
        at = c * 64
        for kx in range(3):
            for ky in range(3):
                ref[at + kx * 16 + ky * 4 + 3] = sh.next(ref[at + kx * 16 + ky * 4], 2)
        for kx in range(3):
            for kz in range(4):
                ref[at + kx * 16 + 12 + kz] = sh.next(ref[at + kx * 16 + kz], 1)
        for ky in range(4):
            for kz in range(4):
                ref[at + 48 + ky * 4 + kz] = sh.next(ref[at + ky * 4 + kz], 0)
        return carry

    lax.fori_loop(0, 3, one, 0)


def corner_fold(ref, sh):
    def one(c, carry):
        at = c * 64
        for ky in range(4):
            for kz in range(4):
                n = at + ky * 4 + kz
                ref[n] = ref[n] + sh.prev(ref[n + 48], 0)
        for kx in range(3):
            for kz in range(4):
                n = at + kx * 16 + kz
                ref[n] = ref[n] + sh.prev(ref[n + 12], 1)
        for kx in range(3):
            for ky in range(3):
                n = at + kx * 16 + ky * 4
                ref[n] = ref[n] + sh.prev(ref[n + 3], 2)
        return carry

    lax.fori_loop(0, 3, one, 0)


def slopes_at_points(src, dst, a_s, b_s):
    def one(c, carry):
        at = c * 64
        for line in range(16):
            h = halves([src[at + k * 16 + line] for k in range(4)])
            v = apply_table(VALUES, 1, h)
            s = apply_table(SLOPES, -1, h)
            for p in range(4):
                a_s[p * 16 + line] = v[p]
                a_s[64 + p * 16 + line] = s[p]
        for p in range(4):
            for kz in range(4):
                hv = halves([a_s[p * 16 + k * 4 + kz] for k in range(4)])
                hs = halves([a_s[64 + p * 16 + k * 4 + kz] for k in range(4)])
                sv = apply_table(VALUES, 1, hs)
                vs = apply_table(SLOPES, -1, hv)
                vv = apply_table(VALUES, 1, hv)
                for r in range(4):
                    b_s[p * 16 + r * 4 + kz] = sv[r]
                    b_s[64 + p * 16 + r * 4 + kz] = vs[r]
                    b_s[128 + p * 16 + r * 4 + kz] = vv[r]
        for pr in range(16):
            for col in range(3):
                h = halves([b_s[64 * col + pr * 4 + k] for k in range(4)])
                out = apply_table(SLOPES, -1, h) if col == 2 else apply_table(VALUES, 1, h)
                for t in range(4):
                    dst[c * 192 + 64 * col + pr * 4 + t] = out[t]
        return carry

    lax.fori_loop(0, 3, one, 0)


def points_to_corners(src, dst, a_s, b_s):
    values_t, slopes_t = VALUES.T, SLOPES.T

    def one(c, carry):
        at = c * 64
        for pr in range(16):
            for col in range(3):
                h = halves([src[c * 192 + 64 * col + pr * 4 + t] for t in range(4)])
                out = apply_table(slopes_t, -1, h) if col == 2 else apply_table(values_t, 1, h)
                for k in range(4):
                    b_s[64 * col + pr * 4 + k] = out[k]
        for p in range(4):
            for kz in range(4):
                sv = apply_table(values_t, 1, halves([b_s[p * 16 + r * 4 + kz] for r in range(4)]))
                vs = apply_table(slopes_t, -1, halves([b_s[64 + p * 16 + r * 4 + kz] for r in range(4)]))
                vv = apply_table(values_t, 1, halves([b_s[128 + p * 16 + r * 4 + kz] for r in range(4)]))
                for k in range(4):
                    a_s[p * 16 + k * 4 + kz] = vv[k] + vs[k]
                    a_s[64 + p * 16 + k * 4 + kz] = sv[k]
        for line in range(16):
            v = apply_table(values_t, 1, halves([a_s[p * 16 + line] for p in range(4)]))
            s = apply_table(slopes_t, -1, halves([a_s[64 + p * 16 + line] for p in range(4)]))
            for k in range(4):
                dst[at + k * 16 + line] = v[k] + s[k]
        return carry

    lax.fori_loop(0, 3, one, 0)


def legendre_line(u):
    base = p0 * u[0]
    out = [None] * 4
    for p in range(2):
        even = base + float(LEGENDRE[p, 2]) * u[2]
        odd = float(LEGENDRE[p, 1]) * u[1]
        out[p] = even + odd
        out[3 - p] = even - odd
    return out


def sample_sizes(u_s, size_s, a_s):
    for bc in range(9):
        out = legendre_line([u_s[a * 9 + bc, 1] for a in range(3)])
        for p in range(4):
            a_s[p * 9 + bc] = out[p]
    for p in range(4):
        grid = [[None] * 3 for _ in range(4)]
        for c in range(3):
            out = legendre_line([a_s[p * 9 + b * 3 + c] for b in range(3)])
            for r in range(4):
                grid[r][c] = out[r]
        for r in range(4):
            out = legendre_line(grid[r])
            for t in range(4):
                size_s[p * 16 + r * 4 + t] = jnp.exp(theta_size * out[t])


PAIRS = ((0, 0), (1, 1), (2, 2), (0, 1), (0, 2), (1, 2))
AT = {pair: n for n, pair in enumerate(PAIRS)} | {(b, a): n for n, (a, b) in enumerate(PAIRS)}


def dot6(x, y):
    return x[0] * y[0] + x[1] * y[1] + x[2] * y[2] + 2.0 * (x[3] * y[3] + x[4] * y[4] + x[5] * y[5])


def weight_of(pr):
    def w(k):
        return jnp.where((k == 0) | (k == 3), jnp.float32(WEIGHTS[0]), jnp.float32(WEIGHTS[1]))

    return w(pr >> 2) * w(pr & 3)


def jacobian(j_s, q):
    jac = [[j_s[c * 192 + col * 64 + q] for col in range(3)] for c in range(3)]
    for c in range(3):
        jac[c][c] = jac[c][c] + 1.0
    return jac


def stress(j_s, size_s, g_s, p_s):
    def one(pr, energy):
        pair_weight = weight_of(pr)
        for t in range(4):
            q = pr * 4 + t
            jac = jacobian(j_s, q)
            size = size_s[q]
            inverse = 1.0 / size
            inverse2 = inverse * inverse
            weighted = (pair_weight * float(WEIGHTS[t])) * size
            dev = []
            for n, (a, b) in enumerate(PAIRS):
                gram = (jac[0][a] * jac[0][b] + jac[1][a] * jac[1][b] + jac[2][a] * jac[2][b]) * inverse2
                dev.append(gram - 1.0 if a == b else gram)
                g_s[n * 64 + q] = dev[n]
            energy = energy + weighted * size * size * dot6(dev, dev)
            scaled = [4.0 * weighted * d for d in dev]
            for c in range(3):
                for col in range(3):
                    p_s[c * 192 + col * 64 + q] = (
                        jac[c][0] * scaled[AT[0, col]]
                        + jac[c][1] * scaled[AT[1, col]]
                        + jac[c][2] * scaled[AT[2, col]]
                    )
        return energy

    return lax.fori_loop(0, 16, one, jnp.zeros((8, 128), jnp.float32))


def trial_terms(j_s, size_s, g_s, d_s):
    def one(pr, sums):
        e2, e3, e4 = sums
        pair_weight = weight_of(pr)
        for t in range(4):
            q = pr * 4 + t
            jac = jacobian(j_s, q)
            der = [[d_s[c * 192 + col * 64 + q] for col in range(3)] for c in range(3)]
            size = size_s[q]
            inverse = 1.0 / size
            inverse2 = inverse * inverse
            weighted = (pair_weight * float(WEIGHTS[t])) * size * size * size
            dev, first, second = [], [], []
            for n, (a, b) in enumerate(PAIRS):
                dev.append(g_s[n * 64 + q])
                if a == b:
                    f = 2.0 * (jac[0][a] * der[0][a] + jac[1][a] * der[1][a] + jac[2][a] * der[2][a])
                else:
                    f = (
                        jac[0][a] * der[0][b] + jac[1][a] * der[1][b] + jac[2][a] * der[2][b]
                        + jac[0][b] * der[0][a] + jac[1][b] * der[1][a] + jac[2][b] * der[2][a]
                    )
                first.append(f * inverse2)
                second.append((der[0][a] * der[0][b] + der[1][a] * der[1][b] + der[2][a] * der[2][b]) * inverse2)
            e2 = e2 + weighted * (dot6(first, first) + 2.0 * dot6(dev, second))
            e3 = e3 - 2.0 * weighted * dot6(first, second)
            e4 = e4 + weighted * dot6(second, second)
        return e2, e3, e4

    zero = jnp.zeros((8, 128), jnp.float32)
    return lax.fori_loop(0, 16, one, (zero, zero, zero))


def remap(u_s, v_s, mid_s, face_s, time_step, sh):
    for d in range(3):
        v = v_s[d]
        face = 0.5 * (v + sh.next(v, d))
        face_s[4 * d] = 2.0 * time_step * jnp.maximum(face, 0.0)
        face_s[4 * d + 1] = 2.0 * time_step * jnp.minimum(face, 0.0)
        face_s[4 * d + 2] = (2.0 * root3) * time_step * v
        face_s[4 * d + 3] = (2.0 * root15) * time_step * v

    def terms(src, d, m, step):
        u0, u1, u2 = src[m], src[m + step], src[m + 2 * step]
        even = p0 * u0 + p2 * u2
        odd = p1 * u1
        flux = face_s[4 * d] * (even + odd) + face_s[4 * d + 1] * sh.next(even - odd, d)
        before = sh.prev(flux, d)
        jump = before - flux
        return (
            p0 * jump,
            face_s[4 * d + 2] * u0 - p1 * (flux + before),
            face_s[4 * d + 3] * u1 + p2 * jump,
        )

    def substep(_, carry):
        for d, step, starts in (
            (0, 9, range(9)),
            (1, 3, (0, 1, 2, 9, 10, 11, 18, 19, 20)),
            (2, 1, range(0, 27, 3)),
        ):
            for m in starts:
                for n, term in enumerate(terms(u_s, d, m, step)):
                    at = m + n * step
                    mid_s[at] = (u_s[at] if d == 0 else mid_s[at]) + term
        for d, step, starts in (
            (0, 9, range(9)),
            (1, 3, (0, 1, 2, 9, 10, 11, 18, 19, 20)),
            (2, 1, range(0, 27, 3)),
        ):
            for m in starts:
                for n, term in enumerate(terms(mid_s, d, m, step)):
                    at = m + n * step
                    old = 0.5 * (u_s[at] + mid_s[at]) if d == 0 else u_s[at]
                    u_s[at] = old + 0.5 * term
        return carry

    lax.fori_loop(0, SUBSTEPS, substep, 0)


def main_kernel(
    in_ref, out_ref, t_s, u_s, v_s, mid_s, face_s, x_s, a_s, b_s, j_s, p_s, g_s, size_s
):
    sh = Shifts()
    for zz in range(6):
        stacked = jnp.concatenate(
            [in_ref[pl.ds(4 * zz + z, NXY, stride=IN_ROWS), :] for z in range(4)], axis=0
        )
        t_s[...] = stacked.T
        half = 4 * (zz % 2)
        for m in range(27):
            u_s[m, zz // 2, half : half + 4, :] = t_s[4 * m : 4 * m + 4, :]
        for d in range(3):
            v_s[d, zz // 2, half : half + 4, :] = t_s[108 + 4 * d : 112 + 4 * d, :]
    for kz in range(3):
        for part in range(2):
            stacked = jnp.concatenate(
                [
                    in_ref[pl.ds(X_ROW + 3 * (4 * part + z) + kz, NXY, stride=IN_ROWS), :]
                    for z in range(4)
                ],
                axis=0,
            )
            t_s[...] = stacked.T
            half = 4 * part
            for n in range(27):
                c, kx, ky = n // 9, (n // 3) % 3, n % 3
                x_s[c * 64 + kx * 16 + ky * 4 + kz, half : half + 4, :] = t_s[4 * n : 4 * n + 4, :]
    fastest = jnp.max(in_ref[pl.ds(MAX_ROW, NXY, stride=IN_ROWS), :], axis=0, keepdims=True)
    time_step = jnp.broadcast_to(courant / jnp.maximum(fastest, 0.25), (8, 128))
    remap(u_s, v_s, mid_s, face_s, time_step, Shifts(3))

    corner_fill(x_s, sh)
    slopes_at_points(x_s, j_s, a_s, b_s)
    sample_sizes(u_s, size_s, a_s)
    energy = stress(j_s, size_s, g_s, p_s)
    points_to_corners(p_s, x_s, a_s, b_s)
    corner_fold(x_s, sh)
    own = jnp.where(sh.low, sh.z, 1 - sh.z) > 0
    square = jnp.zeros((8, 128), jnp.float32)
    for n in range(27):
        for kz in range(3):
            grad = x_s[(n // 9) * 64 + ((n // 3) % 3) * 16 + (n % 3) * 4 + kz]
            square = square + grad * grad
    corner_fill(x_s, sh)
    slopes_at_points(x_s, p_s, a_s, b_s)
    sums = (energy, square) + trial_terms(j_s, size_s, g_s, p_s)
    t_s[108:128, :] = jnp.zeros((20, 128), jnp.float32)
    for n, part in enumerate(sums):
        total = jnp.sum(jnp.where(own, part, 0.0), axis=(0, 1), keepdims=True)
        t_s[108 + n : 109 + n, :] = jnp.broadcast_to(total, (1, 128))
    for part in range(2):
        half = 4 * part
        layers = ((1, 0), (2, 1), (3, 2)) if part == 0 else ((0, 3),)
        for m in range(27):
            t_s[4 * m : 4 * m + 4, :] = u_s[m, 1, half : half + 4, :]
        back = t_s[...].T
        for z, layer in layers:
            out_ref[pl.ds(layer, NXY, stride=OUT_ROWS), :] = back[32 * z : 32 * z + 32, :]
        for kz in range(3):
            for n in range(27):
                c, kx, ky = n // 9, (n // 3) % 3, n % 3
                t_s[4 * n : 4 * n + 4, :] = x_s[c * 64 + kx * 16 + ky * 4 + kz, half : half + 4, :]
            back = t_s[...].T
            for z, layer in layers:
                out_ref[pl.ds(4 + 3 * layer + kz, NXY, stride=OUT_ROWS), :] = back[32 * z : 32 * z + 32, :]


def unpack_kernel(in_ref, u_ref, g_ref, sums_ref, u_s, g_s):
    for layer in range(4):
        u_s[pl.ds(layer, NXY, stride=4), :] = in_ref[pl.ds(layer, NXY, stride=OUT_ROWS), :]
    for r in range(12):
        g_s[pl.ds(r, NXY, stride=12), :] = in_ref[pl.ds(4 + r, NXY, stride=OUT_ROWS), :]
    sums_ref[...] = jnp.sum(in_ref[pl.ds(0, NXY, stride=OUT_ROWS), :], axis=0, keepdims=True)
    u_ref[...] = u_s[...].T[0:108, :]
    for n in range(3):
        g_ref[:, 128 * n : 128 * n + 128] = g_s[128 * n : 128 * n + 128, :].T[0:108, :]


def shape(*dims):
    return jax.ShapeDtypeStruct(dims, jnp.float32)


def vmem(*dims):
    return pltpu.VMEM(dims, jnp.float32)


SMEM = pl.BlockSpec(memory_space=pltpu.SMEM)
VMEM = pl.BlockSpec(memory_space=pltpu.VMEM)


def on_device(displacement, size_field_modes, velocity):
    at_z = lax.axis_index(GZ).reshape(1).astype(jnp.int32)
    u = size_field_modes.reshape(108, 128)
    v = velocity.reshape(12, 128)
    x = displacement.reshape(3, 2, 3, 2, 3, 384).transpose(0, 2, 4, 1, 3, 5).reshape(108, 384)
    tuv, tx, halo = pl.pallas_call(
        transpose_kernel,
        out_shape=(shape(128, 128), shape(384, 128), shape(NZ, HALO_ROWS, 128)),
        in_specs=[SMEM, VMEM, VMEM, VMEM],
        out_specs=(VMEM, VMEM, VMEM),
        scratch_shapes=[vmem(128, 128), vmem(128, 384)],
        name="transpose",
    )(at_z, u, v, x)
    halo = lax.all_to_all(halo, GZ, 0, 0)
    packed = pl.pallas_call(
        pack_kernel,
        out_shape=shape(NXY * IN_ROWS, 128),
        in_specs=[SMEM, VMEM, VMEM, VMEM],
        out_specs=VMEM,
        scratch_shapes=[vmem(160, 128), vmem(408, 128)],
        name="pack",
    )(at_z, tuv, tx, halo)
    spread = lax.all_to_all(packed.reshape(NXY, IN_ROWS, 128), XY, 0, 0)
    result = pl.pallas_call(
        main_kernel,
        out_shape=shape(NXY * OUT_ROWS, 128),
        in_specs=[VMEM],
        out_specs=VMEM,
        scratch_shapes=[
            vmem(128, 128),
            vmem(27, 3, 8, 128),
            vmem(3, 3, 8, 128),
            vmem(27, 3, 8, 128),
            vmem(12, 3, 8, 128),
            vmem(192, 8, 128),
            vmem(128, 8, 128),
            vmem(192, 8, 128),
            vmem(576, 8, 128),
            vmem(576, 8, 128),
            vmem(384, 8, 128),
            vmem(64, 8, 128),
        ],
        name="remap_and_gradient",
    )(spread.reshape(NXY * IN_ROWS, 128))
    result = lax.all_to_all(result.reshape(NXY, OUT_ROWS, 128), XY, 0, 0)
    advected, gradient, sums = pl.pallas_call(
        unpack_kernel,
        out_shape=(shape(108, 128), shape(108, 384), shape(1, 128)),
        in_specs=[VMEM],
        out_specs=(VMEM, VMEM, VMEM),
        scratch_shapes=[vmem(128, 128), vmem(384, 128)],
        name="unpack",
    )(result.reshape(NXY * OUT_ROWS, 128))
    sums = lax.all_to_all(jnp.broadcast_to(sums[None], (NZ, 1, 128)), GZ, 0, 0)
    sums = jnp.sum(sums, axis=0)[0]
    e0, square, e2, e3, e4 = (sums[108 + n] for n in range(5))
    elements = float(512 * NXY * NZ)
    entries = 81.0 * elements
    step = trial_step / jnp.sqrt(1.0 + square / entries)
    trial = e0 + step * (-square + step * (e2 + step * (e3 + step * e4)))
    checks = jnp.stack([e0 / elements, square / entries, trial / elements])
    gradient = gradient.reshape(3, 3, 3, 2, 2, 384).transpose(0, 3, 1, 4, 2, 5).reshape(3, 6, 6, 384)
    return advected.reshape(27, 2, 2, 128), gradient, checks


def solution(mesh):
    finer = Mesh(
        mesh.devices.reshape(4, 2, mesh.shape["gy"], 4, 2), ("gx_0", "gx_1", "gy", "gz_0", "gz_1")
    )
    return jax.shard_map(
        on_device,
        mesh=finer,
        in_specs=(P(None, GX, "gy", GZ), P(None, GX, "gy", GZ), P(None, GX, "gy", GZ)),
        out_specs=(P(None, GX, "gy", GZ), P(None, GX, "gy", GZ), P()),
        check_vma=False,
    )
```

```python
import jax
import jax.numpy as jnp
import numpy as np
from jax import lax
from jax.experimental import pallas as pl
from jax.experimental.pallas import tpu as pltpu
from jax.sharding import Mesh
from jax.sharding import PartitionSpec as P

SUBSTEPS = 4
GX = ("gx_0", "gx_1")
GZ = ("gz_0", "gz_1")
XY = ("gx_0", "gx_1", "gy")

NZ = 8
NXY = 32
HALO_ROWS = 16
IN_ROWS = 48
SUM_LANE = 120
OUT_ROWS = 16

p0 = 0.7071067811865476
p1 = 1.224744871391589
p2 = 1.5811388300841898
root3 = 1.7320508075688772
root15 = 3.872983346207417
courant = 0.1
theta_size = 0.3
trial_step = 0.05


def build_tables():
    points = np.array(
        [-0.8611363115940526, -0.3399810435848563, 0.3399810435848563, 0.8611363115940526]
    )
    weights = np.array(
        [0.3478548451374538, 0.6521451548625461, 0.6521451548625461, 0.3478548451374538]
    )
    points = 0.5 * (points + 1.0)
    weights = 0.5 * weights
    node_points = np.array([0.0, 1.0 / 3.0, 2.0 / 3.0, 1.0])
    value_table = np.zeros((4, 4))
    slope_table = np.zeros((4, 4))
    for column in range(4):
        others = [node_points[member] for member in range(4) if member != column]
        denominator = np.prod([node_points[column] - member for member in others])
        for quad_row in range(4):
            gauss_point = points[quad_row]
            value_table[quad_row, column] = (
                np.prod([gauss_point - member for member in others]) / denominator
            )
            slope_table[quad_row, column] = (
                sum(
                    np.prod(
                        [gauss_point - others[position] for position in range(3) if position != skipped]
                    )
                    for skipped in range(3)
                )
                / denominator
            )
    centred = 2.0 * points - 1.0
    legendre_table = np.stack(
        [
            np.full(4, p0),
            p1 * centred,
            p2 * 0.5 * (3.0 * centred**2 - 1.0),
        ],
        axis=1,
    )
    return value_table, slope_table, legendre_table, weights


VALUES, SLOPES, LEGENDRE, WEIGHTS = build_tables()


def iota(shape, dim):
    return lax.broadcasted_iota(jnp.int32, shape, dim)


def lanes(x, by):
    return pltpu.roll(x, (-by) % 128, x.ndim - 1)


def rows(x, by):
    return pltpu.roll(x, (-by) % 8, x.ndim - 2)


def following(x, d):
    return rows(x, 1) if d == 1 else lanes(x, 8 if d == 0 else 1)


def preceding(x, d):
    return rows(x, -1) if d == 1 else lanes(x, -8 if d == 0 else -1)


def following3(x, d):
    if d < 2:
        return following(x, d)
    return jnp.stack([x[1], x[2], lanes(x[0], 1)])


def preceding3(x, d):
    if d < 2:
        return preceding(x, d)
    return jnp.stack([lanes(x[2], -1), x[0], x[1]])


def halves(x):
    return (x[0] + x[3], x[1] + x[2], x[0] - x[3], x[1] - x[2])


def apply_table(table, sign, half):
    ea, eb, oa, ob = half
    out = [None] * 4
    for p in range(2):
        even = float(0.5 * (table[p, 0] + table[p, 3])) * ea + float(0.5 * (table[p, 1] + table[p, 2])) * eb
        odd = float(0.5 * (table[p, 0] - table[p, 3])) * oa + float(0.5 * (table[p, 1] - table[p, 2])) * ob
        out[p] = even + odd
        out[3 - p] = even - odd if sign > 0 else odd - even
    return out


def transpose_kernel(g_ref, u_ref, v_ref, x_ref, tuv_ref, tx_ref, halo_ref, uv_s, x_s):
    zero = jnp.zeros((16, 384), jnp.float32)
    for a in range(2):
        for m in range(27):
            uv_s[64 * a + 2 * m : 64 * a + 2 * m + 2, :] = u_ref[m, a]
        for d in range(3):
            uv_s[64 * a + 54 + 2 * d : 64 * a + 56 + 2 * d, :] = v_ref[d, a]
        uv_s[64 * a + 60 : 64 * a + 64, :] = zero[0:4, 0:128]
        at = 64 * (1 - a)
        for n in range(27):
            c, kx, ky = n // 9, (n // 3) % 3, n % 3
            for b in range(2):
                x_s[at + 2 * n + b : at + 2 * n + b + 1, :] = x_ref[c, 3 * a + kx, ky + 3 * b : ky + 3 * b + 1, :]
        x_s[at + 54 : at + 64, :] = zero[0:10]
    tuv_ref[...] = uv_s[...].T
    for n in range(3):
        tx_ref[128 * n : 128 * n + 128, :] = x_s[:, 128 * n : 128 * n + 128].T
    speed = jnp.abs(v_ref[0]) + jnp.abs(v_ref[1]) + jnp.abs(v_ref[2])
    speed = jnp.maximum(speed[0], speed[1])
    fastest = jnp.broadcast_to(jnp.max(speed, axis=(0, 1), keepdims=True), (1, 128))
    for n in range(NZ):
        halo_ref[n, :, :] = zero[0:16, 0:128]
        halo_ref[n, 13:14, :] = fastest
    up = lax.rem(g_ref[0] + 1, NZ)
    down = lax.rem(g_ref[0] + NZ - 1, NZ)
    halo_ref[up, 0:9, :] = tuv_ref[119:128, :]
    halo_ref[up, 9:12, :] = tx_ref[381:384, :]
    halo_ref[down, 0:9, :] = tuv_ref[0:9, :]
    halo_ref[down, 9:13, :] = tx_ref[0:4, :]


def pack_kernel(g_ref, tuv_ref, tx_ref, halo_ref, out_ref, uv_s, x_s, uv2_s, x2_s):
    below = lax.rem(g_ref[0] + NZ - 1, NZ)
    above = lax.rem(g_ref[0] + 1, NZ)
    uv_s[0:16, :] = jnp.zeros((16, 128), jnp.float32)
    uv_s[144:160, :] = jnp.zeros((16, 128), jnp.float32)
    x_s[0:8, :] = jnp.zeros((8, 128), jnp.float32)
    x_s[392:408, :] = jnp.zeros((16, 128), jnp.float32)
    uv_s[16:144, :] = tuv_ref[...]
    x_s[8:392, :] = tx_ref[...]
    uv_s[7:16, :] = halo_ref[below, 0:9, :]
    uv_s[144:153, :] = halo_ref[above, 0:9, :]
    x_s[5:8, :] = halo_ref[below, 9:12, :]
    x_s[392:396, :] = halo_ref[above, 9:13, :]
    uv2_s[...] = lanes(uv_s[...], 64)
    x2_s[...] = lanes(x_s[...], 64)
    fastest = halo_ref[0, 13:14, :]
    for n in range(1, NZ):
        fastest = jnp.maximum(fastest, halo_ref[n, 13:14, :])
    lane = iota((24, 128), 1)
    for k in range(NXY):
        at = IN_ROWS * k
        uv, x = pl.ds(4 * k + 7, 24), pl.ds(12 * k + 5, 24)
        first = jnp.where(lane < 64, uv_s[uv, :], x_s[x, :])
        out_ref[at : at + 24, :] = jnp.where(lane < 120, first, fastest)
        out_ref[at + 24 : at + 48, :] = jnp.where(lane < 64, uv2_s[uv, :], x2_s[x, :])


def corner_fill(ref):
    def one(c, carry):
        at = c * 64
        for kx in range(3):
            for ky in range(3):
                ref[at + kx * 16 + ky * 4 + 3] = following(ref[at + kx * 16 + ky * 4], 2)
        for kx in range(3):
            for kz in range(4):
                ref[at + kx * 16 + 12 + kz] = following(ref[at + kx * 16 + kz], 1)
        for ky in range(4):
            for kz in range(4):
                ref[at + 48 + ky * 4 + kz] = following(ref[at + ky * 4 + kz], 0)
        return carry

    lax.fori_loop(0, 3, one, 0)


def corner_fold(ref):
    def one(c, carry):
        at = c * 64
        for ky in range(4):
            for kz in range(4):
                n = at + ky * 4 + kz
                ref[n] = ref[n] + preceding(ref[n + 48], 0)
        for kx in range(3):
            for kz in range(4):
                n = at + kx * 16 + kz
                ref[n] = ref[n] + preceding(ref[n + 12], 1)
        for kx in range(3):
            for ky in range(3):
                n = at + kx * 16 + ky * 4
                ref[n] = ref[n] + preceding(ref[n + 3], 2)
        return carry

    lax.fori_loop(0, 3, one, 0)


def slopes_at_points(src, dst, a_s, b_s):
    def one(c, carry):
        at = c * 64
        for line in range(16):
            h = halves([src[at + k * 16 + line] for k in range(4)])
            v = apply_table(VALUES, 1, h)
            s = apply_table(SLOPES, -1, h)
            for p in range(4):
                a_s[p * 16 + line] = v[p]
                a_s[64 + p * 16 + line] = s[p]
        for p in range(4):
            for kz in range(4):
                hv = halves([a_s[p * 16 + k * 4 + kz] for k in range(4)])
                hs = halves([a_s[64 + p * 16 + k * 4 + kz] for k in range(4)])
                sv = apply_table(VALUES, 1, hs)
                vs = apply_table(SLOPES, -1, hv)
                vv = apply_table(VALUES, 1, hv)
                for r in range(4):
                    b_s[p * 16 + r * 4 + kz] = sv[r]
                    b_s[64 + p * 16 + r * 4 + kz] = vs[r]
                    b_s[128 + p * 16 + r * 4 + kz] = vv[r]
        for pr in range(16):
            for col in range(3):
                h = halves([b_s[64 * col + pr * 4 + k] for k in range(4)])
                out = apply_table(SLOPES, -1, h) if col == 2 else apply_table(VALUES, 1, h)
                for t in range(4):
                    dst[c * 192 + 64 * col + pr * 4 + t] = out[t]
        return carry

    lax.fori_loop(0, 3, one, 0)


def points_to_corners(src, dst, a_s, b_s):
    values_t, slopes_t = VALUES.T, SLOPES.T

    def one(c, carry):
        at = c * 64
        for pr in range(16):
            for col in range(3):
                h = halves([src[c * 192 + 64 * col + pr * 4 + t] for t in range(4)])
                out = apply_table(slopes_t, -1, h) if col == 2 else apply_table(values_t, 1, h)
                for k in range(4):
                    b_s[64 * col + pr * 4 + k] = out[k]
        for p in range(4):
            for kz in range(4):
                sv = apply_table(values_t, 1, halves([b_s[p * 16 + r * 4 + kz] for r in range(4)]))
                vs = apply_table(slopes_t, -1, halves([b_s[64 + p * 16 + r * 4 + kz] for r in range(4)]))
                vv = apply_table(values_t, 1, halves([b_s[128 + p * 16 + r * 4 + kz] for r in range(4)]))
                for k in range(4):
                    a_s[p * 16 + k * 4 + kz] = vv[k] + vs[k]
                    a_s[64 + p * 16 + k * 4 + kz] = sv[k]
        for line in range(16):
            v = apply_table(values_t, 1, halves([a_s[p * 16 + line] for p in range(4)]))
            s = apply_table(slopes_t, -1, halves([a_s[64 + p * 16 + line] for p in range(4)]))
            for k in range(4):
                dst[at + k * 16 + line] = v[k] + s[k]
        return carry

    lax.fori_loop(0, 3, one, 0)


def legendre_line(u):
    base = p0 * u[0]
    out = [None] * 4
    for p in range(2):
        even = base + float(LEGENDRE[p, 2]) * u[2]
        odd = float(LEGENDRE[p, 1]) * u[1]
        out[p] = even + odd
        out[3 - p] = even - odd
    return out


def sample_sizes(u_s, size_s, a_s):
    for bc in range(9):
        out = legendre_line([u_s[8 * (a * 9 + bc) : 8 * (a * 9 + bc) + 8, :] for a in range(3)])
        for p in range(4):
            a_s[p * 9 + bc] = out[p]
    for p in range(4):
        grid = [[None] * 3 for _ in range(4)]
        for c in range(3):
            out = legendre_line([a_s[p * 9 + b * 3 + c] for b in range(3)])
            for r in range(4):
                grid[r][c] = out[r]
        for r in range(4):
            out = legendre_line(grid[r])
            for t in range(4):
                size_s[p * 16 + r * 4 + t] = jnp.exp(theta_size * out[t])


PAIRS = ((0, 0), (1, 1), (2, 2), (0, 1), (0, 2), (1, 2))
AT = {pair: n for n, pair in enumerate(PAIRS)} | {(b, a): n for n, (a, b) in enumerate(PAIRS)}


def dot6(x, y):
    return x[0] * y[0] + x[1] * y[1] + x[2] * y[2] + 2.0 * (x[3] * y[3] + x[4] * y[4] + x[5] * y[5])


def weight_of(pr):
    def w(k):
        return jnp.where((k == 0) | (k == 3), jnp.float32(WEIGHTS[0]), jnp.float32(WEIGHTS[1]))

    return w(pr >> 2) * w(pr & 3)


def jacobian(j_s, q):
    jac = [[j_s[c * 192 + col * 64 + q] for col in range(3)] for c in range(3)]
    for c in range(3):
        jac[c][c] = jac[c][c] + 1.0
    return jac


def stress(j_s, size_s, g_s, p_s):
    def one(pr, energy):
        pair_weight = weight_of(pr)
        for t in range(4):
            q = pr * 4 + t
            jac = jacobian(j_s, q)
            size = size_s[q]
            inverse = 1.0 / size
            inverse2 = inverse * inverse
            weighted = (pair_weight * float(WEIGHTS[t])) * size
            dev = []
            for n, (a, b) in enumerate(PAIRS):
                gram = (jac[0][a] * jac[0][b] + jac[1][a] * jac[1][b] + jac[2][a] * jac[2][b]) * inverse2
                dev.append(gram - 1.0 if a == b else gram)
                g_s[n * 64 + q] = dev[n]
            energy = energy + weighted * size * size * dot6(dev, dev)
            scaled = [4.0 * weighted * d for d in dev]
            for c in range(3):
                for col in range(3):
                    p_s[c * 192 + col * 64 + q] = (
                        jac[c][0] * scaled[AT[0, col]]
                        + jac[c][1] * scaled[AT[1, col]]
                        + jac[c][2] * scaled[AT[2, col]]
                    )
        return energy

    return lax.fori_loop(0, 16, one, jnp.zeros((8, 128), jnp.float32))


def trial_terms(j_s, size_s, g_s, d_s):
    def one(pr, sums):
        e2, e3, e4 = sums
        pair_weight = weight_of(pr)
        for t in range(4):
            q = pr * 4 + t
            jac = jacobian(j_s, q)
            der = [[d_s[c * 192 + col * 64 + q] for col in range(3)] for c in range(3)]
            size = size_s[q]
            inverse = 1.0 / size
            inverse2 = inverse * inverse
            weighted = (pair_weight * float(WEIGHTS[t])) * size * size * size
            dev, first, second = [], [], []
            for n, (a, b) in enumerate(PAIRS):
                dev.append(g_s[n * 64 + q])
                if a == b:
                    f = 2.0 * (jac[0][a] * der[0][a] + jac[1][a] * der[1][a] + jac[2][a] * der[2][a])
                else:
                    f = (
                        jac[0][a] * der[0][b] + jac[1][a] * der[1][b] + jac[2][a] * der[2][b]
                        + jac[0][b] * der[0][a] + jac[1][b] * der[1][a] + jac[2][b] * der[2][a]
                    )
                first.append(f * inverse2)
                second.append((der[0][a] * der[0][b] + der[1][a] * der[1][b] + der[2][a] * der[2][b]) * inverse2)
            e2 = e2 + weighted * (dot6(first, first) + 2.0 * dot6(dev, second))
            e3 = e3 - 2.0 * weighted * dot6(first, second)
            e4 = e4 + weighted * dot6(second, second)
        return e2, e3, e4

    zero = jnp.zeros((8, 128), jnp.float32)
    return lax.fori_loop(0, 16, one, (zero, zero, zero))


def remap(u_s, v_s, mid_s, face_s, time_step):
    def mode(ref, m):
        return ref[24 * m : 24 * m + 24, :].reshape(3, 8, 128)

    def put(ref, m, value):
        ref[24 * m : 24 * m + 24, :] = value.reshape(24, 128)

    for d in range(3):
        v = mode(v_s, d)
        face = 0.5 * (v + following3(v, d))
        put(face_s, 4 * d, 2.0 * time_step * jnp.maximum(face, 0.0))
        put(face_s, 4 * d + 1, 2.0 * time_step * jnp.minimum(face, 0.0))
        put(face_s, 4 * d + 2, (2.0 * root3) * time_step * v)
        put(face_s, 4 * d + 3, (2.0 * root15) * time_step * v)

    def terms(src, d, m, step):
        u0, u1, u2 = mode(src, m), mode(src, m + step), mode(src, m + 2 * step)
        even = p0 * u0 + p2 * u2
        odd = p1 * u1
        flux = mode(face_s, 4 * d) * (even + odd) + mode(face_s, 4 * d + 1) * following3(even - odd, d)
        before = preceding3(flux, d)
        jump = before - flux
        return (
            p0 * jump,
            mode(face_s, 4 * d + 2) * u0 - p1 * (flux + before),
            mode(face_s, 4 * d + 3) * u1 + p2 * jump,
        )

    dims = (
        (0, 9, range(9)),
        (1, 3, (0, 1, 2, 9, 10, 11, 18, 19, 20)),
        (2, 1, range(0, 27, 3)),
    )

    def substep(_, carry):
        for d, step, starts in dims:
            for m in starts:
                for n, term in enumerate(terms(u_s, d, m, step)):
                    at = m + n * step
                    put(mid_s, at, mode(u_s if d == 0 else mid_s, at) + term)
        for d, step, starts in dims:
            for m in starts:
                for n, term in enumerate(terms(mid_s, d, m, step)):
                    at = m + n * step
                    old = 0.5 * (mode(u_s, at) + mode(mid_s, at)) if d == 0 else mode(u_s, at)
                    put(u_s, at, old + 0.5 * term)
        return carry

    lax.fori_loop(0, SUBSTEPS, substep, 0)


def main_kernel(
    in_ref, out_ref, t_s, u_s, v_s, mid_s, face_s, uf_s, g3_s, x_s, a_s, b_s, j_s, p_s, g_s, size_s
):
    corners = [(n, kz, (n // 9) * 64 + ((n // 3) % 3) * 16 + (n % 3) * 4 + kz) for n in range(27) for kz in range(3)]
    for t in range(3):
        for j in range(4):
            stacked = [
                in_ref[pl.ds((4 * i + j) * IN_ROWS + 24 * a + t, 8, stride=3), :]
                for i in range(8)
                for a in range(2)
            ]
            t_s[...] = jnp.concatenate(stacked, axis=0).T
            for b in range(2):
                y = 2 * j + b
                u_s[pl.ds(8 * t + y, 27, stride=24), :] = t_s[pl.ds(b, 27, stride=2), :]
                v_s[pl.ds(8 * t + y, 3, stride=24), :] = t_s[pl.ds(54 + b, 3, stride=2), :]
                g3_s[pl.ds(216 * t + y, 27, stride=8), :] = t_s[pl.ds(64 + b, 27, stride=2), :]
    lane = iota((8, 128), 1)
    fastest = jnp.max(in_ref[pl.ds(0, NXY, stride=IN_ROWS), :], axis=0, keepdims=True)
    fastest = jnp.where(iota((1, 128), 1) < 120, 0.0, fastest)
    fastest = jnp.broadcast_to(jnp.max(fastest, axis=1, keepdims=True), (8, 128))
    remap(u_s, v_s, mid_s, face_s, courant / jnp.maximum(fastest, 0.25))

    layer = lane & 7
    for m in range(27):
        u0, u1, u2 = (u_s[24 * m + 8 * t : 24 * m + 8 * t + 8, :] for t in range(3))
        value = jnp.where(layer == 3, u2, u0)
        value = jnp.where(layer < 2, lanes(jnp.where(layer == 2, u2, u0), 2), value)
        value = jnp.where(layer == 2, lanes(u1, 1), value)
        uf_s[8 * m : 8 * m + 8, :] = jnp.where(layer == 5, lanes(u1, -1), value)
    for n, kz, at in corners:
        x_s[at] = g3_s[216 * kz + 8 * n : 216 * kz + 8 * n + 8, :]
    corner_fill(x_s)
    slopes_at_points(x_s, j_s, a_s, b_s)
    sample_sizes(uf_s, size_s, a_s)
    energy = stress(j_s, size_s, g_s, p_s)
    points_to_corners(p_s, x_s, a_s, b_s)
    corner_fold(x_s)
    square = jnp.zeros((8, 128), jnp.float32)
    for n, kz, at in corners:
        grad = x_s[at]
        g3_s[216 * kz + 8 * n : 216 * kz + 8 * n + 8, :] = grad
        square = square + grad * grad
    corner_fill(x_s)
    slopes_at_points(x_s, p_s, a_s, b_s)
    sums = (energy, square) + trial_terms(j_s, size_s, g_s, p_s)
    own = jnp.abs(2 * layer - 5) < 4
    t_s[...] = jnp.zeros((128, 128), jnp.float32)
    for n, part in enumerate(sums):
        total = jnp.sum(jnp.where(own, part, 0.0), axis=(0, 1), keepdims=True)
        t_s[SUM_LANE + n : SUM_LANE + 1 + n, :] = jnp.broadcast_to(total, (1, 128))
    for p in range(2):
        for j in range(4):
            for b in range(2):
                y = 2 * j + b
                first = uf_s[pl.ds(y, 27, stride=8), :] if p == 0 else g3_s[pl.ds(216 + y, 27, stride=8), :]
                t_s[pl.ds(b, 27, stride=2), :] = first
                t_s[pl.ds(64 + b, 27, stride=2), :] = g3_s[pl.ds(432 * p + y, 27, stride=8), :]
            back = t_s[...].T
            for i in range(8):
                for a in range(2):
                    to = (4 * i + j) * OUT_ROWS + 8 * p + 4 * a
                    at = (2 * i + a) * 8 + 1
                    out_ref[to : to + 4, :] = back[at : at + 4, :]


def unpack_kernel(in_ref, u_ref, g_ref, sums_ref, u_s, g_s):
    def part(p, a, layer):
        return in_ref[pl.ds(8 * p + 4 * a + layer, NXY, stride=OUT_ROWS), :]

    low = iota((NXY, 128), 1) < 64
    for layer in range(4):
        for a in range(2):
            u_s[pl.ds(128 * a + layer, NXY, stride=4), :] = part(0, a, layer)
        for kz in range(3):
            first, second = part((kz + 1) // 2, 0, layer), part((kz + 1) // 2, 1, layer)
            if kz == 1:
                both = jnp.where(low, first, lanes(second, 64))
            else:
                both = jnp.where(low, lanes(first, 64), second)
            g_s[pl.ds(3 * layer + kz, NXY, stride=12), :] = both
    sums_ref[...] = jnp.broadcast_to(jnp.sum(part(0, 0, 0), axis=0, keepdims=True)[None], (NZ, 1, 128))
    for a in range(2):
        back = u_s[128 * a : 128 * a + 128, :].T
        for m in range(27):
            u_ref[m, a] = back[2 * m : 2 * m + 2, :]
    for n in range(3):
        back = g_s[128 * n : 128 * n + 128, :].T
        for a in range(2):
            for q in range(27):
                c, kx, ky = q // 9, (q // 3) % 3, q % 3
                for b in range(2):
                    at = 64 * a + 2 * q + b
                    g_ref[c, 3 * a + kx, ky + 3 * b : ky + 3 * b + 1, 128 * n : 128 * n + 128] = back[at : at + 1, :]


def checks_kernel(sums_ref, out_ref):
    sums = sums_ref[0]
    for n in range(1, NZ):
        sums = sums + sums_ref[n]
    lane = iota((1, 128), 1)
    e0, square, e2, e3, e4 = (
        jnp.sum(jnp.where(lane == SUM_LANE + n, sums, 0.0), axis=1, keepdims=True) for n in range(5)
    )
    elements = float(512 * NXY * NZ)
    entries = 81.0 * elements
    step = trial_step / jnp.sqrt(1.0 + square / entries)
    trial = e0 + step * (-square + step * (e2 + step * (e3 + step * e4)))
    for n, value in enumerate((e0 / elements, square / entries, trial / elements)):
        out_ref[n] = value[0, 0]


def shape(*dims):
    return jax.ShapeDtypeStruct(dims, jnp.float32)


def vmem(*dims):
    return pltpu.VMEM(dims, jnp.float32)


MAIN_SCRATCH = [
    vmem(128, 128),
    vmem(27 * 24, 128),
    vmem(3 * 24, 128),
    vmem(27 * 24, 128),
    vmem(12 * 24, 128),
    vmem(27 * 8, 128),
    vmem(81 * 8, 128),
    vmem(192, 8, 128),
    vmem(128, 8, 128),
    vmem(192, 8, 128),
    vmem(576, 8, 128),
    vmem(576, 8, 128),
    vmem(384, 8, 128),
    vmem(64, 8, 128),
]
SMEM = pl.BlockSpec(memory_space=pltpu.SMEM)
VMEM = pl.BlockSpec(memory_space=pltpu.VMEM)


def on_device(displacement, size_field_modes, velocity):
    at_z = lax.axis_index(GZ).reshape(1).astype(jnp.int32)
    tuv, tx, halo = pl.pallas_call(
        transpose_kernel,
        out_shape=(shape(128, 128), shape(384, 128), shape(NZ, HALO_ROWS, 128)),
        in_specs=[SMEM, VMEM, VMEM, VMEM],
        out_specs=(VMEM, VMEM, VMEM),
        scratch_shapes=[vmem(128, 128), vmem(128, 384)],
        name="transpose",
    )(at_z, size_field_modes, velocity, displacement)
    halo = lax.all_to_all(halo, GZ, 0, 0)
    packed = pl.pallas_call(
        pack_kernel,
        out_shape=shape(NXY * IN_ROWS, 128),
        in_specs=[SMEM, VMEM, VMEM, VMEM],
        out_specs=VMEM,
        scratch_shapes=[vmem(160, 128), vmem(408, 128), vmem(160, 128), vmem(408, 128)],
        name="pack",
    )(at_z, tuv, tx, halo)
    spread = lax.all_to_all(packed.reshape(NXY, IN_ROWS, 128), XY, 0, 0)
    result = pl.pallas_call(
        main_kernel,
        out_shape=shape(NXY * OUT_ROWS, 128),
        in_specs=[VMEM],
        out_specs=VMEM,
        scratch_shapes=MAIN_SCRATCH,
        name="remap_and_gradient",
    )(spread.reshape(NXY * IN_ROWS, 128))
    result = lax.all_to_all(result.reshape(NXY, OUT_ROWS, 128), XY, 0, 0)
    advected, gradient, sums = pl.pallas_call(
        unpack_kernel,
        out_shape=(shape(27, 2, 2, 128), shape(3, 6, 6, 384), shape(NZ, 1, 128)),
        in_specs=[VMEM],
        out_specs=(VMEM, VMEM, VMEM),
        scratch_shapes=[vmem(256, 128), vmem(384, 128)],
        name="unpack",
    )(result.reshape(NXY * OUT_ROWS, 128))
    sums = lax.all_to_all(sums, GZ, 0, 0)
    checks = pl.pallas_call(
        checks_kernel, out_shape=shape(3), in_specs=[VMEM], out_specs=SMEM, name="checks"
    )(sums)
    return advected, gradient, checks


def solution(mesh):
    finer = Mesh(
        mesh.devices.reshape(4, 2, mesh.shape["gy"], 4, 2), ("gx_0", "gx_1", "gy", "gz_0", "gz_1")
    )
    return jax.shard_map(
        on_device,
        mesh=finer,
        in_specs=(P(None, GX, "gy", GZ), P(None, GX, "gy", GZ), P(None, GX, "gy", GZ)),
        out_specs=(P(None, GX, "gy", GZ), P(None, GX, "gy", GZ), P()),
        check_vma=False,
    )
```

```python
import jax
import jax.numpy as jnp
import numpy as np
from jax import lax
from jax.experimental import pallas as pl
from jax.experimental.pallas import tpu as pltpu
from jax.sharding import Mesh
from jax.sharding import PartitionSpec as P

SUBSTEPS = 4
GX = ("gx_0", "gx_1")
GZ = ("gz_0", "gz_1")
XY = ("gx_0", "gx_1", "gy")

NZ = 8
NXY = 32
HALO_ROWS = 16
IN_ROWS = 48
SUM_LANE = 120
OUT_ROWS = 16

p0 = 0.7071067811865476
p1 = 1.224744871391589
p2 = 1.5811388300841898
root3 = 1.7320508075688772
root15 = 3.872983346207417
courant = 0.1
theta_size = 0.3
trial_step = 0.05


def build_tables():
    points = np.array(
        [-0.8611363115940526, -0.3399810435848563, 0.3399810435848563, 0.8611363115940526]
    )
    weights = np.array(
        [0.3478548451374538, 0.6521451548625461, 0.6521451548625461, 0.3478548451374538]
    )
    points = 0.5 * (points + 1.0)
    weights = 0.5 * weights
    node_points = np.array([0.0, 1.0 / 3.0, 2.0 / 3.0, 1.0])
    value_table = np.zeros((4, 4))
    slope_table = np.zeros((4, 4))
    for column in range(4):
        others = [node_points[member] for member in range(4) if member != column]
        denominator = np.prod([node_points[column] - member for member in others])
        for quad_row in range(4):
            gauss_point = points[quad_row]
            value_table[quad_row, column] = (
                np.prod([gauss_point - member for member in others]) / denominator
            )
            slope_table[quad_row, column] = (
                sum(
                    np.prod(
                        [gauss_point - others[position] for position in range(3) if position != skipped]
                    )
                    for skipped in range(3)
                )
                / denominator
            )
    centred = 2.0 * points - 1.0
    legendre_table = np.stack(
        [
            np.full(4, p0),
            p1 * centred,
            p2 * 0.5 * (3.0 * centred**2 - 1.0),
        ],
        axis=1,
    )
    return value_table, slope_table, legendre_table, weights


VALUES, SLOPES, LEGENDRE, WEIGHTS = build_tables()


def iota(shape, dim):
    return lax.broadcasted_iota(jnp.int32, shape, dim)


def lanes(x, by):
    return pltpu.roll(x, (-by) % 128, x.ndim - 1)


def rows(x, by):
    return pltpu.roll(x, (-by) % 8, x.ndim - 2)


def following(x, d):
    return rows(x, 1) if d == 1 else lanes(x, 8 if d == 0 else 1)


def preceding(x, d):
    return rows(x, -1) if d == 1 else lanes(x, -8 if d == 0 else -1)


def following3(x, d):
    if d < 2:
        return following(x, d)
    return jnp.stack([x[1], x[2], lanes(x[0], 1)])


def preceding3(x, d):
    if d < 2:
        return preceding(x, d)
    return jnp.stack([lanes(x[2], -1), x[0], x[1]])


def halves(x):
    return (x[0] + x[3], x[1] + x[2], x[0] - x[3], x[1] - x[2])


def apply_table(table, sign, half):
    ea, eb, oa, ob = half
    out = [None] * 4
    for p in range(2):
        even = float(0.5 * (table[p, 0] + table[p, 3])) * ea + float(0.5 * (table[p, 1] + table[p, 2])) * eb
        odd = float(0.5 * (table[p, 0] - table[p, 3])) * oa + float(0.5 * (table[p, 1] - table[p, 2])) * ob
        out[p] = even + odd
        out[3 - p] = even - odd if sign > 0 else odd - even
    return out


def transpose_kernel(g_ref, u_ref, v_ref, x_ref, tuv_ref, tx_ref, halo_ref, uv_s, x_s):
    zero = jnp.zeros((16, 384), jnp.float32)
    for a in range(2):
        for m in range(27):
            uv_s[64 * a + 2 * m : 64 * a + 2 * m + 2, :] = u_ref[m, a]
        for d in range(3):
            uv_s[64 * a + 54 + 2 * d : 64 * a + 56 + 2 * d, :] = v_ref[d, a]
        uv_s[64 * a + 60 : 64 * a + 64, :] = zero[0:4, 0:128]
        at = 64 * (1 - a)
        for n in range(27):
            c, kx, ky = n // 9, (n // 3) % 3, n % 3
            for b in range(2):
                x_s[at + 2 * n + b : at + 2 * n + b + 1, :] = x_ref[c, 3 * a + kx, ky + 3 * b : ky + 3 * b + 1, :]
        x_s[at + 54 : at + 64, :] = zero[0:10]
    tuv_ref[...] = uv_s[...].T
    for n in range(3):
        tx_ref[128 * n : 128 * n + 128, :] = x_s[:, 128 * n : 128 * n + 128].T
    speed = jnp.abs(v_ref[0]) + jnp.abs(v_ref[1]) + jnp.abs(v_ref[2])
    speed = jnp.maximum(speed[0], speed[1])
    fastest = jnp.broadcast_to(jnp.max(speed, axis=(0, 1), keepdims=True), (1, 128))
    for n in range(NZ):
        halo_ref[n, :, :] = zero[0:16, 0:128]
        halo_ref[n, 13:14, :] = fastest
    up = lax.rem(g_ref[0] + 1, NZ)
    down = lax.rem(g_ref[0] + NZ - 1, NZ)
    halo_ref[up, 0:9, :] = tuv_ref[119:128, :]
    halo_ref[up, 9:12, :] = tx_ref[381:384, :]
    halo_ref[down, 0:9, :] = tuv_ref[0:9, :]
    halo_ref[down, 9:13, :] = tx_ref[0:4, :]


def pack_kernel(g_ref, tuv_ref, tx_ref, halo_ref, out_ref, uv_s, x_s, uv2_s, x2_s):
    below = lax.rem(g_ref[0] + NZ - 1, NZ)
    above = lax.rem(g_ref[0] + 1, NZ)
    uv_s[0:16, :] = jnp.zeros((16, 128), jnp.float32)
    uv_s[144:160, :] = jnp.zeros((16, 128), jnp.float32)
    x_s[0:8, :] = jnp.zeros((8, 128), jnp.float32)
    x_s[392:408, :] = jnp.zeros((16, 128), jnp.float32)
    uv_s[16:144, :] = tuv_ref[...]
    x_s[8:392, :] = tx_ref[...]
    uv_s[7:16, :] = halo_ref[below, 0:9, :]
    uv_s[144:153, :] = halo_ref[above, 0:9, :]
    x_s[5:8, :] = halo_ref[below, 9:12, :]
    x_s[392:396, :] = halo_ref[above, 9:13, :]
    uv2_s[...] = lanes(uv_s[...], 64)
    x2_s[...] = lanes(x_s[...], 64)
    fastest = halo_ref[0, 13:14, :]
    for n in range(1, NZ):
        fastest = jnp.maximum(fastest, halo_ref[n, 13:14, :])
    lane = iota((24, 128), 1)
    for k in range(NXY):
        at = IN_ROWS * k
        uv, x = pl.ds(4 * k + 7, 24), pl.ds(12 * k + 5, 24)
        first = jnp.where(lane < 64, uv_s[uv, :], x_s[x, :])
        out_ref[at : at + 24, :] = jnp.where(lane < 120, first, fastest)
        out_ref[at + 24 : at + 48, :] = jnp.where(lane < 64, uv2_s[uv, :], x2_s[x, :])


def corner_fill(ref):
    def one(c, carry):
        at = c * 64
        for kx in range(3):
            for ky in range(3):
                ref[at + kx * 16 + ky * 4 + 3] = following(ref[at + kx * 16 + ky * 4], 2)
        for kx in range(3):
            for kz in range(4):
                ref[at + kx * 16 + 12 + kz] = following(ref[at + kx * 16 + kz], 1)
        for ky in range(4):
            for kz in range(4):
                ref[at + 48 + ky * 4 + kz] = following(ref[at + ky * 4 + kz], 0)
        return carry

    lax.fori_loop(0, 3, one, 0)


def corner_fold(ref):
    def one(c, carry):
        at = c * 64
        for ky in range(4):
            for kz in range(4):
                n = at + ky * 4 + kz
                ref[n] = ref[n] + preceding(ref[n + 48], 0)
        for kx in range(3):
            for kz in range(4):
                n = at + kx * 16 + kz
                ref[n] = ref[n] + preceding(ref[n + 12], 1)
        for kx in range(3):
            for ky in range(3):
                n = at + kx * 16 + ky * 4
                ref[n] = ref[n] + preceding(ref[n + 3], 2)
        return carry

    lax.fori_loop(0, 3, one, 0)


def slopes_at_points(src, dst, a_s, b_s):
    def one(c, carry):
        at = c * 64
        for line in range(16):
            h = halves([src[at + k * 16 + line] for k in range(4)])
            v = apply_table(VALUES, 1, h)
            s = apply_table(SLOPES, -1, h)
            for p in range(4):
                a_s[p * 16 + line] = v[p]
                a_s[64 + p * 16 + line] = s[p]
        for p in range(4):
            for kz in range(4):
                hv = halves([a_s[p * 16 + k * 4 + kz] for k in range(4)])
                hs = halves([a_s[64 + p * 16 + k * 4 + kz] for k in range(4)])
                sv = apply_table(VALUES, 1, hs)
                vs = apply_table(SLOPES, -1, hv)
                vv = apply_table(VALUES, 1, hv)
                for r in range(4):
                    b_s[p * 16 + r * 4 + kz] = sv[r]
                    b_s[64 + p * 16 + r * 4 + kz] = vs[r]
                    b_s[128 + p * 16 + r * 4 + kz] = vv[r]
        for pr in range(16):
            for col in range(3):
                h = halves([b_s[64 * col + pr * 4 + k] for k in range(4)])
                out = apply_table(SLOPES, -1, h) if col == 2 else apply_table(VALUES, 1, h)
                for t in range(4):
                    dst[c * 192 + 64 * col + pr * 4 + t] = out[t]
        return carry

    lax.fori_loop(0, 3, one, 0)


def points_to_corners(src, dst, a_s, b_s):
    values_t, slopes_t = VALUES.T, SLOPES.T

    def one(c, carry):
        at = c * 64
        for pr in range(16):
            for col in range(3):
                h = halves([src[c * 192 + 64 * col + pr * 4 + t] for t in range(4)])
                out = apply_table(slopes_t, -1, h) if col == 2 else apply_table(values_t, 1, h)
                for k in range(4):
                    b_s[64 * col + pr * 4 + k] = out[k]
        for p in range(4):
            for kz in range(4):
                sv = apply_table(values_t, 1, halves([b_s[p * 16 + r * 4 + kz] for r in range(4)]))
                vs = apply_table(slopes_t, -1, halves([b_s[64 + p * 16 + r * 4 + kz] for r in range(4)]))
                vv = apply_table(values_t, 1, halves([b_s[128 + p * 16 + r * 4 + kz] for r in range(4)]))
                for k in range(4):
                    a_s[p * 16 + k * 4 + kz] = vv[k] + vs[k]
                    a_s[64 + p * 16 + k * 4 + kz] = sv[k]
        for line in range(16):
            v = apply_table(values_t, 1, halves([a_s[p * 16 + line] for p in range(4)]))
            s = apply_table(slopes_t, -1, halves([a_s[64 + p * 16 + line] for p in range(4)]))
            for k in range(4):
                dst[at + k * 16 + line] = v[k] + s[k]
        return carry

    lax.fori_loop(0, 3, one, 0)


def legendre_line(u):
    base = p0 * u[0]
    out = [None] * 4
    for p in range(2):
        even = base + float(LEGENDRE[p, 2]) * u[2]
        odd = float(LEGENDRE[p, 1]) * u[1]
        out[p] = even + odd
        out[3 - p] = even - odd
    return out


def sample_sizes(u_s, size_s, a_s):
    for bc in range(9):
        out = legendre_line([u_s[8 * (a * 9 + bc) : 8 * (a * 9 + bc) + 8, :] for a in range(3)])
        for p in range(4):
            a_s[p * 9 + bc] = out[p]
    for p in range(4):
        grid = [[None] * 3 for _ in range(4)]
        for c in range(3):
            out = legendre_line([a_s[p * 9 + b * 3 + c] for b in range(3)])
            for r in range(4):
                grid[r][c] = out[r]
        for r in range(4):
            out = legendre_line(grid[r])
            for t in range(4):
                size_s[p * 16 + r * 4 + t] = jnp.exp(theta_size * out[t])


PAIRS = ((0, 0), (1, 1), (2, 2), (0, 1), (0, 2), (1, 2))
AT = {pair: n for n, pair in enumerate(PAIRS)} | {(b, a): n for n, (a, b) in enumerate(PAIRS)}


def dot6(x, y):
    return x[0] * y[0] + x[1] * y[1] + x[2] * y[2] + 2.0 * (x[3] * y[3] + x[4] * y[4] + x[5] * y[5])


def weight_of(pr):
    def w(k):
        return jnp.where((k == 0) | (k == 3), jnp.float32(WEIGHTS[0]), jnp.float32(WEIGHTS[1]))

    return w(pr >> 2) * w(pr & 3)


def jacobian(j_s, q):
    jac = [[j_s[c * 192 + col * 64 + q] for col in range(3)] for c in range(3)]
    for c in range(3):
        jac[c][c] = jac[c][c] + 1.0
    return jac


def stress(j_s, size_s, g_s, p_s):
    def one(pr, energy):
        pair_weight = weight_of(pr)
        for t in range(4):
            q = pr * 4 + t
            jac = jacobian(j_s, q)
            size = size_s[q]
            inverse = 1.0 / size
            inverse2 = inverse * inverse
            weighted = (pair_weight * float(WEIGHTS[t])) * size
            dev = []
            for n, (a, b) in enumerate(PAIRS):
                gram = (jac[0][a] * jac[0][b] + jac[1][a] * jac[1][b] + jac[2][a] * jac[2][b]) * inverse2
                dev.append(gram - 1.0 if a == b else gram)
                g_s[n * 64 + q] = dev[n]
            energy = energy + weighted * size * size * dot6(dev, dev)
            scaled = [4.0 * weighted * d for d in dev]
            for c in range(3):
                for col in range(3):
                    p_s[c * 192 + col * 64 + q] = (
                        jac[c][0] * scaled[AT[0, col]]
                        + jac[c][1] * scaled[AT[1, col]]
                        + jac[c][2] * scaled[AT[2, col]]
                    )
        return energy

    return lax.fori_loop(0, 16, one, jnp.zeros((8, 128), jnp.float32))


def trial_terms(j_s, size_s, g_s, d_s):
    def one(pr, sums):
        e2, e3, e4 = sums
        pair_weight = weight_of(pr)
        for t in range(4):
            q = pr * 4 + t
            jac = jacobian(j_s, q)
            der = [[d_s[c * 192 + col * 64 + q] for col in range(3)] for c in range(3)]
            size = size_s[q]
            inverse = 1.0 / size
            inverse2 = inverse * inverse
            weighted = (pair_weight * float(WEIGHTS[t])) * size * size * size
            dev, first, second = [], [], []
            for n, (a, b) in enumerate(PAIRS):
                dev.append(g_s[n * 64 + q])
                if a == b:
                    f = 2.0 * (jac[0][a] * der[0][a] + jac[1][a] * der[1][a] + jac[2][a] * der[2][a])
                else:
                    f = (
                        jac[0][a] * der[0][b] + jac[1][a] * der[1][b] + jac[2][a] * der[2][b]
                        + jac[0][b] * der[0][a] + jac[1][b] * der[1][a] + jac[2][b] * der[2][a]
                    )
                first.append(f * inverse2)
                second.append((der[0][a] * der[0][b] + der[1][a] * der[1][b] + der[2][a] * der[2][b]) * inverse2)
            e2 = e2 + weighted * (dot6(first, first) + 2.0 * dot6(dev, second))
            e3 = e3 - 2.0 * weighted * dot6(first, second)
            e4 = e4 + weighted * dot6(second, second)
        return e2, e3, e4

    zero = jnp.zeros((8, 128), jnp.float32)
    return lax.fori_loop(0, 16, one, (zero, zero, zero))


def remap(u_s, v_s, mid_s, face_s, time_step):
    def mode(ref, m):
        return ref[24 * m : 24 * m + 24, :].reshape(3, 8, 128)

    def put(ref, m, value):
        ref[24 * m : 24 * m + 24, :] = value.reshape(24, 128)

    for d in range(3):
        v = mode(v_s, d)
        face = 0.5 * (v + following3(v, d))
        put(face_s, 4 * d, 2.0 * time_step * jnp.maximum(face, 0.0))
        put(face_s, 4 * d + 1, 2.0 * time_step * jnp.minimum(face, 0.0))
        put(face_s, 4 * d + 2, (2.0 * root3) * time_step * v)
        put(face_s, 4 * d + 3, (2.0 * root15) * time_step * v)

    def terms(src, d, m, step):
        u0, u1, u2 = mode(src, m), mode(src, m + step), mode(src, m + 2 * step)
        even = p0 * u0 + p2 * u2
        odd = p1 * u1
        flux = mode(face_s, 4 * d) * (even + odd) + mode(face_s, 4 * d + 1) * following3(even - odd, d)
        before = preceding3(flux, d)
        jump = before - flux
        return (
            p0 * jump,
            mode(face_s, 4 * d + 2) * u0 - p1 * (flux + before),
            mode(face_s, 4 * d + 3) * u1 + p2 * jump,
        )

    dims = (
        (0, 9, range(9)),
        (1, 3, (0, 1, 2, 9, 10, 11, 18, 19, 20)),
        (2, 1, range(0, 27, 3)),
    )

    def substep(_, carry):
        for d, step, starts in dims:
            for m in starts:
                for n, term in enumerate(terms(u_s, d, m, step)):
                    at = m + n * step
                    put(mid_s, at, mode(u_s if d == 0 else mid_s, at) + term)
        for d, step, starts in dims:
            for m in starts:
                for n, term in enumerate(terms(mid_s, d, m, step)):
                    at = m + n * step
                    old = 0.5 * (mode(u_s, at) + mode(mid_s, at)) if d == 0 else mode(u_s, at)
                    put(u_s, at, old + 0.5 * term)
        return carry

    lax.fori_loop(0, SUBSTEPS, substep, 0)


def main_kernel(
    in_ref, out_ref, t_s, u_s, v_s, mid_s, face_s, uf_s, g3_s, x_s, a_s, b_s, j_s, p_s, g_s, size_s
):
    corners = [(n, kz, (n // 9) * 64 + ((n // 3) % 3) * 16 + (n % 3) * 4 + kz) for n in range(27) for kz in range(3)]
    for t in range(3):
        for j in range(4):
            stacked = [
                in_ref[pl.ds((4 * i + j) * IN_ROWS + 24 * a + t, 8, stride=3), :]
                for i in range(8)
                for a in range(2)
            ]
            t_s[...] = jnp.concatenate(stacked, axis=0).T
            for b in range(2):
                y = 2 * j + b
                u_s[pl.ds(8 * t + y, 27, stride=24), :] = t_s[pl.ds(b, 27, stride=2), :]
                v_s[pl.ds(8 * t + y, 3, stride=24), :] = t_s[pl.ds(54 + b, 3, stride=2), :]
                g3_s[pl.ds(216 * t + y, 27, stride=8), :] = t_s[pl.ds(64 + b, 27, stride=2), :]
    lane = iota((8, 128), 1)
    fastest = jnp.max(in_ref[pl.ds(0, NXY, stride=IN_ROWS), :], axis=0, keepdims=True)
    fastest = jnp.where(iota((1, 128), 1) < 120, 0.0, fastest)
    fastest = jnp.broadcast_to(jnp.max(fastest, axis=1, keepdims=True), (8, 128))
    remap(u_s, v_s, mid_s, face_s, courant / jnp.maximum(fastest, 0.25))

    layer = lane & 7
    for m in range(27):
        u0, u1, u2 = (u_s[24 * m + 8 * t : 24 * m + 8 * t + 8, :] for t in range(3))
        value = jnp.where(layer == 3, u2, u0)
        value = jnp.where(layer < 2, lanes(jnp.where(layer == 2, u2, u0), 2), value)
        value = jnp.where(layer == 2, lanes(u1, 1), value)
        uf_s[8 * m : 8 * m + 8, :] = jnp.where(layer == 5, lanes(u1, -1), value)
    for n, kz, at in corners:
        x_s[at] = g3_s[216 * kz + 8 * n : 216 * kz + 8 * n + 8, :]
    corner_fill(x_s)
    slopes_at_points(x_s, j_s, a_s, b_s)
    sample_sizes(uf_s, size_s, a_s)
    energy = stress(j_s, size_s, g_s, p_s)
    points_to_corners(p_s, x_s, a_s, b_s)
    corner_fold(x_s)
    square = jnp.zeros((8, 128), jnp.float32)
    for n, kz, at in corners:
        grad = x_s[at]
        g3_s[216 * kz + 8 * n : 216 * kz + 8 * n + 8, :] = grad
        square = square + grad * grad
    corner_fill(x_s)
    slopes_at_points(x_s, p_s, a_s, b_s)
    sums = (energy, square) + trial_terms(j_s, size_s, g_s, p_s)
    own = jnp.abs(2 * layer - 5) < 4
    t_s[...] = jnp.zeros((128, 128), jnp.float32)
    for n, part in enumerate(sums):
        total = jnp.sum(jnp.where(own, part, 0.0), axis=(0, 1), keepdims=True)
        t_s[SUM_LANE + n : SUM_LANE + 1 + n, :] = jnp.broadcast_to(total, (1, 128))
    for p in range(2):
        for j in range(4):
            for b in range(2):
                y = 2 * j + b
                first = uf_s[pl.ds(y, 27, stride=8), :] if p == 0 else g3_s[pl.ds(216 + y, 27, stride=8), :]
                t_s[pl.ds(b, 27, stride=2), :] = first
                t_s[pl.ds(64 + b, 27, stride=2), :] = g3_s[pl.ds(432 * p + y, 27, stride=8), :]
            back = t_s[...].T
            for i in range(8):
                for a in range(2):
                    to = (4 * i + j) * OUT_ROWS + 8 * p + 4 * a
                    at = (2 * i + a) * 8 + 1
                    out_ref[to : to + 4, :] = back[at : at + 4, :]


def unpack_kernel(in_ref, u_ref, g_ref, sums_ref, u_s, g_s):
    def part(p, a, layer):
        return in_ref[pl.ds(8 * p + 4 * a + layer, NXY, stride=OUT_ROWS), :]

    low = iota((NXY, 128), 1) < 64
    for layer in range(4):
        for a in range(2):
            u_s[pl.ds(128 * a + layer, NXY, stride=4), :] = part(0, a, layer)
        for kz in range(3):
            first, second = part((kz + 1) // 2, 0, layer), part((kz + 1) // 2, 1, layer)
            if kz == 1:
                both = jnp.where(low, first, lanes(second, 64))
            else:
                both = jnp.where(low, lanes(first, 64), second)
            g_s[pl.ds(3 * layer + kz, NXY, stride=12), :] = both
    sums_ref[...] = jnp.broadcast_to(jnp.sum(part(0, 0, 0), axis=0, keepdims=True)[None], (NZ, 1, 128))
    for a in range(2):
        back = u_s[128 * a : 128 * a + 128, :].T
        for m in range(27):
            u_ref[m, a] = back[2 * m : 2 * m + 2, :]
    for n in range(3):
        back = g_s[128 * n : 128 * n + 128, :].T
        for a in range(2):
            for q in range(27):
                c, kx, ky = q // 9, (q // 3) % 3, q % 3
                for b in range(2):
                    at = 64 * a + 2 * q + b
                    g_ref[c, 3 * a + kx, ky + 3 * b : ky + 3 * b + 1, 128 * n : 128 * n + 128] = back[at : at + 1, :]


def checks_kernel(sums_ref, out_ref):
    sums = sums_ref[0]
    for n in range(1, NZ):
        sums = sums + sums_ref[n]
    lane = iota((1, 128), 1)
    e0, square, e2, e3, e4 = (
        jnp.sum(jnp.where(lane == SUM_LANE + n, sums, 0.0), axis=1, keepdims=True) for n in range(5)
    )
    elements = float(512 * NXY * NZ)
    entries = 81.0 * elements
    step = trial_step / jnp.sqrt(1.0 + square / entries)
    trial = e0 + step * (-square + step * (e2 + step * (e3 + step * e4)))
    for n, value in enumerate((e0 / elements, square / entries, trial / elements)):
        out_ref[n] = value[0, 0]


def shape(*dims):
    return jax.ShapeDtypeStruct(dims, jnp.float32)


def on_chip(*dims):
    return pltpu.VMEM(dims, jnp.float32)


def keep(x):
    return pltpu.with_memory_space_constraint(x, pltpu.VMEM)


def vmem(*dims):
    return pltpu.VMEM(dims, jnp.float32)


MAIN_SCRATCH = [
    vmem(128, 128),
    vmem(27 * 24, 128),
    vmem(3 * 24, 128),
    vmem(27 * 24, 128),
    vmem(12 * 24, 128),
    vmem(27 * 8, 128),
    vmem(81 * 8, 128),
    vmem(192, 8, 128),
    vmem(128, 8, 128),
    vmem(192, 8, 128),
    vmem(576, 8, 128),
    vmem(576, 8, 128),
    vmem(384, 8, 128),
    vmem(64, 8, 128),
]
SMEM = pl.BlockSpec(memory_space=pltpu.SMEM)
VMEM = pl.BlockSpec(memory_space=pltpu.VMEM)


def on_device(displacement, size_field_modes, velocity):
    at_z = lax.axis_index(GZ).reshape(1).astype(jnp.int32)
    tuv, tx, halo = pl.pallas_call(
        transpose_kernel,
        out_shape=(on_chip(128, 128), on_chip(384, 128), on_chip(NZ, HALO_ROWS, 128)),
        in_specs=[SMEM, VMEM, VMEM, VMEM],
        out_specs=(VMEM, VMEM, VMEM),
        scratch_shapes=[vmem(128, 128), vmem(128, 384)],
        name="transpose",
    )(at_z, size_field_modes, velocity, displacement)
    halo = lax.all_to_all(halo, GZ, 0, 0)
    packed = pl.pallas_call(
        pack_kernel,
        out_shape=on_chip(NXY * IN_ROWS, 128),
        in_specs=[SMEM, VMEM, VMEM, VMEM],
        out_specs=VMEM,
        scratch_shapes=[vmem(160, 128), vmem(408, 128), vmem(160, 128), vmem(408, 128)],
        name="pack",
    )(at_z, keep(tuv), keep(tx), keep(halo))
    spread = lax.all_to_all(packed.reshape(NXY, IN_ROWS, 128), XY, 0, 0)
    result = pl.pallas_call(
        main_kernel,
        out_shape=on_chip(NXY * OUT_ROWS, 128),
        in_specs=[VMEM],
        out_specs=VMEM,
        scratch_shapes=MAIN_SCRATCH,
        name="remap_and_gradient",
    )(keep(spread.reshape(NXY * IN_ROWS, 128)))
    result = lax.all_to_all(result.reshape(NXY, OUT_ROWS, 128), XY, 0, 0)
    advected, gradient, sums = pl.pallas_call(
        unpack_kernel,
        out_shape=(shape(27, 2, 2, 128), shape(3, 6, 6, 384), on_chip(NZ, 1, 128)),
        in_specs=[VMEM],
        out_specs=(VMEM, VMEM, VMEM),
        scratch_shapes=[vmem(256, 128), vmem(384, 128)],
        name="unpack",
    )(keep(result.reshape(NXY * OUT_ROWS, 128)))
    sums = lax.all_to_all(sums, GZ, 0, 0)
    checks = pl.pallas_call(
        checks_kernel, out_shape=shape(3), in_specs=[VMEM], out_specs=SMEM, name="checks"
    )(keep(sums))
    return advected, gradient, checks


def solution(mesh):
    finer = Mesh(
        mesh.devices.reshape(4, 2, mesh.shape["gy"], 4, 2), ("gx_0", "gx_1", "gy", "gz_0", "gz_1")
    )
    return jax.shard_map(
        on_device,
        mesh=finer,
        in_specs=(P(None, GX, "gy", GZ), P(None, GX, "gy", GZ), P(None, GX, "gy", GZ)),
        out_specs=(P(None, GX, "gy", GZ), P(None, GX, "gy", GZ), P()),
        check_vma=False,
    )
```

```python
import jax
import jax.numpy as jnp
import numpy as np
from jax import lax
from jax.experimental import pallas as pl
from jax.experimental.pallas import tpu as pltpu
from jax.sharding import Mesh
from jax.sharding import PartitionSpec as P

SUBSTEPS = 4
GX = ("gx_0", "gx_1")
GZ = ("gz_0", "gz_1")
XY = ("gx_0", "gx_1", "gy")

NZ = 8
NXY = 32
HALO_ROWS = 16
IN_ROWS = 40
SUM_LANE = 120
OUT_ROWS = 16

p0 = 0.7071067811865476
p1 = 1.224744871391589
p2 = 1.5811388300841898
root3 = 1.7320508075688772
root15 = 3.872983346207417
courant = 0.1
theta_size = 0.3
trial_step = 0.05


def build_tables():
    points = np.array(
        [-0.8611363115940526, -0.3399810435848563, 0.3399810435848563, 0.8611363115940526]
    )
    weights = np.array(
        [0.3478548451374538, 0.6521451548625461, 0.6521451548625461, 0.3478548451374538]
    )
    points = 0.5 * (points + 1.0)
    weights = 0.5 * weights
    node_points = np.array([0.0, 1.0 / 3.0, 2.0 / 3.0, 1.0])
    value_table = np.zeros((4, 4))
    slope_table = np.zeros((4, 4))
    for column in range(4):
        others = [node_points[member] for member in range(4) if member != column]
        denominator = np.prod([node_points[column] - member for member in others])
        for quad_row in range(4):
            gauss_point = points[quad_row]
            value_table[quad_row, column] = (
                np.prod([gauss_point - member for member in others]) / denominator
            )
            slope_table[quad_row, column] = (
                sum(
                    np.prod(
                        [gauss_point - others[position] for position in range(3) if position != skipped]
                    )
                    for skipped in range(3)
                )
                / denominator
            )
    centred = 2.0 * points - 1.0
    legendre_table = np.stack(
        [
            np.full(4, p0),
            p1 * centred,
            p2 * 0.5 * (3.0 * centred**2 - 1.0),
        ],
        axis=1,
    )
    return value_table, slope_table, legendre_table, weights


VALUES, SLOPES, LEGENDRE, WEIGHTS = build_tables()


def iota(shape, dim):
    return lax.broadcasted_iota(jnp.int32, shape, dim)


def lanes(x, by):
    return pltpu.roll(x, (-by) % 128, x.ndim - 1)


def rows(x, by):
    return pltpu.roll(x, (-by) % 8, x.ndim - 2)


def following(x, d):
    return rows(x, 1) if d == 1 else lanes(x, 8 if d == 0 else 1)


def preceding(x, d):
    return rows(x, -1) if d == 1 else lanes(x, -8 if d == 0 else -1)


def following3(x, d):
    if d < 2:
        return following(x, d)
    return jnp.stack([x[1], x[2], lanes(x[0], 1)])


def preceding3(x, d):
    if d < 2:
        return preceding(x, d)
    return jnp.stack([lanes(x[2], -1), x[0], x[1]])


def halves(x):
    return (x[0] + x[3], x[1] + x[2], x[0] - x[3], x[1] - x[2])


def apply_table(table, sign, half):
    ea, eb, oa, ob = half
    out = [None] * 4
    for p in range(2):
        even = float(0.5 * (table[p, 0] + table[p, 3])) * ea + float(0.5 * (table[p, 1] + table[p, 2])) * eb
        odd = float(0.5 * (table[p, 0] - table[p, 3])) * oa + float(0.5 * (table[p, 1] - table[p, 2])) * ob
        out[p] = even + odd
        out[3 - p] = even - odd if sign > 0 else odd - even
    return out


def transpose_kernel(g_ref, u_ref, v_ref, x_ref, tuv_ref, tx_ref, halo_ref, uv_s, x_s):
    zero = jnp.zeros((16, 384), jnp.float32)
    for a in range(2):
        for m in range(27):
            uv_s[64 * a + 2 * m : 64 * a + 2 * m + 2, :] = u_ref[m, a]
        for d in range(3):
            uv_s[64 * a + 54 + 2 * d : 64 * a + 56 + 2 * d, :] = v_ref[d, a]
        uv_s[64 * a + 60 : 64 * a + 64, :] = zero[0:4, 0:128]
        at = 64 * (1 - a)
        for n in range(27):
            c, kx, ky = n // 9, (n // 3) % 3, n % 3
            for b in range(2):
                x_s[at + 2 * n + b : at + 2 * n + b + 1, :] = x_ref[c, 3 * a + kx, ky + 3 * b : ky + 3 * b + 1, :]
        x_s[at + 54 : at + 64, :] = zero[0:10]
    tuv_ref[...] = uv_s[...].T
    for n in range(3):
        tx_ref[128 * n : 128 * n + 128, :] = x_s[:, 128 * n : 128 * n + 128].T
    speed = jnp.abs(v_ref[0]) + jnp.abs(v_ref[1]) + jnp.abs(v_ref[2])
    speed = jnp.maximum(speed[0], speed[1])
    fastest = jnp.broadcast_to(jnp.max(speed, axis=(0, 1), keepdims=True), (1, 128))
    for n in range(NZ):
        halo_ref[n, :, :] = zero[0:16, 0:128]
        halo_ref[n, 13:14, :] = fastest
    up = lax.rem(g_ref[0] + 1, NZ)
    down = lax.rem(g_ref[0] + NZ - 1, NZ)
    halo_ref[up, 0:9, :] = tuv_ref[119:128, :]
    halo_ref[up, 9:12, :] = tx_ref[381:384, :]
    halo_ref[down, 0:9, :] = tuv_ref[0:9, :]
    halo_ref[down, 9:13, :] = tx_ref[0:4, :]


def pack_kernel(g_ref, tuv_ref, tx_ref, halo_ref, out_ref, uv_s, x_s, uv2_s, x2_s, plus_s, minus_s):
    below = lax.rem(g_ref[0] + NZ - 1, NZ)
    above = lax.rem(g_ref[0] + 1, NZ)
    uv_s[0:16, :] = jnp.zeros((16, 128), jnp.float32)
    uv_s[144:160, :] = jnp.zeros((16, 128), jnp.float32)
    x_s[0:8, :] = jnp.zeros((8, 128), jnp.float32)
    x_s[392:408, :] = jnp.zeros((16, 128), jnp.float32)
    uv_s[16:144, :] = tuv_ref[...]
    x_s[8:392, :] = tx_ref[...]
    uv_s[7:16, :] = halo_ref[below, 0:9, :]
    uv_s[144:153, :] = halo_ref[above, 0:9, :]
    x_s[5:8, :] = halo_ref[below, 9:12, :]
    x_s[392:396, :] = halo_ref[above, 9:13, :]
    uv = uv_s[...]
    uv2_s[...] = lanes(uv, 64)
    x2_s[...] = lanes(x_s[...], 64)
    lane = iota((160, 128), 1) & 63
    along_z = (lane >> 1) % 3
    even = uv + (p2 / p0) * lanes(uv, 4)
    odd = (p1 / p0) * lanes(uv, 2)
    field = lane < 54
    plus_s[...] = jnp.where(field, jnp.where(along_z == 0, even + odd, 0.0), jnp.where(lane >= 58, uv, 0.0))
    minus = lanes(even - odd, -2)
    minus_s[...] = jnp.where(field, jnp.where(along_z == 1, minus, 0.0), jnp.where(lane < 56, lanes(uv, 4), 0.0))
    fastest = halo_ref[0, 13:14, :]
    for n in range(1, NZ):
        fastest = jnp.maximum(fastest, halo_ref[n, 13:14, :])
    lane, row = iota((20, 128), 1), iota((20, 128), 0)
    at_speed = jnp.where(row == 0, lane, 0) >= SUM_LANE
    for k in range(NXY):
        at = IN_ROWS * k
        uv, x = pl.ds(4 * k + 8, 20), pl.ds(12 * k + 5, 20)
        first = jnp.where(lane < 64, uv_s[uv, :], x_s[x, :])
        out_ref[at : at + 20, :] = jnp.where(at_speed, fastest, first)
        out_ref[at + 20 : at + 40, :] = jnp.where(lane < 64, uv2_s[uv, :], x2_s[x, :])
    outer = plus_s[pl.ds(7, NXY, stride=4), :] + minus_s[pl.ds(28, NXY, stride=4), :]
    low = iota((NXY, 128), 1) < 64
    last = pl.ds(27, NXY, stride=4)
    out_ref[pl.ds(19, NXY, stride=IN_ROWS), :] = jnp.where(low, uv_s[last, :], lanes(outer, 64))
    out_ref[pl.ds(39, NXY, stride=IN_ROWS), :] = jnp.where(low, uv2_s[last, :], outer)


def corner_fill(ref):
    def one(c, carry):
        at = c * 64
        for kx in range(3):
            for ky in range(3):
                ref[at + kx * 16 + ky * 4 + 3] = following(ref[at + kx * 16 + ky * 4], 2)
        for kx in range(3):
            for kz in range(4):
                ref[at + kx * 16 + 12 + kz] = following(ref[at + kx * 16 + kz], 1)
        for ky in range(4):
            for kz in range(4):
                ref[at + 48 + ky * 4 + kz] = following(ref[at + ky * 4 + kz], 0)
        return carry

    lax.fori_loop(0, 3, one, 0)


def corner_fold(ref):
    def one(c, carry):
        at = c * 64
        for ky in range(4):
            for kz in range(4):
                n = at + ky * 4 + kz
                ref[n] = ref[n] + preceding(ref[n + 48], 0)
        for kx in range(3):
            for kz in range(4):
                n = at + kx * 16 + kz
                ref[n] = ref[n] + preceding(ref[n + 12], 1)
        for kx in range(3):
            for ky in range(3):
                n = at + kx * 16 + ky * 4
                ref[n] = ref[n] + preceding(ref[n + 3], 2)
        return carry

    lax.fori_loop(0, 3, one, 0)


def parts(x):
    ea, eb = x[0] + x[3], x[1] + x[2]
    return ea - eb, 0.5 * eb, x[0] - x[3], x[1] - x[2]


def values_of(part):
    d, half, oa, ob = part
    out = [None] * 4
    for p in range(2):
        even = float(0.5 * (VALUES[p, 0] + VALUES[p, 3])) * d + half
        odd = float(0.5 * (VALUES[p, 0] - VALUES[p, 3])) * oa + float(0.5 * (VALUES[p, 1] - VALUES[p, 2])) * ob
        out[p], out[3 - p] = even + odd, even - odd
    return out


def slopes_of(part):
    d, _, oa, ob = part
    out = [None] * 4
    for p in range(2):
        even = float(0.5 * (SLOPES[p, 0] + SLOPES[p, 3])) * d
        odd = float(0.5 * (SLOPES[p, 0] - SLOPES[p, 3])) * oa + float(0.5 * (SLOPES[p, 1] - SLOPES[p, 2])) * ob
        out[p], out[3 - p] = even + odd, odd - even
    return out


def both_back(v, s):
    (va, vb, wa, wb), (sa, sb, ta, tb) = halves(v), halves(s)
    out = [None] * 4
    for k in range(2):
        first = float(0.5 * (VALUES[0, k] + VALUES[3, k])) * va + float(0.5 * (VALUES[1, k] + VALUES[2, k])) * vb
        first = first + float(0.5 * (SLOPES[0, k] - SLOPES[3, k])) * ta + float(0.5 * (SLOPES[1, k] - SLOPES[2, k])) * tb
        second = float(0.5 * (VALUES[0, k] - VALUES[3, k])) * wa + float(0.5 * (VALUES[1, k] - VALUES[2, k])) * wb
        second = second + float(0.5 * (SLOPES[0, k] + SLOPES[3, k])) * sa + float(0.5 * (SLOPES[1, k] + SLOPES[2, k])) * sb
        out[k], out[3 - k] = first + second, first - second
    return out


def slopes_at_points(src, dst, a_s, b_s):
    def one(c, carry):
        at = c * 64
        for line in range(16):
            part = parts([src[at + k * 16 + line] for k in range(4)])
            v, s = values_of(part), slopes_of(part)
            for p in range(4):
                a_s[p * 16 + line] = v[p]
                a_s[64 + p * 16 + line] = s[p]
        for p in range(4):
            for kz in range(4):
                pv = parts([a_s[p * 16 + k * 4 + kz] for k in range(4)])
                ps = parts([a_s[64 + p * 16 + k * 4 + kz] for k in range(4)])
                sv, vs, vv = values_of(ps), slopes_of(pv), values_of(pv)
                for r in range(4):
                    b_s[p * 16 + r * 4 + kz] = sv[r]
                    b_s[64 + p * 16 + r * 4 + kz] = vs[r]
                    b_s[128 + p * 16 + r * 4 + kz] = vv[r]
        for pr in range(16):
            for col in range(3):
                part = parts([b_s[64 * col + pr * 4 + k] for k in range(4)])
                out = slopes_of(part) if col == 2 else values_of(part)
                for t in range(4):
                    dst[c * 192 + 64 * col + pr * 4 + t] = out[t]
        return carry

    lax.fori_loop(0, 3, one, 0)


def points_to_corners(src, dst, a_s, b_s):
    values_t, slopes_t = VALUES.T, SLOPES.T

    def one(c, carry):
        at = c * 64
        for pr in range(16):
            for col in range(3):
                h = halves([src[c * 192 + 64 * col + pr * 4 + t] for t in range(4)])
                out = apply_table(slopes_t, -1, h) if col == 2 else apply_table(values_t, 1, h)
                for k in range(4):
                    b_s[64 * col + pr * 4 + k] = out[k]
        for p in range(4):
            for kz in range(4):
                sv = apply_table(values_t, 1, halves([b_s[p * 16 + r * 4 + kz] for r in range(4)]))
                vs = [b_s[64 + p * 16 + r * 4 + kz] for r in range(4)]
                v = both_back([b_s[128 + p * 16 + r * 4 + kz] for r in range(4)], vs)
                for k in range(4):
                    a_s[p * 16 + k * 4 + kz] = v[k]
                    a_s[64 + p * 16 + k * 4 + kz] = sv[k]
        for line in range(16):
            out = both_back([a_s[p * 16 + line] for p in range(4)], [a_s[64 + p * 16 + line] for p in range(4)])
            for k in range(4):
                dst[at + k * 16 + line] = out[k]
        return carry

    lax.fori_loop(0, 3, one, 0)


def legendre_line(u):
    base = p0 * u[0]
    out = [None] * 4
    for p in range(2):
        even = base + float(LEGENDRE[p, 2]) * u[2]
        odd = float(LEGENDRE[p, 1]) * u[1]
        out[p] = even + odd
        out[3 - p] = even - odd
    return out


def sample_sizes(u_s, size_s, a_s):
    for bc in range(9):
        out = legendre_line([u_s[8 * (a * 9 + bc) : 8 * (a * 9 + bc) + 8, :] for a in range(3)])
        for p in range(4):
            a_s[p * 9 + bc] = out[p]
    for p in range(4):
        grid = [[None] * 3 for _ in range(4)]
        for c in range(3):
            out = legendre_line([a_s[p * 9 + b * 3 + c] for b in range(3)])
            for r in range(4):
                grid[r][c] = out[r]
        for r in range(4):
            out = legendre_line(grid[r])
            for t in range(4):
                size_s[p * 16 + r * 4 + t] = jnp.exp(theta_size * out[t])


PAIRS = ((0, 0), (1, 1), (2, 2), (0, 1), (0, 2), (1, 2))
AT = {pair: n for n, pair in enumerate(PAIRS)} | {(b, a): n for n, (a, b) in enumerate(PAIRS)}


def dot3(x, y, at):
    return x[at] * y[at] + x[at + 1] * y[at + 1] + x[at + 2] * y[at + 2]


def dot6(x, y):
    return dot3(x, y, 0) + 2.0 * dot3(x, y, 3)


def weight_of(pr):
    def w(k):
        return jnp.where((k == 0) | (k == 3), jnp.float32(WEIGHTS[0]), jnp.float32(WEIGHTS[1]))

    return w(pr >> 2) * w(pr & 3)


def jacobian(j_s, q):
    return [[j_s[c * 192 + col * 64 + q] for col in range(3)] for c in range(3)]


def stress(j_s, size_s, g_s, p_s):
    def one(pr, energy):
        pair_weight = weight_of(pr)
        for t in range(4):
            q = pr * 4 + t
            jac = jacobian(j_s, q)
            for c in range(3):
                jac[c][c] = jac[c][c] + 1.0
                j_s[c * 192 + c * 64 + q] = jac[c][c]
            size = size_s[q]
            inverse = 1.0 / size
            inverse2 = inverse * inverse
            weighted = (pair_weight * float(WEIGHTS[t])) * size
            dev = []
            for n, (a, b) in enumerate(PAIRS):
                gram = (jac[0][a] * jac[0][b] + jac[1][a] * jac[1][b] + jac[2][a] * jac[2][b]) * inverse2
                dev.append(gram - 1.0 if a == b else gram)
                g_s[n * 64 + q] = dev[n]
            energy = energy + weighted * size * size * dot6(dev, dev)
            scaled = [4.0 * weighted * d for d in dev]
            for c in range(3):
                for col in range(3):
                    p_s[c * 192 + col * 64 + q] = (
                        jac[c][0] * scaled[AT[0, col]]
                        + jac[c][1] * scaled[AT[1, col]]
                        + jac[c][2] * scaled[AT[2, col]]
                    )
        return energy

    return lax.fori_loop(0, 16, one, jnp.zeros((8, 128), jnp.float32))


def trial_terms(j_s, size_s, g_s, d_s):
    def one(pr, sums):
        e2, e3, e4 = sums
        pair_weight = weight_of(pr)
        for t in range(4):
            q = pr * 4 + t
            jac = jacobian(j_s, q)
            der = jacobian(d_s, q)
            size = size_s[q]
            point_weight = pair_weight * float(WEIGHTS[t])
            dev, first, second = [], [], []
            for n, (a, b) in enumerate(PAIRS):
                dev.append(g_s[n * 64 + q])
                cross = jac[0][a] * der[0][b] + jac[1][a] * der[1][b] + jac[2][a] * der[2][b]
                if a != b:
                    cross = cross + (jac[0][b] * der[0][a] + jac[1][b] * der[1][a] + jac[2][b] * der[2][a])
                first.append(cross)
                second.append(der[0][a] * der[0][b] + der[1][a] * der[1][b] + der[2][a] * der[2][b])
            square = 2.0 * dot3(first, first, 0) + dot3(first, first, 3)
            mixed = dot3(first, second, 0) + dot3(first, second, 3)
            low, high = point_weight * size, point_weight / size
            e2 = e2 + (high * square + low * dot6(dev, second))
            e3 = e3 + high * mixed
            e4 = e4 + high * dot6(second, second)
        return e2, e3, e4

    zero = jnp.zeros((8, 128), jnp.float32)
    e2, e3, e4 = lax.fori_loop(0, 16, one, (zero, zero, zero))
    return 2.0 * e2, -4.0 * e3, e4


def remap(u_s, v_s, mid_s, face_s, time_step):
    def mode(ref, m):
        return ref[24 * m : 24 * m + 24, :].reshape(3, 8, 128)

    def put(ref, m, value):
        ref[24 * m : 24 * m + 24, :] = value.reshape(24, 128)

    for d in range(3):
        v = mode(v_s, d)
        face = 0.5 * (v + following3(v, d))
        put(face_s, 4 * d, 2.0 * time_step * jnp.maximum(face, 0.0))
        put(face_s, 4 * d + 1, 2.0 * time_step * jnp.minimum(face, 0.0))
        put(face_s, 4 * d + 2, (2.0 * root3) * time_step * v)
        put(face_s, 4 * d + 3, (2.0 * root15) * time_step * v)

    def terms(src, d, m, step):
        u0, u1, u2 = mode(src, m), mode(src, m + step), mode(src, m + 2 * step)
        even = p0 * u0 + p2 * u2
        odd = p1 * u1
        flux = mode(face_s, 4 * d) * (even + odd) + mode(face_s, 4 * d + 1) * following3(even - odd, d)
        before = preceding3(flux, d)
        jump = before - flux
        return (
            p0 * jump,
            mode(face_s, 4 * d + 2) * u0 - p1 * (flux + before),
            mode(face_s, 4 * d + 3) * u1 + p2 * jump,
        )

    dims = (
        (0, 9, range(9)),
        (1, 3, (0, 1, 2, 9, 10, 11, 18, 19, 20)),
        (2, 1, range(0, 27, 3)),
    )

    def substep(_, carry):
        for d, step, starts in dims:
            for m in starts:
                for n, term in enumerate(terms(u_s, d, m, step)):
                    at = m + n * step
                    put(mid_s, at, mode(u_s if d == 0 else mid_s, at) + term)
        for d, step, starts in dims:
            for m in starts:
                for n, term in enumerate(terms(mid_s, d, m, step)):
                    at = m + n * step
                    old = 0.5 * (mode(u_s, at) + mode(mid_s, at)) if d == 0 else mode(u_s, at)
                    put(u_s, at, old + 0.5 * term)
        return carry

    lax.fori_loop(0, SUBSTEPS, substep, 0)


def main_kernel(
    in_ref, out_ref, in_s, outer_s, t_s, u_s, v_s, mid_s, face_s, uf_s, g3_s, x_s, a_s, b_s, j_s, p_s, g_s, size_s
):
    corners = [(n, kz, (n // 9) * 64 + ((n // 3) % 3) * 16 + (n % 3) * 4 + kz) for n in range(27) for kz in range(3)]
    in_s[0:8, :] = jnp.zeros((8, 128), jnp.float32)
    in_s[8 : 8 + NXY * IN_ROWS, :] = in_ref[...]
    in_s[8 + NXY * IN_ROWS : 16 + NXY * IN_ROWS, :] = jnp.zeros((8, 128), jnp.float32)
    outer = lanes(in_ref[pl.ds(19, 2 * NXY, stride=20), :], 64)
    lane = iota((2 * NXY, 128), 1)
    trace = jnp.where(lane < 54, (lane >> 1) % 3, 1) == 0
    speed = jnp.abs(2 * lane - 117) < 2
    outer_s[0:64, :] = jnp.where(trace, outer, jnp.where(speed, outer, 0.0))
    outer_s[64:128, :] = jnp.where(trace, lanes(outer, 2), jnp.where(speed, lanes(outer, -4), 0.0))
    row = iota((8, 128), 0)
    for t in range(3):
        for j in range(4):
            stacked = []
            for i in range(8):
                for a in range(2):
                    n = 2 * (4 * i + j) + a
                    block = in_s[pl.ds(8 + 20 * n + t - 1, 8, stride=3), :]
                    if t == 0:
                        block = jnp.where(row == 0, outer_s[n : n + 1, :], block)
                        block = jnp.where(row == 7, outer_s[64 + n : 65 + n, :], block)
                    stacked.append(block)
            t_s[...] = jnp.concatenate(stacked, axis=0).T
            for b in range(2):
                y = 2 * j + b
                u_s[pl.ds(8 * t + y, 27, stride=24), :] = t_s[pl.ds(b, 27, stride=2), :]
                v_s[pl.ds(8 * t + y, 3, stride=24), :] = t_s[pl.ds(54 + b, 3, stride=2), :]
                nodes = t_s[pl.ds(64 + b, 27, stride=2), :]
                if t == 0:
                    nodes = lanes(nodes, 1)
                g3_s[pl.ds(216 * ((t + 2) % 3) + y, 27, stride=8), :] = nodes
    lane = iota((8, 128), 1)
    fastest = jnp.max(in_ref[pl.ds(0, NXY, stride=IN_ROWS), :], axis=0, keepdims=True)
    fastest = jnp.where(iota((1, 128), 1) < SUM_LANE, 0.0, fastest)
    fastest = jnp.broadcast_to(jnp.max(fastest, axis=1, keepdims=True), (8, 128))
    remap(u_s, v_s, mid_s, face_s, courant / jnp.maximum(fastest, 0.25))

    layer = lane & 7
    for m in range(27):
        u0, u1, u2 = (u_s[24 * m + 8 * t : 24 * m + 8 * t + 8, :] for t in range(3))
        value = jnp.where(layer == 3, u2, u0)
        value = jnp.where(layer < 2, lanes(jnp.where(layer == 2, u2, u0), 2), value)
        value = jnp.where(layer == 2, lanes(u1, 1), value)
        uf_s[8 * m : 8 * m + 8, :] = jnp.where(layer == 5, lanes(u1, -1), value)
    for n, kz, at in corners:
        x_s[at] = g3_s[216 * kz + 8 * n : 216 * kz + 8 * n + 8, :]
    corner_fill(x_s)
    slopes_at_points(x_s, j_s, a_s, b_s)
    sample_sizes(uf_s, size_s, a_s)
    energy = stress(j_s, size_s, g_s, p_s)
    points_to_corners(p_s, x_s, a_s, b_s)
    corner_fold(x_s)
    square = jnp.zeros((8, 128), jnp.float32)
    for n, kz, at in corners:
        grad = x_s[at]
        g3_s[216 * kz + 8 * n : 216 * kz + 8 * n + 8, :] = grad
        square = square + grad * grad
    own = jnp.abs(2 * layer - 5) < 4

    def own_sum(x):
        return jnp.sum(jnp.where(own, x, 0.0), axis=(0, 1), keepdims=True)

    square = own_sum(square)
    length = jnp.sqrt(1.0 + square * (1.0 / (512.0 * 81.0)))
    shorter = jnp.broadcast_to(1.0 / length, (8, 128))
    for n, kz, at in corners:
        x_s[at] = x_s[at] * shorter
    corner_fill(x_s)
    slopes_at_points(x_s, p_s, a_s, b_s)
    e2, e3, e4 = trial_terms(j_s, size_s, g_s, p_s)
    t_s[...] = jnp.zeros((128, 128), jnp.float32)
    length = jnp.broadcast_to(length, (8, 128))
    t_s[SUM_LANE:128, :] = length
    for n, total in enumerate((own_sum(energy), square, own_sum(e2), own_sum(e3), own_sum(e4))):
        t_s[SUM_LANE + n : SUM_LANE + 1 + n, :] = jnp.where(layer[0:1] == 1, total, length[0:1])
    for p in range(2):
        for j in range(4):
            for b in range(2):
                y = 2 * j + b
                first = uf_s[pl.ds(y, 27, stride=8), :] if p == 0 else g3_s[pl.ds(216 + y, 27, stride=8), :]
                t_s[pl.ds(b, 27, stride=2), :] = first
                t_s[pl.ds(64 + b, 27, stride=2), :] = g3_s[pl.ds(432 * p + y, 27, stride=8), :]
            back = t_s[...].T
            for i in range(8):
                for a in range(2):
                    to = (4 * i + j) * OUT_ROWS + 8 * p + 4 * a
                    at = (2 * i + a) * 8 + 1
                    out_ref[to : to + 4, :] = back[at : at + 4, :]


def unpack_kernel(in_ref, u_ref, g_ref, sums_ref, u_s, g_s):
    def part(p, a, layer):
        return in_ref[pl.ds(8 * p + 4 * a + layer, NXY, stride=OUT_ROWS), :]

    low = iota((NXY, 128), 1) < 64
    for layer in range(4):
        for a in range(2):
            u_s[pl.ds(128 * a + layer, NXY, stride=4), :] = part(0, a, layer)
        for kz in range(3):
            first, second = part((kz + 1) // 2, 0, layer), part((kz + 1) // 2, 1, layer)
            if kz == 1:
                both = jnp.where(low, first, lanes(second, 64))
            else:
                both = jnp.where(low, lanes(first, 64), second)
            g_s[pl.ds(3 * layer + kz, NXY, stride=12), :] = both
    lane = iota((NXY, 128), 1)
    length = jnp.where(lane < SUM_LANE, 1.0, part(0, 0, 1))
    longest = jnp.max(length, axis=0, keepdims=True)
    ratio = length / longest
    ratio2 = ratio * ratio
    power = jnp.where(lane < SUM_LANE + 3, ratio2, jnp.where(lane < SUM_LANE + 4, ratio2 * ratio, ratio2 * ratio2))
    power = jnp.where(lane < SUM_LANE + 2, 1.0, power)
    total = jnp.sum(part(0, 0, 0) * power, axis=0, keepdims=True)
    total = jnp.where(lane[0:1] < SUM_LANE + 5, total, longest)
    sums_ref[...] = jnp.broadcast_to(total[None], (NZ, 1, 128))
    for a in range(2):
        back = u_s[128 * a : 128 * a + 128, :].T
        for m in range(27):
            u_ref[m, a] = back[2 * m : 2 * m + 2, :]
    for n in range(3):
        back = g_s[128 * n : 128 * n + 128, :].T
        for a in range(2):
            for q in range(27):
                c, kx, ky = q // 9, (q // 3) % 3, q % 3
                for b in range(2):
                    at = 64 * a + 2 * q + b
                    g_ref[c, 3 * a + kx, ky + 3 * b : ky + 3 * b + 1, 128 * n : 128 * n + 128] = back[at : at + 1, :]


def checks_kernel(sums_ref, out_ref):
    sums = jnp.concatenate([sums_ref[n] for n in range(NZ)], axis=0)
    lane = iota((NZ, 128), 1)
    e0, square, e2, e3, e4, length = (
        jnp.sum(jnp.where(lane == SUM_LANE + n, sums, 0.0), axis=1, keepdims=True) for n in range(6)
    )
    e0 = jnp.sum(e0, axis=0, keepdims=True)
    square = jnp.sum(square, axis=0, keepdims=True)
    elements = float(512 * NXY * NZ)
    entries = 81.0 * elements
    step = trial_step / jnp.sqrt(1.0 + square / entries)
    x = step * length
    trial = e0 - step * square + jnp.sum(x * x * (e2 + x * (e3 + x * e4)), axis=0, keepdims=True)
    for n, value in enumerate((e0 / elements, square / entries, trial / elements)):
        out_ref[n] = value[0, 0]


def shape(*dims):
    return jax.ShapeDtypeStruct(dims, jnp.float32)


def on_chip(*dims):
    return pltpu.VMEM(dims, jnp.float32)


def keep(x):
    return pltpu.with_memory_space_constraint(x, pltpu.VMEM)


def vmem(*dims):
    return pltpu.VMEM(dims, jnp.float32)


MAIN_SCRATCH = [
    vmem(16 + NXY * IN_ROWS, 128),
    vmem(128, 128),
    vmem(128, 128),
    vmem(27 * 24, 128),
    vmem(3 * 24, 128),
    vmem(27 * 24, 128),
    vmem(12 * 24, 128),
    vmem(27 * 8, 128),
    vmem(81 * 8, 128),
    vmem(192, 8, 128),
    vmem(128, 8, 128),
    vmem(192, 8, 128),
    vmem(576, 8, 128),
    vmem(576, 8, 128),
    vmem(384, 8, 128),
    vmem(64, 8, 128),
]
SMEM = pl.BlockSpec(memory_space=pltpu.SMEM)
VMEM = pl.BlockSpec(memory_space=pltpu.VMEM)


def on_device(displacement, size_field_modes, velocity):
    at_z = lax.axis_index(GZ).reshape(1).astype(jnp.int32)
    tuv, tx, halo = pl.pallas_call(
        transpose_kernel,
        out_shape=(on_chip(128, 128), on_chip(384, 128), on_chip(NZ, HALO_ROWS, 128)),
        in_specs=[SMEM, VMEM, VMEM, VMEM],
        out_specs=(VMEM, VMEM, VMEM),
        scratch_shapes=[vmem(128, 128), vmem(128, 384)],
        name="transpose",
    )(at_z, size_field_modes, velocity, displacement)
    halo = lax.all_to_all(halo, GZ, 0, 0)
    packed = pl.pallas_call(
        pack_kernel,
        out_shape=on_chip(NXY * IN_ROWS, 128),
        in_specs=[SMEM, VMEM, VMEM, VMEM],
        out_specs=VMEM,
        scratch_shapes=[
            vmem(160, 128),
            vmem(408, 128),
            vmem(160, 128),
            vmem(408, 128),
            vmem(160, 128),
            vmem(160, 128),
        ],
        name="pack",
    )(at_z, keep(tuv), keep(tx), keep(halo))
    spread = lax.all_to_all(packed.reshape(NXY, IN_ROWS, 128), XY, 0, 0)
    result = pl.pallas_call(
        main_kernel,
        out_shape=on_chip(NXY * OUT_ROWS, 128),
        in_specs=[VMEM],
        out_specs=VMEM,
        scratch_shapes=MAIN_SCRATCH,
        name="remap_and_gradient",
    )(keep(spread.reshape(NXY * IN_ROWS, 128)))
    result = lax.all_to_all(result.reshape(NXY, OUT_ROWS, 128), XY, 0, 0)
    advected, gradient, sums = pl.pallas_call(
        unpack_kernel,
        out_shape=(shape(27, 2, 2, 128), shape(3, 6, 6, 384), on_chip(NZ, 1, 128)),
        in_specs=[VMEM],
        out_specs=(VMEM, VMEM, VMEM),
        scratch_shapes=[vmem(256, 128), vmem(384, 128)],
        name="unpack",
    )(keep(result.reshape(NXY * OUT_ROWS, 128)))
    sums = lax.all_to_all(sums, GZ, 0, 0)
    checks = pl.pallas_call(
        checks_kernel, out_shape=shape(3), in_specs=[VMEM], out_specs=SMEM, name="checks"
    )(keep(sums))
    return advected, gradient, checks


def solution(mesh):
    finer = Mesh(
        mesh.devices.reshape(4, 2, mesh.shape["gy"], 4, 2), ("gx_0", "gx_1", "gy", "gz_0", "gz_1")
    )
    return jax.shard_map(
        on_device,
        mesh=finer,
        in_specs=(P(None, GX, "gy", GZ), P(None, GX, "gy", GZ), P(None, GX, "gy", GZ)),
        out_specs=(P(None, GX, "gy", GZ), P(None, GX, "gy", GZ), P()),
        check_vma=False,
    )
```

```python
import jax
import jax.numpy as jnp
import numpy as np
from jax import lax
from jax.experimental import pallas as pl
from jax.experimental.pallas import tpu as pltpu
from jax.sharding import Mesh
from jax.sharding import PartitionSpec as P

SUBSTEPS = 4
GX = ("gx_0", "gx_1")
GZ = ("gz_0", "gz_1")
XY = ("gx_0", "gx_1", "gy")

NZ = 8
NXY = 32
HALO_ROWS = 16
IN_ROWS = 40
SUM_LANE = 120
OUT_ROWS = 16

p0 = 0.7071067811865476
p1 = 1.224744871391589
p2 = 1.5811388300841898
root3 = 1.7320508075688772
root15 = 3.872983346207417
courant = 0.1
theta_size = 0.3
trial_step = 0.05


def build_tables():
    points = np.array(
        [-0.8611363115940526, -0.3399810435848563, 0.3399810435848563, 0.8611363115940526]
    )
    weights = np.array(
        [0.3478548451374538, 0.6521451548625461, 0.6521451548625461, 0.3478548451374538]
    )
    points = 0.5 * (points + 1.0)
    weights = 0.5 * weights
    node_points = np.array([0.0, 1.0 / 3.0, 2.0 / 3.0, 1.0])
    value_table = np.zeros((4, 4))
    slope_table = np.zeros((4, 4))
    for column in range(4):
        others = [node_points[member] for member in range(4) if member != column]
        denominator = np.prod([node_points[column] - member for member in others])
        for quad_row in range(4):
            gauss_point = points[quad_row]
            value_table[quad_row, column] = (
                np.prod([gauss_point - member for member in others]) / denominator
            )
            slope_table[quad_row, column] = (
                sum(
                    np.prod(
                        [gauss_point - others[position] for position in range(3) if position != skipped]
                    )
                    for skipped in range(3)
                )
                / denominator
            )
    centred = 2.0 * points - 1.0
    legendre_table = np.stack(
        [
            np.full(4, p0),
            p1 * centred,
            p2 * 0.5 * (3.0 * centred**2 - 1.0),
        ],
        axis=1,
    )
    return value_table, slope_table, legendre_table, weights


VALUES, SLOPES, LEGENDRE, WEIGHTS = build_tables()


def iota(shape, dim):
    return lax.broadcasted_iota(jnp.int32, shape, dim)


def lanes(x, by):
    return pltpu.roll(x, (-by) % 128, x.ndim - 1)


def rows(x, by):
    return pltpu.roll(x, (-by) % 8, x.ndim - 2)


def following(x, d):
    return rows(x, 1) if d == 1 else lanes(x, 8 if d == 0 else 1)


def preceding(x, d):
    return rows(x, -1) if d == 1 else lanes(x, -8 if d == 0 else -1)


def following3(x, d):
    if d < 2:
        return following(x, d)
    return jnp.stack([x[1], x[2], lanes(x[0], 1)])


def preceding3(x, d):
    if d < 2:
        return preceding(x, d)
    return jnp.stack([lanes(x[2], -1), x[0], x[1]])


def halves(x):
    return (x[0] + x[3], x[1] + x[2], x[0] - x[3], x[1] - x[2])


def apply_table(table, sign, half):
    ea, eb, oa, ob = half
    out = [None] * 4
    for p in range(2):
        even = float(0.5 * (table[p, 0] + table[p, 3])) * ea + float(0.5 * (table[p, 1] + table[p, 2])) * eb
        odd = float(0.5 * (table[p, 0] - table[p, 3])) * oa + float(0.5 * (table[p, 1] - table[p, 2])) * ob
        out[p] = even + odd
        out[3 - p] = even - odd if sign > 0 else odd - even
    return out


def transpose_kernel(g_ref, u_ref, v_ref, x_ref, tuv_ref, tx_ref, halo_ref, uv_s, x_s):
    zero = jnp.zeros((16, 384), jnp.float32)
    for a in range(2):
        for m in range(27):
            uv_s[64 * a + 2 * m : 64 * a + 2 * m + 2, :] = u_ref[m, a]
        for d in range(3):
            uv_s[64 * a + 54 + 2 * d : 64 * a + 56 + 2 * d, :] = v_ref[d, a]
        uv_s[64 * a + 60 : 64 * a + 64, :] = zero[0:4, 0:128]
        at = 64 * (1 - a)
        for n in range(27):
            c, kx, ky = n // 9, (n // 3) % 3, n % 3
            for b in range(2):
                x_s[at + 2 * n + b : at + 2 * n + b + 1, :] = x_ref[c, 3 * a + kx, ky + 3 * b : ky + 3 * b + 1, :]
        x_s[at + 54 : at + 64, :] = zero[0:10]
    tuv_ref[...] = uv_s[...].T
    for n in range(3):
        tx_ref[128 * n : 128 * n + 128, :] = x_s[:, 128 * n : 128 * n + 128].T
    speed = jnp.abs(v_ref[0]) + jnp.abs(v_ref[1]) + jnp.abs(v_ref[2])
    speed = jnp.maximum(speed[0], speed[1])
    fastest = jnp.broadcast_to(jnp.max(speed, axis=(0, 1), keepdims=True), (1, 128))
    for n in range(NZ):
        halo_ref[n, :, :] = zero[0:16, 0:128]
        halo_ref[n, 13:14, :] = fastest
    up = lax.rem(g_ref[0] + 1, NZ)
    down = lax.rem(g_ref[0] + NZ - 1, NZ)
    halo_ref[up, 0:9, :] = tuv_ref[119:128, :]
    halo_ref[up, 9:12, :] = tx_ref[381:384, :]
    halo_ref[down, 0:9, :] = tuv_ref[0:9, :]
    halo_ref[down, 9:13, :] = tx_ref[0:4, :]


def pack_kernel(g_ref, tuv_ref, tx_ref, halo_ref, out_ref, uv_s, x_s, uv2_s, x2_s, plus_s, minus_s):
    below = lax.rem(g_ref[0] + NZ - 1, NZ)
    above = lax.rem(g_ref[0] + 1, NZ)
    uv_s[0:16, :] = jnp.zeros((16, 128), jnp.float32)
    uv_s[144:160, :] = jnp.zeros((16, 128), jnp.float32)
    x_s[0:8, :] = jnp.zeros((8, 128), jnp.float32)
    x_s[392:408, :] = jnp.zeros((16, 128), jnp.float32)
    uv_s[16:144, :] = tuv_ref[...]
    x_s[8:392, :] = tx_ref[...]
    uv_s[7:16, :] = halo_ref[below, 0:9, :]
    uv_s[144:153, :] = halo_ref[above, 0:9, :]
    x_s[5:8, :] = halo_ref[below, 9:12, :]
    x_s[392:396, :] = halo_ref[above, 9:13, :]
    uv = uv_s[...]
    uv2_s[...] = lanes(uv, 64)
    x2_s[...] = lanes(x_s[...], 64)
    lane = iota((160, 128), 1) & 63
    along_z = (lane >> 1) % 3
    even = uv + (p2 / p0) * lanes(uv, 4)
    odd = (p1 / p0) * lanes(uv, 2)
    field = lane < 54
    plus_s[...] = jnp.where(field, jnp.where(along_z == 0, even + odd, 0.0), jnp.where(lane >= 58, uv, 0.0))
    minus = lanes(even - odd, -2)
    minus_s[...] = jnp.where(field, jnp.where(along_z == 1, minus, 0.0), jnp.where(lane < 56, lanes(uv, 4), 0.0))
    fastest = halo_ref[0, 13:14, :]
    for n in range(1, NZ):
        fastest = jnp.maximum(fastest, halo_ref[n, 13:14, :])
    lane, row = iota((20, 128), 1), iota((20, 128), 0)
    at_speed = jnp.where(row == 0, lane, 0) >= SUM_LANE
    for k in range(NXY):
        at = IN_ROWS * k
        uv, x = pl.ds(4 * k + 8, 20), pl.ds(12 * k + 5, 20)
        first = jnp.where(lane < 64, uv_s[uv, :], x_s[x, :])
        out_ref[at : at + 20, :] = jnp.where(at_speed, fastest, first)
        out_ref[at + 20 : at + 40, :] = jnp.where(lane < 64, uv2_s[uv, :], x2_s[x, :])
    outer = plus_s[pl.ds(7, NXY, stride=4), :] + minus_s[pl.ds(28, NXY, stride=4), :]
    low = iota((NXY, 128), 1) < 64
    last = pl.ds(27, NXY, stride=4)
    out_ref[pl.ds(19, NXY, stride=IN_ROWS), :] = jnp.where(low, uv_s[last, :], lanes(outer, 64))
    out_ref[pl.ds(39, NXY, stride=IN_ROWS), :] = jnp.where(low, uv2_s[last, :], outer)


def corner_fill(ref):
    def one(c, carry):
        at = c * 64
        for kx in range(3):
            for ky in range(3):
                ref[at + kx * 16 + ky * 4 + 3] = following(ref[at + kx * 16 + ky * 4], 2)
        for ky in range(3):
            for kz in range(4):
                ref[at + 48 + ky * 4 + kz] = following(ref[at + ky * 4 + kz], 0)
        for kx in range(4):
            for kz in range(4):
                ref[at + kx * 16 + 12 + kz] = following(ref[at + kx * 16 + kz], 1)
        return carry

    lax.fori_loop(0, 3, one, 0)


def corner_fold(ref):
    def one(c, carry):
        at = c * 64
        for kx in range(4):
            for kz in range(4):
                n = at + kx * 16 + kz
                ref[n] = ref[n] + preceding(ref[n + 12], 1)
        for ky in range(3):
            for kz in range(4):
                n = at + ky * 4 + kz
                ref[n] = ref[n] + preceding(ref[n + 48], 0)
        for kx in range(3):
            for ky in range(3):
                n = at + kx * 16 + ky * 4
                ref[n] = ref[n] + preceding(ref[n + 3], 2)
        return carry

    lax.fori_loop(0, 3, one, 0)


def parts(x):
    ea, eb = x[0] + x[3], x[1] + x[2]
    return ea - eb, 0.5 * eb, x[0] - x[3], x[1] - x[2]


def values_of(part):
    d, half, oa, ob = part
    out = [None] * 4
    for p in range(2):
        even = float(0.5 * (VALUES[p, 0] + VALUES[p, 3])) * d + half
        odd = float(0.5 * (VALUES[p, 0] - VALUES[p, 3])) * oa + float(0.5 * (VALUES[p, 1] - VALUES[p, 2])) * ob
        out[p], out[3 - p] = even + odd, even - odd
    return out


def slopes_of(part):
    d, _, oa, ob = part
    out = [None] * 4
    for p in range(2):
        even = float(0.5 * (SLOPES[p, 0] + SLOPES[p, 3])) * d
        odd = float(0.5 * (SLOPES[p, 0] - SLOPES[p, 3])) * oa + float(0.5 * (SLOPES[p, 1] - SLOPES[p, 2])) * ob
        out[p], out[3 - p] = even + odd, odd - even
    return out


def both_back(v, s):
    (va, vb, wa, wb), (sa, sb, ta, tb) = halves(v), halves(s)
    out = [None] * 4
    for k in range(2):
        first = float(0.5 * (VALUES[0, k] + VALUES[3, k])) * va + float(0.5 * (VALUES[1, k] + VALUES[2, k])) * vb
        first = first + float(0.5 * (SLOPES[0, k] - SLOPES[3, k])) * ta + float(0.5 * (SLOPES[1, k] - SLOPES[2, k])) * tb
        second = float(0.5 * (VALUES[0, k] - VALUES[3, k])) * wa + float(0.5 * (VALUES[1, k] - VALUES[2, k])) * wb
        second = second + float(0.5 * (SLOPES[0, k] + SLOPES[3, k])) * sa + float(0.5 * (SLOPES[1, k] + SLOPES[2, k])) * sb
        out[k], out[3 - k] = first + second, first - second
    return out


def slopes_at_points(src, dst, a_s, b_s):
    def one(c, carry):
        at = c * 64
        for line in range(16):
            part = parts([src[at + k * 16 + line] for k in range(4)])
            v, s = values_of(part), slopes_of(part)
            for p in range(4):
                a_s[p * 16 + line] = v[p]
                a_s[64 + p * 16 + line] = s[p]
        for p in range(4):
            for kz in range(4):
                pv = parts([a_s[p * 16 + k * 4 + kz] for k in range(4)])
                ps = parts([a_s[64 + p * 16 + k * 4 + kz] for k in range(4)])
                sv, vs, vv = values_of(ps), slopes_of(pv), values_of(pv)
                for r in range(4):
                    b_s[p * 16 + r * 4 + kz] = sv[r]
                    b_s[64 + p * 16 + r * 4 + kz] = vs[r]
                    b_s[128 + p * 16 + r * 4 + kz] = vv[r]
        for pr in range(16):
            for col in range(3):
                part = parts([b_s[64 * col + pr * 4 + k] for k in range(4)])
                out = slopes_of(part) if col == 2 else values_of(part)
                for t in range(4):
                    dst[c * 192 + 64 * col + pr * 4 + t] = out[t]
        return carry

    lax.fori_loop(0, 3, one, 0)


def points_to_corners(src, dst, a_s, b_s):
    values_t, slopes_t = VALUES.T, SLOPES.T

    def one(c, carry):
        at = c * 64
        for pr in range(16):
            for col in range(3):
                h = halves([src[c * 192 + 64 * col + pr * 4 + t] for t in range(4)])
                out = apply_table(slopes_t, -1, h) if col == 2 else apply_table(values_t, 1, h)
                for k in range(4):
                    b_s[64 * col + pr * 4 + k] = out[k]
        for p in range(4):
            for kz in range(4):
                sv = apply_table(values_t, 1, halves([b_s[p * 16 + r * 4 + kz] for r in range(4)]))
                vs = [b_s[64 + p * 16 + r * 4 + kz] for r in range(4)]
                v = both_back([b_s[128 + p * 16 + r * 4 + kz] for r in range(4)], vs)
                for k in range(4):
                    a_s[p * 16 + k * 4 + kz] = v[k]
                    a_s[64 + p * 16 + k * 4 + kz] = sv[k]
        for line in range(16):
            out = both_back([a_s[p * 16 + line] for p in range(4)], [a_s[64 + p * 16 + line] for p in range(4)])
            for k in range(4):
                dst[at + k * 16 + line] = out[k]
        return carry

    lax.fori_loop(0, 3, one, 0)


def legendre_line(u):
    base = p0 * u[0]
    out = [None] * 4
    for p in range(2):
        even = base + float(LEGENDRE[p, 2]) * u[2]
        odd = float(LEGENDRE[p, 1]) * u[1]
        out[p] = even + odd
        out[3 - p] = even - odd
    return out


def sample_sizes(u_s, size_s, a_s):
    for bc in range(9):
        out = legendre_line([u_s[8 * (a * 9 + bc) : 8 * (a * 9 + bc) + 8, :] for a in range(3)])
        for p in range(4):
            a_s[p * 9 + bc] = out[p]
    for p in range(4):
        grid = [[None] * 3 for _ in range(4)]
        for c in range(3):
            out = legendre_line([a_s[p * 9 + b * 3 + c] for b in range(3)])
            for r in range(4):
                grid[r][c] = out[r]
        for r in range(4):
            out = legendre_line(grid[r])
            for t in range(4):
                size_s[p * 16 + r * 4 + t] = jnp.exp(theta_size * out[t])


PAIRS = ((0, 0), (1, 1), (2, 2), (0, 1), (0, 2), (1, 2))
AT = {pair: n for n, pair in enumerate(PAIRS)} | {(b, a): n for n, (a, b) in enumerate(PAIRS)}


def dot3(x, y, at):
    return x[at] * y[at] + x[at + 1] * y[at + 1] + x[at + 2] * y[at + 2]


def dot6(x, y):
    return dot3(x, y, 0) + 2.0 * dot3(x, y, 3)


def weight_of(pr):
    def w(k):
        return jnp.where((k == 0) | (k == 3), jnp.float32(WEIGHTS[0]), jnp.float32(WEIGHTS[1]))

    return w(pr >> 2) * w(pr & 3)


def jacobian(j_s, q):
    return [[j_s[c * 192 + col * 64 + q] for col in range(3)] for c in range(3)]


def stress(j_s, size_s, g_s, p_s):
    def one(pr, energy):
        pair_weight = weight_of(pr)
        for t in range(4):
            q = pr * 4 + t
            jac = jacobian(j_s, q)
            for c in range(3):
                jac[c][c] = jac[c][c] + 1.0
                j_s[c * 192 + c * 64 + q] = jac[c][c]
            size = size_s[q]
            inverse = 1.0 / size
            inverse2 = inverse * inverse
            weighted = (pair_weight * float(WEIGHTS[t])) * size
            dev = []
            for n, (a, b) in enumerate(PAIRS):
                gram = (jac[0][a] * jac[0][b] + jac[1][a] * jac[1][b] + jac[2][a] * jac[2][b]) * inverse2
                dev.append(gram - 1.0 if a == b else gram)
                g_s[n * 64 + q] = dev[n]
            energy = energy + weighted * size * size * dot6(dev, dev)
            scaled = [4.0 * weighted * d for d in dev]
            for c in range(3):
                for col in range(3):
                    p_s[c * 192 + col * 64 + q] = (
                        jac[c][0] * scaled[AT[0, col]]
                        + jac[c][1] * scaled[AT[1, col]]
                        + jac[c][2] * scaled[AT[2, col]]
                    )
        return energy

    return lax.fori_loop(0, 16, one, jnp.zeros((8, 128), jnp.float32))


def trial_terms(j_s, size_s, g_s, d_s):
    def one(pr, sums):
        e2, e3, e4 = sums
        pair_weight = weight_of(pr)
        for t in range(4):
            q = pr * 4 + t
            jac = jacobian(j_s, q)
            der = jacobian(d_s, q)
            size = size_s[q]
            point_weight = pair_weight * float(WEIGHTS[t])
            dev, first, second = [], [], []
            for n, (a, b) in enumerate(PAIRS):
                dev.append(g_s[n * 64 + q])
                cross = jac[0][a] * der[0][b] + jac[1][a] * der[1][b] + jac[2][a] * der[2][b]
                if a != b:
                    cross = cross + (jac[0][b] * der[0][a] + jac[1][b] * der[1][a] + jac[2][b] * der[2][a])
                first.append(cross)
                second.append(der[0][a] * der[0][b] + der[1][a] * der[1][b] + der[2][a] * der[2][b])
            square = 2.0 * dot3(first, first, 0) + dot3(first, first, 3)
            mixed = dot3(first, second, 0) + dot3(first, second, 3)
            low, high = point_weight * size, point_weight / size
            e2 = e2 + (high * square + low * dot6(dev, second))
            e3 = e3 + high * mixed
            e4 = e4 + high * dot6(second, second)
        return e2, e3, e4

    zero = jnp.zeros((8, 128), jnp.float32)
    e2, e3, e4 = lax.fori_loop(0, 16, one, (zero, zero, zero))
    return 2.0 * e2, -4.0 * e3, e4


def remap(u_s, v_s, mid_s, face_s, time_step):
    def mode(ref, m):
        return ref[24 * m : 24 * m + 24, :].reshape(3, 8, 128)

    def put(ref, m, value):
        ref[24 * m : 24 * m + 24, :] = value.reshape(24, 128)

    for d in range(3):
        v = mode(v_s, d)
        face = 0.5 * (v + following3(v, d))
        put(face_s, 4 * d, 2.0 * time_step * jnp.maximum(face, 0.0))
        put(face_s, 4 * d + 1, 2.0 * time_step * jnp.minimum(face, 0.0))
        put(face_s, 4 * d + 2, (2.0 * root3) * time_step * v)
        put(face_s, 4 * d + 3, (2.0 * root15) * time_step * v)

    def terms(src, d, m, step):
        u0, u1, u2 = mode(src, m), mode(src, m + step), mode(src, m + 2 * step)
        even = p0 * u0 + p2 * u2
        odd = p1 * u1
        flux = mode(face_s, 4 * d) * (even + odd) + mode(face_s, 4 * d + 1) * following3(even - odd, d)
        before = preceding3(flux, d)
        jump = before - flux
        return (
            p0 * jump,
            mode(face_s, 4 * d + 2) * u0 - p1 * (flux + before),
            mode(face_s, 4 * d + 3) * u1 + p2 * jump,
        )

    dims = (
        (0, 9, range(9)),
        (1, 3, (0, 1, 2, 9, 10, 11, 18, 19, 20)),
        (2, 1, range(0, 27, 3)),
    )

    def substep(_, carry):
        for d, step, starts in dims:
            for m in starts:
                for n, term in enumerate(terms(u_s, d, m, step)):
                    at = m + n * step
                    put(mid_s, at, mode(u_s if d == 0 else mid_s, at) + term)
        for d, step, starts in dims:
            for m in starts:
                for n, term in enumerate(terms(mid_s, d, m, step)):
                    at = m + n * step
                    old = 0.5 * (mode(u_s, at) + mode(mid_s, at)) if d == 0 else mode(u_s, at)
                    put(u_s, at, old + 0.5 * term)
        return carry

    lax.fori_loop(0, SUBSTEPS, substep, 0)


def main_kernel(
    in_ref, out_ref, in_s, outer_s, t_s, u_s, v_s, mid_s, face_s, uf_s, g3_s, x_s, a_s, b_s, j_s, p_s, g_s, size_s
):
    corners = [(n, kz, (n // 9) * 64 + ((n // 3) % 3) * 16 + (n % 3) * 4 + kz) for n in range(27) for kz in range(3)]
    in_s[0:8, :] = jnp.zeros((8, 128), jnp.float32)
    in_s[8 : 8 + NXY * IN_ROWS, :] = in_ref[...]
    in_s[8 + NXY * IN_ROWS : 16 + NXY * IN_ROWS, :] = jnp.zeros((8, 128), jnp.float32)
    outer = lanes(in_ref[pl.ds(19, 2 * NXY, stride=20), :], 64)
    lane = iota((2 * NXY, 128), 1)
    trace = jnp.where(lane < 54, (lane >> 1) % 3, 1) == 0
    speed = jnp.abs(2 * lane - 117) < 2
    outer_s[0:64, :] = jnp.where(trace, outer, jnp.where(speed, outer, 0.0))
    outer_s[64:128, :] = jnp.where(trace, lanes(outer, 2), jnp.where(speed, lanes(outer, -4), 0.0))
    row = iota((8, 128), 0)
    for t in range(3):
        for j in range(4):
            stacked = []
            for i in range(8):
                for a in range(2):
                    n = 2 * (4 * i + j) + a
                    block = in_s[pl.ds(8 + 20 * n + t - 1, 8, stride=3), :]
                    if t == 0:
                        block = jnp.where(row == 0, outer_s[n : n + 1, :], block)
                        block = jnp.where(row == 7, outer_s[64 + n : 65 + n, :], block)
                    stacked.append(block)
            t_s[...] = jnp.concatenate(stacked, axis=0).T
            for b in range(2):
                y = 2 * j + b
                u_s[pl.ds(8 * t + y, 27, stride=24), :] = t_s[pl.ds(b, 27, stride=2), :]
                v_s[pl.ds(8 * t + y, 3, stride=24), :] = t_s[pl.ds(54 + b, 3, stride=2), :]
                nodes = t_s[pl.ds(64 + b, 27, stride=2), :]
                if t == 0:
                    nodes = lanes(nodes, 1)
                g3_s[pl.ds(216 * ((t + 2) % 3) + y, 27, stride=8), :] = nodes
    lane = iota((8, 128), 1)
    fastest = jnp.max(in_ref[pl.ds(0, NXY, stride=IN_ROWS), :], axis=0, keepdims=True)
    fastest = jnp.where(iota((1, 128), 1) < SUM_LANE, 0.0, fastest)
    fastest = jnp.broadcast_to(jnp.max(fastest, axis=1, keepdims=True), (8, 128))
    remap(u_s, v_s, mid_s, face_s, courant / jnp.maximum(fastest, 0.25))

    layer = lane & 7
    for m in range(27):
        u0, u1, u2 = (u_s[24 * m + 8 * t : 24 * m + 8 * t + 8, :] for t in range(3))
        value = jnp.where(layer == 3, u2, u0)
        value = jnp.where(layer < 2, lanes(jnp.where(layer == 2, u2, u0), 2), value)
        value = jnp.where(layer == 2, lanes(u1, 1), value)
        uf_s[8 * m : 8 * m + 8, :] = jnp.where(layer == 5, lanes(u1, -1), value)
    for n, kz, at in corners:
        x_s[at] = g3_s[216 * kz + 8 * n : 216 * kz + 8 * n + 8, :]
    corner_fill(x_s)
    slopes_at_points(x_s, j_s, a_s, b_s)
    sample_sizes(uf_s, size_s, a_s)
    energy = stress(j_s, size_s, g_s, p_s)
    points_to_corners(p_s, x_s, a_s, b_s)
    corner_fold(x_s)
    square = jnp.zeros((8, 128), jnp.float32)
    for n, kz, at in corners:
        grad = x_s[at]
        g3_s[216 * kz + 8 * n : 216 * kz + 8 * n + 8, :] = grad
        square = square + grad * grad
    own = jnp.abs(2 * layer - 5) < 4

    def own_sum(x):
        return jnp.sum(jnp.where(own, x, 0.0), axis=(0, 1), keepdims=True)

    square = own_sum(square)
    length = jnp.sqrt(1.0 + square * (1.0 / (512.0 * 81.0)))
    shorter = jnp.broadcast_to(1.0 / length, (8, 128))
    for n, kz, at in corners:
        x_s[at] = x_s[at] * shorter
    corner_fill(x_s)
    slopes_at_points(x_s, p_s, a_s, b_s)
    e2, e3, e4 = trial_terms(j_s, size_s, g_s, p_s)
    t_s[...] = jnp.zeros((128, 128), jnp.float32)
    length = jnp.broadcast_to(length, (8, 128))
    t_s[SUM_LANE:128, :] = length
    for n, total in enumerate((own_sum(energy), square, own_sum(e2), own_sum(e3), own_sum(e4))):
        t_s[SUM_LANE + n : SUM_LANE + 1 + n, :] = jnp.where(layer[0:1] == 1, total, length[0:1])
    for p in range(2):
        for j in range(4):
            for b in range(2):
                y = 2 * j + b
                first = uf_s[pl.ds(y, 27, stride=8), :] if p == 0 else g3_s[pl.ds(216 + y, 27, stride=8), :]
                t_s[pl.ds(b, 27, stride=2), :] = first
                t_s[pl.ds(64 + b, 27, stride=2), :] = g3_s[pl.ds(432 * p + y, 27, stride=8), :]
            back = t_s[...].T
            for i in range(8):
                for a in range(2):
                    to = (4 * i + j) * OUT_ROWS + 8 * p + 4 * a
                    at = (2 * i + a) * 8 + 1
                    out_ref[to : to + 4, :] = back[at : at + 4, :]


def unpack_kernel(in_ref, u_ref, g_ref, sums_ref, u_s, g_s):
    def part(p, a, layer):
        return in_ref[pl.ds(8 * p + 4 * a + layer, NXY, stride=OUT_ROWS), :]

    low = iota((NXY, 128), 1) < 64
    for layer in range(4):
        for a in range(2):
            u_s[pl.ds(128 * a + layer, NXY, stride=4), :] = part(0, a, layer)
        for kz in range(3):
            first, second = part((kz + 1) // 2, 0, layer), part((kz + 1) // 2, 1, layer)
            if kz == 1:
                both = jnp.where(low, first, lanes(second, 64))
            else:
                both = jnp.where(low, lanes(first, 64), second)
            g_s[pl.ds(3 * layer + kz, NXY, stride=12), :] = both
    lane = iota((NXY, 128), 1)
    length = jnp.where(lane < SUM_LANE, 1.0, part(0, 0, 1))
    longest = jnp.max(length, axis=0, keepdims=True)
    ratio = length / longest
    ratio2 = ratio * ratio
    power = jnp.where(lane < SUM_LANE + 3, ratio2, jnp.where(lane < SUM_LANE + 4, ratio2 * ratio, ratio2 * ratio2))
    power = jnp.where(lane < SUM_LANE + 2, 1.0, power)
    total = jnp.sum(part(0, 0, 0) * power, axis=0, keepdims=True)
    total = jnp.where(lane[0:1] < SUM_LANE + 5, total, longest)
    sums_ref[...] = jnp.broadcast_to(total[None], (NZ, 1, 128))
    for a in range(2):
        back = u_s[128 * a : 128 * a + 128, :].T
        for m in range(27):
            u_ref[m, a] = back[2 * m : 2 * m + 2, :]
    for n in range(3):
        back = g_s[128 * n : 128 * n + 128, :].T
        for a in range(2):
            for q in range(27):
                c, kx, ky = q // 9, (q // 3) % 3, q % 3
                for b in range(2):
                    at = 64 * a + 2 * q + b
                    g_ref[c, 3 * a + kx, ky + 3 * b : ky + 3 * b + 1, 128 * n : 128 * n + 128] = back[at : at + 1, :]


def checks_kernel(sums_ref, out_ref):
    sums = jnp.concatenate([sums_ref[n] for n in range(NZ)], axis=0)
    lane = iota((NZ, 128), 1)
    e0, square, e2, e3, e4, length = (
        jnp.sum(jnp.where(lane == SUM_LANE + n, sums, 0.0), axis=1, keepdims=True) for n in range(6)
    )
    e0 = jnp.sum(e0, axis=0, keepdims=True)
    square = jnp.sum(square, axis=0, keepdims=True)
    elements = float(512 * NXY * NZ)
    entries = 81.0 * elements
    step = trial_step / jnp.sqrt(1.0 + square / entries)
    x = step * length
    trial = e0 - step * square + jnp.sum(x * x * (e2 + x * (e3 + x * e4)), axis=0, keepdims=True)
    for n, value in enumerate((e0 / elements, square / entries, trial / elements)):
        out_ref[n] = value[0, 0]


def shape(*dims):
    return jax.ShapeDtypeStruct(dims, jnp.float32)


def on_chip(*dims):
    return pltpu.VMEM(dims, jnp.float32)


def keep(x):
    return pltpu.with_memory_space_constraint(x, pltpu.VMEM)


def vmem(*dims):
    return pltpu.VMEM(dims, jnp.float32)


MAIN_SCRATCH = [
    vmem(16 + NXY * IN_ROWS, 128),
    vmem(128, 128),
    vmem(128, 128),
    vmem(27 * 24, 128),
    vmem(3 * 24, 128),
    vmem(27 * 24, 128),
    vmem(12 * 24, 128),
    vmem(27 * 8, 128),
    vmem(81 * 8, 128),
    vmem(192, 8, 128),
    vmem(128, 8, 128),
    vmem(192, 8, 128),
    vmem(576, 8, 128),
    vmem(576, 8, 128),
    vmem(384, 8, 128),
    vmem(64, 8, 128),
]
SMEM = pl.BlockSpec(memory_space=pltpu.SMEM)
VMEM = pl.BlockSpec(memory_space=pltpu.VMEM)


def near_groups():
    groups = []
    for z in range(4):
        for core in range(2):
            for x in range(4):
                group = []
                for y in range(4):
                    for half in range(2):
                        at = z if half == 0 else 3 - z
                        group.append((((at * 2 + core) * 4 + x) * 4 + y) * 2 + half)
                groups.append(group)
    return groups


def on_device(displacement, size_field_modes, velocity):
    at_z = lax.axis_index(GZ).reshape(1).astype(jnp.int32)
    tuv, tx, halo = pl.pallas_call(
        transpose_kernel,
        out_shape=(on_chip(128, 128), on_chip(384, 128), on_chip(NZ, HALO_ROWS, 128)),
        in_specs=[SMEM, VMEM, VMEM, VMEM],
        out_specs=(VMEM, VMEM, VMEM),
        scratch_shapes=[vmem(128, 128), vmem(128, 384)],
        name="transpose",
    )(at_z, size_field_modes, velocity, displacement)
    halo = lax.all_to_all(halo, GZ, 0, 0)
    packed = pl.pallas_call(
        pack_kernel,
        out_shape=on_chip(NXY * IN_ROWS, 128),
        in_specs=[SMEM, VMEM, VMEM, VMEM],
        out_specs=VMEM,
        scratch_shapes=[
            vmem(160, 128),
            vmem(408, 128),
            vmem(160, 128),
            vmem(408, 128),
            vmem(160, 128),
            vmem(160, 128),
        ],
        name="pack",
    )(at_z, keep(tuv), keep(tx), keep(halo))
    spread = lax.all_to_all(packed.reshape(NXY, IN_ROWS, 128), XY, 0, 0)
    result = pl.pallas_call(
        main_kernel,
        out_shape=on_chip(NXY * OUT_ROWS, 128),
        in_specs=[VMEM],
        out_specs=VMEM,
        scratch_shapes=MAIN_SCRATCH,
        name="remap_and_gradient",
    )(keep(spread.reshape(NXY * IN_ROWS, 128)))
    result = lax.all_to_all(result.reshape(NXY, OUT_ROWS, 128), XY, 0, 0)
    advected, gradient, sums = pl.pallas_call(
        unpack_kernel,
        out_shape=(shape(27, 2, 2, 128), shape(3, 6, 6, 384), on_chip(NZ, 1, 128)),
        in_specs=[VMEM],
        out_specs=(VMEM, VMEM, VMEM),
        scratch_shapes=[vmem(256, 128), vmem(384, 128)],
        name="unpack",
    )(keep(result.reshape(NXY * OUT_ROWS, 128)))
    sums = lax.all_to_all(sums, XY + GZ, 0, 0, axis_index_groups=near_groups())
    checks = pl.pallas_call(
        checks_kernel, out_shape=shape(3), in_specs=[VMEM], out_specs=SMEM, name="checks"
    )(keep(sums))
    return advected, gradient, checks


def solution(mesh):
    finer = Mesh(
        mesh.devices.reshape(4, 2, mesh.shape["gy"], 4, 2), ("gx_0", "gx_1", "gy", "gz_0", "gz_1")
    )
    return jax.shard_map(
        on_device,
        mesh=finer,
        in_specs=(P(None, GX, "gy", GZ), P(None, GX, "gy", GZ), P(None, GX, "gy", GZ)),
        out_specs=(P(None, GX, "gy", GZ), P(None, GX, "gy", GZ), P()),
        check_vma=False,
    )
```

```python
from functools import partial

import jax
import jax.numpy as jnp
import numpy as np
from jax import lax
from jax.experimental import pallas as pl
from jax.experimental.pallas import tpu as pltpu
from jax.sharding import Mesh
from jax.sharding import PartitionSpec as P

SUBSTEPS = 4
GX = ("gx_0", "gx_1")
GZ = ("gz_0", "gz_1")
XY = ("gx_0", "gx_1", "gy")

NZ = 8
NXY = 32
HALO_ROWS = 16
IN_ROWS = 40
SUM_LANE = 120
FAR_SENDER = (2, 3, 0, 1)
OUT_ROWS = 16

p0 = 0.7071067811865476
p1 = 1.224744871391589
p2 = 1.5811388300841898
SCALES = [a * b * c for a in (p0, p1, p2) for b in (p0, p1, p2) for c in (p0, p1, p2)]
courant = 0.1
theta_size = 0.3
trial_step = 0.05


def build_tables():
    points = np.array(
        [-0.8611363115940526, -0.3399810435848563, 0.3399810435848563, 0.8611363115940526]
    )
    weights = np.array(
        [0.3478548451374538, 0.6521451548625461, 0.6521451548625461, 0.3478548451374538]
    )
    points = 0.5 * (points + 1.0)
    weights = 0.5 * weights
    node_points = np.array([0.0, 1.0 / 3.0, 2.0 / 3.0, 1.0])
    value_table = np.zeros((4, 4))
    slope_table = np.zeros((4, 4))
    for column in range(4):
        others = [node_points[member] for member in range(4) if member != column]
        denominator = np.prod([node_points[column] - member for member in others])
        for quad_row in range(4):
            gauss_point = points[quad_row]
            value_table[quad_row, column] = (
                np.prod([gauss_point - member for member in others]) / denominator
            )
            slope_table[quad_row, column] = (
                sum(
                    np.prod(
                        [gauss_point - others[position] for position in range(3) if position != skipped]
                    )
                    for skipped in range(3)
                )
                / denominator
            )
    centred = 2.0 * points - 1.0
    legendre_table = np.stack(
        [
            np.full(4, p0),
            p1 * centred,
            p2 * 0.5 * (3.0 * centred**2 - 1.0),
        ],
        axis=1,
    )
    return value_table, slope_table, legendre_table, weights


VALUES, SLOPES, LEGENDRE, WEIGHTS = build_tables()


def iota(shape, dim):
    return lax.broadcasted_iota(jnp.int32, shape, dim)


def lanes(x, by):
    return pltpu.roll(x, (-by) % 128, x.ndim - 1)


def rows(x, by):
    return pltpu.roll(x, (-by) % 8, x.ndim - 2)


def following(x, d):
    return rows(x, 1) if d == 1 else lanes(x, 8 if d == 0 else 1)


def preceding(x, d):
    return rows(x, -1) if d == 1 else lanes(x, -8 if d == 0 else -1)


def following3(x, d):
    if d < 2:
        return following(x, d)
    return jnp.stack([x[1], x[2], lanes(x[0], 1)])


def preceding3(x, d):
    if d < 2:
        return preceding(x, d)
    return jnp.stack([lanes(x[2], -1), x[0], x[1]])


def halves(x):
    return (x[0] + x[3], x[1] + x[2], x[0] - x[3], x[1] - x[2])


def apply_table(table, sign, half):
    ea, eb, oa, ob = half
    out = [None] * 4
    for p in range(2):
        even = float(0.5 * (table[p, 0] + table[p, 3])) * ea + float(0.5 * (table[p, 1] + table[p, 2])) * eb
        odd = float(0.5 * (table[p, 0] - table[p, 3])) * oa + float(0.5 * (table[p, 1] - table[p, 2])) * ob
        out[p] = even + odd
        out[3 - p] = even - odd if sign > 0 else odd - even
    return out


def transpose_kernel(g_ref, u_ref, v_ref, x_ref, tuv_ref, tx_ref, halo_ref, uv_s, x_s):
    zero = jnp.zeros((16, 384), jnp.float32)
    for a in range(2):
        for m in range(27):
            uv_s[64 * a + 2 * m : 64 * a + 2 * m + 2, :] = SCALES[m] * u_ref[m, a]
        for d in range(3):
            uv_s[64 * a + 54 + 2 * d : 64 * a + 56 + 2 * d, :] = v_ref[d, a]
        uv_s[64 * a + 60 : 64 * a + 64, :] = zero[0:4, 0:128]
        at = 64 * (1 - a)
        for n in range(27):
            c, kx, ky = n // 9, (n // 3) % 3, n % 3
            for b in range(2):
                x_s[at + 2 * n + b : at + 2 * n + b + 1, :] = x_ref[c, 3 * a + kx, ky + 3 * b : ky + 3 * b + 1, :]
        x_s[at + 54 : at + 64, :] = zero[0:10]
    tuv_ref[...] = uv_s[...].T
    for n in range(3):
        tx_ref[128 * n : 128 * n + 128, :] = x_s[:, 128 * n : 128 * n + 128].T
    speed = jnp.abs(v_ref[0]) + jnp.abs(v_ref[1]) + jnp.abs(v_ref[2])
    speed = jnp.maximum(speed[0], speed[1])
    fastest = jnp.broadcast_to(jnp.max(speed, axis=(0, 1), keepdims=True), (1, 128))
    for n in range(NZ):
        halo_ref[n, :, :] = zero[0:16, 0:128]
        halo_ref[n, 13:14, :] = fastest
    at_z = lax.rem(g_ref[0], NZ)
    up = lax.rem(at_z + 1, NZ)
    down = lax.rem(at_z + NZ - 1, NZ)
    halo_ref[up, 0:9, :] = tuv_ref[119:128, :]
    halo_ref[up, 9:12, :] = tx_ref[381:384, :]
    halo_ref[down, 0:9, :] = tuv_ref[0:9, :]
    halo_ref[down, 9:13, :] = tx_ref[0:4, :]


def pack_kernel(g_ref, tuv_ref, tx_ref, halo_ref, out_ref, uv_s, x_s, uv2_s, x2_s, plus_s, minus_s):
    at_z = lax.rem(g_ref[0], NZ)
    below = lax.rem(at_z + NZ - 1, NZ)
    above = lax.rem(at_z + 1, NZ)
    uv_s[0:16, :] = jnp.zeros((16, 128), jnp.float32)
    uv_s[144:160, :] = jnp.zeros((16, 128), jnp.float32)
    x_s[0:8, :] = jnp.zeros((8, 128), jnp.float32)
    x_s[392:408, :] = jnp.zeros((16, 128), jnp.float32)
    uv_s[16:144, :] = tuv_ref[...]
    x_s[8:392, :] = tx_ref[...]
    uv_s[7:16, :] = halo_ref[below, 0:9, :]
    uv_s[144:153, :] = halo_ref[above, 0:9, :]
    x_s[5:8, :] = halo_ref[below, 9:12, :]
    x_s[392:396, :] = halo_ref[above, 9:13, :]
    uv = uv_s[...]
    uv2_s[...] = lanes(uv, 64)
    x2_s[...] = lanes(x_s[...], 64)
    lane = iota((160, 128), 1) & 63
    along_z = (lane >> 1) % 3
    even = uv + lanes(uv, 4)
    odd = lanes(uv, 2)
    field = lane < 54
    plus_s[...] = jnp.where(field, jnp.where(along_z == 0, even + odd, 0.0), jnp.where(lane >= 58, uv, 0.0))
    minus = lanes(even - odd, -2)
    minus_s[...] = jnp.where(field, jnp.where(along_z == 1, minus, 0.0), jnp.where(lane < 56, lanes(uv, 4), 0.0))
    fastest = halo_ref[0, 13:14, :]
    for n in range(1, NZ):
        fastest = jnp.maximum(fastest, halo_ref[n, 13:14, :])
    lane, row = iota((20, 128), 1), iota((20, 128), 0)
    at_speed = jnp.where(row == 0, lane, 0) >= SUM_LANE
    for k in range(NXY):
        at = IN_ROWS * k
        uv, x = pl.ds(4 * k + 8, 20), pl.ds(12 * k + 5, 20)
        first = jnp.where(lane < 64, uv_s[uv, :], x_s[x, :])
        out_ref[at : at + 20, :] = jnp.where(at_speed, fastest, first)
        out_ref[at + 20 : at + 40, :] = jnp.where(lane < 64, uv2_s[uv, :], x2_s[x, :])
    outer = plus_s[pl.ds(7, NXY, stride=4), :] + minus_s[pl.ds(28, NXY, stride=4), :]
    low = iota((NXY, 128), 1) < 64
    last = pl.ds(27, NXY, stride=4)
    out_ref[pl.ds(19, NXY, stride=IN_ROWS), :] = jnp.where(low, uv_s[last, :], lanes(outer, 64))
    out_ref[pl.ds(39, NXY, stride=IN_ROWS), :] = jnp.where(low, uv2_s[last, :], outer)


def corner_fill(ref):
    def one(c, carry):
        at = c * 64
        for kx in range(3):
            for ky in range(3):
                ref[at + kx * 16 + ky * 4 + 3] = following(ref[at + kx * 16 + ky * 4], 2)
        for ky in range(3):
            for kz in range(4):
                ref[at + 48 + ky * 4 + kz] = following(ref[at + ky * 4 + kz], 0)
        for kx in range(4):
            for kz in range(4):
                ref[at + kx * 16 + 12 + kz] = following(ref[at + kx * 16 + kz], 1)
        return carry

    lax.fori_loop(0, 3, one, 0)


def corner_fold(ref):
    def one(c, carry):
        at = c * 64
        for kx in range(4):
            for kz in range(4):
                n = at + kx * 16 + kz
                ref[n] = ref[n] + preceding(ref[n + 12], 1)
        for ky in range(3):
            for kz in range(4):
                n = at + ky * 4 + kz
                ref[n] = ref[n] + preceding(ref[n + 48], 0)
        for kx in range(3):
            for ky in range(3):
                n = at + kx * 16 + ky * 4
                ref[n] = ref[n] + preceding(ref[n + 3], 2)
        return carry

    lax.fori_loop(0, 3, one, 0)


def parts(x):
    ea, eb = x[0] + x[3], x[1] + x[2]
    return ea - eb, 0.5 * eb, x[0] - x[3], x[1] - x[2]


def values_of(part):
    d, half, oa, ob = part
    out = [None] * 4
    for p in range(2):
        even = float(0.5 * (VALUES[p, 0] + VALUES[p, 3])) * d + half
        odd = float(0.5 * (VALUES[p, 0] - VALUES[p, 3])) * oa + float(0.5 * (VALUES[p, 1] - VALUES[p, 2])) * ob
        out[p], out[3 - p] = even + odd, even - odd
    return out


def slopes_of(part):
    d, _, oa, ob = part
    out = [None] * 4
    for p in range(2):
        even = float(0.5 * (SLOPES[p, 0] + SLOPES[p, 3])) * d
        odd = float(0.5 * (SLOPES[p, 0] - SLOPES[p, 3])) * oa + float(0.5 * (SLOPES[p, 1] - SLOPES[p, 2])) * ob
        out[p], out[3 - p] = even + odd, odd - even
    return out


def both_back(v, s):
    (va, vb, wa, wb), (sa, sb, ta, tb) = halves(v), halves(s)
    out = [None] * 4
    for k in range(2):
        first = float(0.5 * (VALUES[0, k] + VALUES[3, k])) * va + float(0.5 * (VALUES[1, k] + VALUES[2, k])) * vb
        first = first + float(0.5 * (SLOPES[0, k] - SLOPES[3, k])) * ta + float(0.5 * (SLOPES[1, k] - SLOPES[2, k])) * tb
        second = float(0.5 * (VALUES[0, k] - VALUES[3, k])) * wa + float(0.5 * (VALUES[1, k] - VALUES[2, k])) * wb
        second = second + float(0.5 * (SLOPES[0, k] + SLOPES[3, k])) * sa + float(0.5 * (SLOPES[1, k] + SLOPES[2, k])) * sb
        out[k], out[3 - k] = first + second, first - second
    return out


def slope_pieces(src, dst, a_s, b_s, c):
    def first(line):
        part = parts([src[c * 64 + k * 16 + line] for k in range(4)])
        v, s = values_of(part), slopes_of(part)
        for p in range(4):
            a_s[p * 16 + line] = v[p]
            a_s[64 + p * 16 + line] = s[p]

    def second(p, kz):
        pv = parts([a_s[p * 16 + k * 4 + kz] for k in range(4)])
        ps = parts([a_s[64 + p * 16 + k * 4 + kz] for k in range(4)])
        sv, vs, vv = values_of(ps), slopes_of(pv), values_of(pv)
        for r in range(4):
            b_s[p * 16 + r * 4 + kz] = sv[r]
            b_s[64 + p * 16 + r * 4 + kz] = vs[r]
            b_s[128 + p * 16 + r * 4 + kz] = vv[r]

    def third(pr, col):
        part = parts([b_s[64 * col + pr * 4 + k] for k in range(4)])
        out = slopes_of(part) if col == 2 else values_of(part)
        for t in range(4):
            dst[c * 192 + 64 * col + pr * 4 + t] = out[t]

    return (
        [partial(first, line) for line in range(16)]
        + [partial(second, p, kz) for p in range(4) for kz in range(4)]
        + [partial(third, pr, col) for pr in range(16) for col in range(3)]
    )


def slopes_at_points(src, dst, a_s, b_s):
    def one(c, carry):
        for piece in slope_pieces(src, dst, a_s, b_s, c):
            piece()
        return carry

    lax.fori_loop(0, 3, one, 0)


def points_to_corners(src, dst, a_s, b_s):
    values_t, slopes_t = VALUES.T, SLOPES.T

    def one(c, carry):
        at = c * 64
        for pr in range(16):
            for col in range(3):
                h = halves([src[c * 192 + 64 * col + pr * 4 + t] for t in range(4)])
                out = apply_table(slopes_t, -1, h) if col == 2 else apply_table(values_t, 1, h)
                for k in range(4):
                    b_s[64 * col + pr * 4 + k] = out[k]
        for p in range(4):
            for kz in range(4):
                sv = apply_table(values_t, 1, halves([b_s[p * 16 + r * 4 + kz] for r in range(4)]))
                vs = [b_s[64 + p * 16 + r * 4 + kz] for r in range(4)]
                v = both_back([b_s[128 + p * 16 + r * 4 + kz] for r in range(4)], vs)
                for k in range(4):
                    a_s[p * 16 + k * 4 + kz] = v[k]
                    a_s[64 + p * 16 + k * 4 + kz] = sv[k]
        for line in range(16):
            out = both_back([a_s[p * 16 + line] for p in range(4)], [a_s[64 + p * 16 + line] for p in range(4)])
            for k in range(4):
                dst[at + k * 16 + line] = out[k]
        return carry

    lax.fori_loop(0, 3, one, 0)


def legendre_line(u):
    out = [None] * 4
    for p in range(2):
        even = u[0] + float(LEGENDRE[p, 2] / p2) * u[2]
        odd = float(LEGENDRE[p, 1] / p1) * u[1]
        out[p] = even + odd
        out[3 - p] = even - odd
    return out


def sample_sizes(u_s, size_s, a_s):
    for bc in range(9):
        out = legendre_line([u_s[8 * (a * 9 + bc) : 8 * (a * 9 + bc) + 8, :] for a in range(3)])
        for p in range(4):
            a_s[p * 9 + bc] = out[p]
    for p in range(4):
        grid = [[None] * 3 for _ in range(4)]
        for c in range(3):
            out = legendre_line([a_s[p * 9 + b * 3 + c] for b in range(3)])
            for r in range(4):
                grid[r][c] = out[r]
        for r in range(4):
            out = legendre_line(grid[r])
            for t in range(4):
                size_s[p * 16 + r * 4 + t] = jnp.exp(theta_size * out[t])


PAIRS = ((0, 0), (1, 1), (2, 2), (0, 1), (0, 2), (1, 2))
AT = {pair: n for n, pair in enumerate(PAIRS)} | {(b, a): n for n, (a, b) in enumerate(PAIRS)}


def dot3(x, y, at):
    return x[at] * y[at] + x[at + 1] * y[at + 1] + x[at + 2] * y[at + 2]


def dot6(x, y):
    return dot3(x, y, 0) + 2.0 * dot3(x, y, 3)


def weight_of(pr):
    def w(k):
        return jnp.where((k == 0) | (k == 3), jnp.float32(WEIGHTS[0]), jnp.float32(WEIGHTS[1]))

    return w(pr >> 2) * w(pr & 3)


def jacobian(j_s, q):
    return [[j_s[c * 192 + col * 64 + q] for col in range(3)] for c in range(3)]


def stress(j_s, size_s, g_s, p_s):
    def one(pr, energy):
        pair_weight = weight_of(pr)
        for t in range(4):
            q = pr * 4 + t
            jac = jacobian(j_s, q)
            for c in range(3):
                jac[c][c] = jac[c][c] + 1.0
                j_s[c * 192 + c * 64 + q] = jac[c][c]
            size = size_s[q]
            inverse = 1.0 / size
            inverse2 = inverse * inverse
            weighted = (pair_weight * float(WEIGHTS[t])) * size
            dev = []
            for n, (a, b) in enumerate(PAIRS):
                gram = (jac[0][a] * jac[0][b] + jac[1][a] * jac[1][b] + jac[2][a] * jac[2][b]) * inverse2
                dev.append(gram - 1.0 if a == b else gram)
                g_s[n * 64 + q] = dev[n]
            energy = energy + weighted * size * size * dot6(dev, dev)
            scaled = [4.0 * weighted * d for d in dev]
            for c in range(3):
                for col in range(3):
                    p_s[c * 192 + col * 64 + q] = (
                        jac[c][0] * scaled[AT[0, col]]
                        + jac[c][1] * scaled[AT[1, col]]
                        + jac[c][2] * scaled[AT[2, col]]
                    )
        return energy

    return lax.fori_loop(0, 16, one, jnp.zeros((8, 128), jnp.float32))


def trial_terms(j_s, size_s, g_s, d_s):
    def one(pr, sums):
        e2, e3, e4 = sums
        pair_weight = weight_of(pr)
        for t in range(4):
            q = pr * 4 + t
            jac = jacobian(j_s, q)
            der = jacobian(d_s, q)
            size = size_s[q]
            point_weight = pair_weight * float(WEIGHTS[t])
            dev, first, second = [], [], []
            for n, (a, b) in enumerate(PAIRS):
                dev.append(g_s[n * 64 + q])
                cross = jac[0][a] * der[0][b] + jac[1][a] * der[1][b] + jac[2][a] * der[2][b]
                if a != b:
                    cross = cross + (jac[0][b] * der[0][a] + jac[1][b] * der[1][a] + jac[2][b] * der[2][a])
                first.append(cross)
                second.append(der[0][a] * der[0][b] + der[1][a] * der[1][b] + der[2][a] * der[2][b])
            square = 2.0 * dot3(first, first, 0) + dot3(first, first, 3)
            mixed = dot3(first, second, 0) + dot3(first, second, 3)
            low, high = point_weight * size, point_weight / size
            e2 = e2 + (high * square + low * dot6(dev, second))
            e3 = e3 + high * mixed
            e4 = e4 + high * dot6(second, second)
        return e2, e3, e4

    zero = jnp.zeros((8, 128), jnp.float32)
    e2, e3, e4 = lax.fori_loop(0, 16, one, (zero, zero, zero))
    return 2.0 * e2, -4.0 * e3, e4


def remap(u_s, v_s, mid_s, face_s, time_step, pieces):
    def mode(ref, m):
        return ref[24 * m : 24 * m + 24, :].reshape(3, 8, 128)

    def put(ref, m, value):
        ref[24 * m : 24 * m + 24, :] = value.reshape(24, 128)

    for d in range(3):
        v = mode(v_s, d)
        face = 0.5 * (v + following3(v, d))
        for stage, part in ((0, time_step), (1, 0.5 * time_step)):
            at = 12 * stage + 4 * d
            put(face_s, at, part * jnp.maximum(face, 0.0))
            put(face_s, at + 1, part * jnp.minimum(face, 0.0))
            put(face_s, at + 2, 6.0 * part * v)
            put(face_s, at + 3, 10.0 * part * v)

    def terms(w, d, stage):
        at = 12 * stage + 4 * d
        even = w[0] + w[2]
        flux = mode(face_s, at) * (even + w[1]) + mode(face_s, at + 1) * following3(even - w[1], d)
        before = preceding3(flux, d)
        jump = before - flux
        return (
            jump,
            mode(face_s, at + 2) * w[0] - 3.0 * (flux + before),
            mode(face_s, at + 3) * w[1] + 5.0 * jump,
        )

    def spare(upto):
        while done[0] < upto * len(pieces):
            pieces[done[0]]()
            done[0] += 1

    done = [0]
    for n in range(SUBSTEPS):
        for stage, src, dst in ((0, u_s, mid_s), (1, mid_s, u_s)):
            at = (2 * n + stage) / (2.0 * SUBSTEPS)
            for m in range(9):
                w = [mode(src, m + 9 * k) for k in range(3)]
                for k, term in enumerate(terms(w, 0, stage)):
                    old = w[k] if stage == 0 else 0.5 * (mode(u_s, m + 9 * k) + w[k])
                    put(dst, m + 9 * k, old + term)
                spare(at + (m + 1) / 27.0 / (2.0 * SUBSTEPS))
            for a in range(3):
                w = [[mode(src, 9 * a + 3 * b + c) for c in range(3)] for b in range(3)]
                acc = [list(terms(w[b], 2, stage)) for b in range(3)]
                spare(at + (9 + 6 * a + 3) / 27.0 / (2.0 * SUBSTEPS))
                for c in range(3):
                    for b, term in enumerate(terms([w[b][c] for b in range(3)], 1, stage)):
                        acc[b][c] = acc[b][c] + term
                for b in range(3):
                    for c in range(3):
                        m = 9 * a + 3 * b + c
                        put(dst, m, mode(dst, m) + acc[b][c])
                spare(at + (9 + 6 * a + 6) / 27.0 / (2.0 * SUBSTEPS))
    spare(1.0)


def main_kernel(
    g_ref, in_ref, out_ref, in_s, outer_s, t_s, u_s, v_s, mid_s, face_s, uf_s, g3_s, x_s, a_s, b_s, j_s, p_s, g_s, size_s
):
    corners = [(n, kz, (n // 9) * 64 + ((n // 3) % 3) * 16 + (n % 3) * 4 + kz) for n in range(27) for kz in range(3)]
    in_s[0:8, :] = jnp.zeros((8, 128), jnp.float32)
    chunk = lax.div(g_ref[0], NZ)
    lane, row = iota((IN_ROWS, 128), 1), iota((IN_ROWS, 128), 0) % 20
    high = lane - 64
    layer = jnp.where(lane < 64, 4 * chunk - 8 + row, (12 * chunk - 3 + row + 384) // 3 - 128)
    upper = jnp.where(high < 54, (high >> 1) % 3, jnp.where(high < 56, 1, 0)) == 1
    layer = jnp.where((row == 19) & (lane >= 64), jnp.where(upper, 4 * chunk + 12, 4 * chunk - 9), layer)
    beyond = jnp.abs(2 * layer - 127) > 128
    for n in range(NXY):
        other = (2 * FAR_SENDER[n // 8] + (n // 4) % 2) * 4 + n % 4
        own, far = in_ref[IN_ROWS * n : IN_ROWS * n + IN_ROWS, :], in_ref[IN_ROWS * other : IN_ROWS * other + IN_ROWS, :]
        in_s[8 + IN_ROWS * n : 8 + IN_ROWS * n + IN_ROWS, :] = jnp.where(beyond, far, own)
    in_s[8 + NXY * IN_ROWS : 16 + NXY * IN_ROWS, :] = jnp.zeros((8, 128), jnp.float32)
    outer = lanes(in_s[pl.ds(8 + 19, 2 * NXY, stride=20), :], 64)
    lane = iota((2 * NXY, 128), 1)
    trace = jnp.where(lane < 54, (lane >> 1) % 3, 1) == 0
    speed = jnp.abs(2 * lane - 117) < 2
    outer_s[0:64, :] = jnp.where(trace, outer, jnp.where(speed, outer, 0.0))
    outer_s[64:128, :] = jnp.where(trace, lanes(outer, 2), jnp.where(speed, lanes(outer, -4), 0.0))
    row = iota((8, 128), 0)
    for t in range(3):
        for j in range(4):
            stacked = []
            for i in range(8):
                for a in range(2):
                    n = 2 * (4 * i + j) + a
                    block = in_s[pl.ds(8 + 20 * n + t - 1, 8, stride=3), :]
                    if t == 0:
                        block = jnp.where(row == 0, outer_s[n : n + 1, :], block)
                        block = jnp.where(row == 7, outer_s[64 + n : 65 + n, :], block)
                    stacked.append(block)
            t_s[...] = jnp.concatenate(stacked, axis=0).T
            for b in range(2):
                y = 2 * j + b
                u_s[pl.ds(8 * t + y, 27, stride=24), :] = t_s[pl.ds(b, 27, stride=2), :]
                v_s[pl.ds(8 * t + y, 3, stride=24), :] = t_s[pl.ds(54 + b, 3, stride=2), :]
                nodes = t_s[pl.ds(64 + b, 27, stride=2), :]
                if t == 0:
                    nodes = lanes(nodes, 1)
                g3_s[pl.ds(216 * ((t + 2) % 3) + y, 27, stride=8), :] = nodes
    lane = iota((8, 128), 1)
    fastest = jnp.max(in_ref[pl.ds(0, NXY, stride=IN_ROWS), :], axis=0, keepdims=True)
    fastest = jnp.where(iota((1, 128), 1) < SUM_LANE, 0.0, fastest)
    fastest = jnp.broadcast_to(jnp.max(fastest, axis=1, keepdims=True), (8, 128))
    for n, kz, at in corners:
        x_s[at] = g3_s[216 * kz + 8 * n : 216 * kz + 8 * n + 8, :]
    corner_fill(x_s)
    pieces = [piece for c in range(3) for piece in slope_pieces(x_s, j_s, a_s, b_s, c)]
    remap(u_s, v_s, mid_s, face_s, courant / jnp.maximum(fastest, 0.25), pieces)

    layer = lane & 7
    for m in range(27):
        u0, u1, u2 = (u_s[24 * m + 8 * t : 24 * m + 8 * t + 8, :] for t in range(3))
        value = jnp.where(layer == 3, u2, u0)
        value = jnp.where(layer < 2, lanes(jnp.where(layer == 2, u2, u0), 2), value)
        value = jnp.where(layer == 2, lanes(u1, 1), value)
        uf_s[8 * m : 8 * m + 8, :] = jnp.where(layer == 5, lanes(u1, -1), value)
    sample_sizes(uf_s, size_s, a_s)
    for m in range(27):
        uf_s[8 * m : 8 * m + 8, :] = (1.0 / SCALES[m]) * uf_s[8 * m : 8 * m + 8, :]
    energy = stress(j_s, size_s, g_s, p_s)
    points_to_corners(p_s, x_s, a_s, b_s)
    corner_fold(x_s)
    square = jnp.zeros((8, 128), jnp.float32)
    for n, kz, at in corners:
        grad = x_s[at]
        g3_s[216 * kz + 8 * n : 216 * kz + 8 * n + 8, :] = grad
        square = square + grad * grad
    own = jnp.abs(2 * layer - 5) < 4

    def own_sum(x):
        return jnp.sum(jnp.where(own, x, 0.0), axis=(0, 1), keepdims=True)

    square = own_sum(square)
    length = jnp.sqrt(1.0 + square * (1.0 / (512.0 * 81.0)))
    shorter = jnp.broadcast_to(1.0 / length, (8, 128))
    for n, kz, at in corners:
        x_s[at] = x_s[at] * shorter
    corner_fill(x_s)
    slopes_at_points(x_s, p_s, a_s, b_s)
    e2, e3, e4 = trial_terms(j_s, size_s, g_s, p_s)
    t_s[...] = jnp.zeros((128, 128), jnp.float32)
    length = jnp.broadcast_to(length, (8, 128))
    t_s[SUM_LANE:128, :] = length
    for n, total in enumerate((own_sum(energy), square, own_sum(e2), own_sum(e3), own_sum(e4))):
        t_s[SUM_LANE + n : SUM_LANE + 1 + n, :] = jnp.where(layer[0:1] == 1, total, length[0:1])
    for p in range(2):
        for j in range(4):
            for b in range(2):
                y = 2 * j + b
                first = uf_s[pl.ds(y, 27, stride=8), :] if p == 0 else g3_s[pl.ds(216 + y, 27, stride=8), :]
                t_s[pl.ds(b, 27, stride=2), :] = first
                t_s[pl.ds(64 + b, 27, stride=2), :] = g3_s[pl.ds(432 * p + y, 27, stride=8), :]
            back = t_s[...].T
            for i in range(8):
                for a in range(2):
                    to = (4 * i + j) * OUT_ROWS + 8 * p + 4 * a
                    at = (2 * i + a) * 8 + 1
                    out_ref[to : to + 4, :] = back[at : at + 4, :]


def unpack_kernel(in_ref, u_ref, g_ref, sums_ref, u_s, g_s):
    def part(p, a, layer):
        return in_ref[pl.ds(8 * p + 4 * a + layer, NXY, stride=OUT_ROWS), :]

    low = iota((NXY, 128), 1) < 64
    for layer in range(4):
        for a in range(2):
            u_s[pl.ds(128 * a + layer, NXY, stride=4), :] = part(0, a, layer)
        for kz in range(3):
            first, second = part((kz + 1) // 2, 0, layer), part((kz + 1) // 2, 1, layer)
            if kz == 1:
                both = jnp.where(low, first, lanes(second, 64))
            else:
                both = jnp.where(low, lanes(first, 64), second)
            g_s[pl.ds(3 * layer + kz, NXY, stride=12), :] = both
    lane = iota((NXY, 128), 1)
    length = jnp.where(lane < SUM_LANE, 1.0, part(0, 0, 1))
    longest = jnp.max(length, axis=0, keepdims=True)
    ratio = length / longest
    ratio2 = ratio * ratio
    power = jnp.where(lane < SUM_LANE + 3, ratio2, jnp.where(lane < SUM_LANE + 4, ratio2 * ratio, ratio2 * ratio2))
    power = jnp.where(lane < SUM_LANE + 2, 1.0, power)
    total = jnp.sum(part(0, 0, 0) * power, axis=0, keepdims=True)
    total = jnp.where(lane[0:1] < SUM_LANE + 5, total, longest)
    sums_ref[...] = jnp.broadcast_to(total[None], (NZ, 1, 128))
    for a in range(2):
        back = u_s[128 * a : 128 * a + 128, :].T
        for m in range(27):
            u_ref[m, a] = back[2 * m : 2 * m + 2, :]
    for n in range(3):
        back = g_s[128 * n : 128 * n + 128, :].T
        for a in range(2):
            for q in range(27):
                c, kx, ky = q // 9, (q // 3) % 3, q % 3
                for b in range(2):
                    at = 64 * a + 2 * q + b
                    g_ref[c, 3 * a + kx, ky + 3 * b : ky + 3 * b + 1, 128 * n : 128 * n + 128] = back[at : at + 1, :]


def checks_kernel(sums_ref, out_ref):
    sums = jnp.concatenate([sums_ref[n] for n in range(NZ)], axis=0)
    lane = iota((NZ, 128), 1)
    e0, square, e2, e3, e4, length = (
        jnp.sum(jnp.where(lane == SUM_LANE + n, sums, 0.0), axis=1, keepdims=True) for n in range(6)
    )
    e0 = jnp.sum(e0, axis=0, keepdims=True)
    square = jnp.sum(square, axis=0, keepdims=True)
    elements = float(512 * NXY * NZ)
    entries = 81.0 * elements
    step = trial_step / jnp.sqrt(1.0 + square / entries)
    x = step * length
    trial = e0 - step * square + jnp.sum(x * x * (e2 + x * (e3 + x * e4)), axis=0, keepdims=True)
    for n, value in enumerate((e0 / elements, square / entries, trial / elements)):
        out_ref[n] = value[0, 0]


def shape(*dims):
    return jax.ShapeDtypeStruct(dims, jnp.float32)


def on_chip(*dims):
    return pltpu.VMEM(dims, jnp.float32)


def keep(x):
    return pltpu.with_memory_space_constraint(x, pltpu.VMEM)


def vmem(*dims):
    return pltpu.VMEM(dims, jnp.float32)


MAIN_SCRATCH = [
    vmem(16 + NXY * IN_ROWS, 128),
    vmem(128, 128),
    vmem(128, 128),
    vmem(27 * 24, 128),
    vmem(3 * 24, 128),
    vmem(27 * 24, 128),
    vmem(24 * 24, 128),
    vmem(27 * 8, 128),
    vmem(81 * 8, 128),
    vmem(192, 8, 128),
    vmem(128, 8, 128),
    vmem(192, 8, 128),
    vmem(576, 8, 128),
    vmem(576, 8, 128),
    vmem(384, 8, 128),
    vmem(64, 8, 128),
]
SMEM = pl.BlockSpec(memory_space=pltpu.SMEM)
VMEM = pl.BlockSpec(memory_space=pltpu.VMEM)


def near_groups(partner):
    groups = []
    for z in range(4):
        for core in range(2):
            for x in range(4):
                group = []
                for y in range(4):
                    for half in range(2):
                        at = z if half == 0 else partner[z]
                        group.append((((at * 2 + core) * 4 + x) * 4 + y) * 2 + half)
                groups.append(group)
    return groups


def on_device(displacement, size_field_modes, velocity):
    place = (lax.axis_index(XY) * NZ + lax.axis_index(GZ)).reshape(1).astype(jnp.int32)
    tuv, tx, halo = pl.pallas_call(
        transpose_kernel,
        out_shape=(on_chip(128, 128), on_chip(384, 128), on_chip(NZ, HALO_ROWS, 128)),
        in_specs=[SMEM, VMEM, VMEM, VMEM],
        out_specs=(VMEM, VMEM, VMEM),
        scratch_shapes=[vmem(128, 128), vmem(128, 384)],
        name="transpose",
    )(place, size_field_modes, velocity, displacement)
    halo = lax.all_to_all(halo, XY + GZ, 0, 0, axis_index_groups=near_groups(FAR_SENDER))
    packed = pl.pallas_call(
        pack_kernel,
        out_shape=on_chip(NXY * IN_ROWS, 128),
        in_specs=[SMEM, VMEM, VMEM, VMEM],
        out_specs=VMEM,
        scratch_shapes=[
            vmem(160, 128),
            vmem(408, 128),
            vmem(160, 128),
            vmem(408, 128),
            vmem(160, 128),
            vmem(160, 128),
        ],
        name="pack",
    )(place, keep(tuv), keep(tx), keep(halo))
    spread = lax.all_to_all(packed.reshape(NXY, IN_ROWS, 128), XY, 0, 0)
    result = pl.pallas_call(
        main_kernel,
        out_shape=on_chip(NXY * OUT_ROWS, 128),
        in_specs=[SMEM, VMEM],
        out_specs=VMEM,
        scratch_shapes=MAIN_SCRATCH,
        name="remap_and_gradient",
    )(place, keep(spread.reshape(NXY * IN_ROWS, 128)))
    result = lax.all_to_all(result.reshape(NXY, OUT_ROWS, 128), XY, 0, 0)
    advected, gradient, sums = pl.pallas_call(
        unpack_kernel,
        out_shape=(shape(27, 2, 2, 128), shape(3, 6, 6, 384), on_chip(NZ, 1, 128)),
        in_specs=[VMEM],
        out_specs=(VMEM, VMEM, VMEM),
        scratch_shapes=[vmem(256, 128), vmem(384, 128)],
        name="unpack",
    )(keep(result.reshape(NXY * OUT_ROWS, 128)))
    sums = lax.all_to_all(sums, XY + GZ, 0, 0, axis_index_groups=near_groups((3, 2, 1, 0)))
    checks = pl.pallas_call(
        checks_kernel, out_shape=shape(3), in_specs=[VMEM], out_specs=SMEM, name="checks"
    )(keep(sums))
    return advected, gradient, checks


def solution(mesh):
    finer = Mesh(
        mesh.devices.reshape(4, 2, mesh.shape["gy"], 4, 2), ("gx_0", "gx_1", "gy", "gz_0", "gz_1")
    )
    return jax.shard_map(
        on_device,
        mesh=finer,
        in_specs=(P(None, GX, "gy", GZ), P(None, GX, "gy", GZ), P(None, GX, "gy", GZ)),
        out_specs=(P(None, GX, "gy", GZ), P(None, GX, "gy", GZ), P()),
        check_vma=False,
    )
```

```python
from functools import partial

import jax
import jax.numpy as jnp
import numpy as np
from jax import lax
from jax.experimental import pallas as pl
from jax.experimental.pallas import tpu as pltpu
from jax.sharding import Mesh
from jax.sharding import PartitionSpec as P

SUBSTEPS = 4
GX = ("gx_0", "gx_1")
GZ = ("gz_0", "gz_1")
XY = ("gx_0", "gx_1", "gy")

NZ = 8
NXY = 32
HALO_ROWS = 16
IN_ROWS = 40
SUM_LANE = 120
FAR_SENDER = (2, 3, 0, 1)
OUT_ROWS = 16

p0 = 0.7071067811865476
p1 = 1.224744871391589
p2 = 1.5811388300841898
SCALES = [a * b * c for a in (p0, p1, p2) for b in (p0, p1, p2) for c in (p0, p1, p2)]
courant = 0.1
theta_size = 0.3
trial_step = 0.05


def build_tables():
    points = np.array(
        [-0.8611363115940526, -0.3399810435848563, 0.3399810435848563, 0.8611363115940526]
    )
    weights = np.array(
        [0.3478548451374538, 0.6521451548625461, 0.6521451548625461, 0.3478548451374538]
    )
    points = 0.5 * (points + 1.0)
    weights = 0.5 * weights
    node_points = np.array([0.0, 1.0 / 3.0, 2.0 / 3.0, 1.0])
    value_table = np.zeros((4, 4))
    slope_table = np.zeros((4, 4))
    for column in range(4):
        others = [node_points[member] for member in range(4) if member != column]
        denominator = np.prod([node_points[column] - member for member in others])
        for quad_row in range(4):
            gauss_point = points[quad_row]
            value_table[quad_row, column] = (
                np.prod([gauss_point - member for member in others]) / denominator
            )
            slope_table[quad_row, column] = (
                sum(
                    np.prod(
                        [gauss_point - others[position] for position in range(3) if position != skipped]
                    )
                    for skipped in range(3)
                )
                / denominator
            )
    centred = 2.0 * points - 1.0
    legendre_table = np.stack(
        [
            np.full(4, p0),
            p1 * centred,
            p2 * 0.5 * (3.0 * centred**2 - 1.0),
        ],
        axis=1,
    )
    return value_table, slope_table, legendre_table, weights


VALUES, SLOPES, LEGENDRE, WEIGHTS = build_tables()


def iota(shape, dim):
    return lax.broadcasted_iota(jnp.int32, shape, dim)


def lanes(x, by):
    return pltpu.roll(x, (-by) % 128, x.ndim - 1)


def rows(x, by):
    return pltpu.roll(x, (-by) % 8, x.ndim - 2)


def following(x, d):
    return rows(x, 1) if d == 1 else lanes(x, 8 if d == 0 else 1)


def preceding(x, d):
    return rows(x, -1) if d == 1 else lanes(x, -8 if d == 0 else -1)


def following3(x, d):
    if d < 2:
        return following(x, d)
    return jnp.stack([x[1], x[2], lanes(x[0], 1)])


def preceding3(x, d):
    if d < 2:
        return preceding(x, d)
    return jnp.stack([lanes(x[2], -1), x[0], x[1]])


def halves(x):
    return (x[0] + x[3], x[1] + x[2], x[0] - x[3], x[1] - x[2])


def apply_table(table, sign, half):
    ea, eb, oa, ob = half
    out = [None] * 4
    for p in range(2):
        even = float(0.5 * (table[p, 0] + table[p, 3])) * ea + float(0.5 * (table[p, 1] + table[p, 2])) * eb
        odd = float(0.5 * (table[p, 0] - table[p, 3])) * oa + float(0.5 * (table[p, 1] - table[p, 2])) * ob
        out[p] = even + odd
        out[3 - p] = even - odd if sign > 0 else odd - even
    return out


def transpose_kernel(g_ref, u_ref, v_ref, x_ref, tuv_ref, tx_ref, halo_ref, uv_s, x_s):
    zero = jnp.zeros((16, 384), jnp.float32)
    for a in range(2):
        for m in range(27):
            uv_s[64 * a + 2 * m : 64 * a + 2 * m + 2, :] = SCALES[m] * u_ref[m, a]
        for d in range(3):
            uv_s[64 * a + 54 + 2 * d : 64 * a + 56 + 2 * d, :] = v_ref[d, a]
        uv_s[64 * a + 60 : 64 * a + 64, :] = zero[0:4, 0:128]
        at = 64 * (1 - a)
        for n in range(27):
            c, kx, ky = n // 9, (n // 3) % 3, n % 3
            for b in range(2):
                x_s[at + 2 * n + b : at + 2 * n + b + 1, :] = x_ref[c, 3 * a + kx, ky + 3 * b : ky + 3 * b + 1, :]
        x_s[at + 54 : at + 64, :] = zero[0:10]
    tuv_ref[...] = uv_s[...].T
    for n in range(3):
        tx_ref[128 * n : 128 * n + 128, :] = x_s[:, 128 * n : 128 * n + 128].T
    speed = jnp.abs(v_ref[0]) + jnp.abs(v_ref[1]) + jnp.abs(v_ref[2])
    speed = jnp.maximum(speed[0], speed[1])
    fastest = jnp.broadcast_to(jnp.max(speed, axis=(0, 1), keepdims=True), (1, 128))
    for n in range(NZ):
        halo_ref[n, :, :] = zero[0:16, 0:128]
        halo_ref[n, 13:14, :] = fastest
    at_z = lax.rem(g_ref[0], NZ)
    up = lax.rem(at_z + 1, NZ)
    down = lax.rem(at_z + NZ - 1, NZ)
    halo_ref[up, 0:9, :] = tuv_ref[119:128, :]
    halo_ref[up, 9:12, :] = tx_ref[381:384, :]
    halo_ref[down, 0:9, :] = tuv_ref[0:9, :]
    halo_ref[down, 9:13, :] = tx_ref[0:4, :]


def pack_kernel(g_ref, tuv_ref, tx_ref, halo_ref, out_ref, uv_s, x_s, uv2_s, x2_s, plus_s, minus_s):
    at_z = lax.rem(g_ref[0], NZ)
    below = lax.rem(at_z + NZ - 1, NZ)
    above = lax.rem(at_z + 1, NZ)
    uv_s[0:16, :] = jnp.zeros((16, 128), jnp.float32)
    uv_s[144:160, :] = jnp.zeros((16, 128), jnp.float32)
    x_s[0:8, :] = jnp.zeros((8, 128), jnp.float32)
    x_s[392:408, :] = jnp.zeros((16, 128), jnp.float32)
    uv_s[16:144, :] = tuv_ref[...]
    x_s[8:392, :] = tx_ref[...]
    uv_s[7:16, :] = halo_ref[below, 0:9, :]
    uv_s[144:153, :] = halo_ref[above, 0:9, :]
    x_s[5:8, :] = halo_ref[below, 9:12, :]
    x_s[392:396, :] = halo_ref[above, 9:13, :]
    uv = uv_s[...]
    uv2_s[...] = lanes(uv, 64)
    x2_s[...] = lanes(x_s[...], 64)
    lane = iota((160, 128), 1) & 63
    along_z = (lane >> 1) % 3
    even = uv + lanes(uv, 4)
    odd = lanes(uv, 2)
    field = lane < 54
    plus_s[...] = jnp.where(field, jnp.where(along_z == 0, even + odd, 0.0), jnp.where(lane >= 58, uv, 0.0))
    minus = lanes(even - odd, -2)
    minus_s[...] = jnp.where(field, jnp.where(along_z == 1, minus, 0.0), jnp.where(lane < 56, lanes(uv, 4), 0.0))
    fastest = halo_ref[0, 13:14, :]
    for n in range(1, NZ):
        fastest = jnp.maximum(fastest, halo_ref[n, 13:14, :])
    lane, row = iota((20, 128), 1), iota((20, 128), 0)
    at_speed = jnp.where(row == 0, lane, 0) >= SUM_LANE
    for k in range(NXY):
        at = IN_ROWS * k
        uv, x = pl.ds(4 * k + 8, 20), pl.ds(12 * k + 5, 20)
        first = jnp.where(lane < 64, uv_s[uv, :], x_s[x, :])
        out_ref[at : at + 20, :] = jnp.where(at_speed, fastest, first)
        out_ref[at + 20 : at + 40, :] = jnp.where(lane < 64, uv2_s[uv, :], x2_s[x, :])
    outer = plus_s[pl.ds(7, NXY, stride=4), :] + minus_s[pl.ds(28, NXY, stride=4), :]
    low = iota((NXY, 128), 1) < 64
    last = pl.ds(27, NXY, stride=4)
    out_ref[pl.ds(19, NXY, stride=IN_ROWS), :] = jnp.where(low, uv_s[last, :], lanes(outer, 64))
    out_ref[pl.ds(39, NXY, stride=IN_ROWS), :] = jnp.where(low, uv2_s[last, :], outer)


def corner_fill(ref):
    def one(c, carry):
        at = c * 64
        for kx in range(3):
            for ky in range(3):
                ref[at + kx * 16 + ky * 4 + 3] = following(ref[at + kx * 16 + ky * 4], 2)
        for ky in range(3):
            for kz in range(4):
                ref[at + 48 + ky * 4 + kz] = following(ref[at + ky * 4 + kz], 0)
        for kx in range(4):
            for kz in range(4):
                ref[at + kx * 16 + 12 + kz] = following(ref[at + kx * 16 + kz], 1)
        return carry

    lax.fori_loop(0, 3, one, 0)


def corner_fold(ref):
    def one(c, carry):
        at = c * 64
        for kx in range(4):
            for kz in range(4):
                n = at + kx * 16 + kz
                ref[n] = ref[n] + preceding(ref[n + 12], 1)
        for ky in range(3):
            for kz in range(4):
                n = at + ky * 4 + kz
                ref[n] = ref[n] + preceding(ref[n + 48], 0)
        for kx in range(3):
            for ky in range(3):
                n = at + kx * 16 + ky * 4
                ref[n] = ref[n] + preceding(ref[n + 3], 2)
        return carry

    lax.fori_loop(0, 3, one, 0)


def parts(x):
    ea, eb = x[0] + x[3], x[1] + x[2]
    return ea - eb, 0.5 * eb, x[0] - x[3], x[1] - x[2]


def values_of(part):
    d, half, oa, ob = part
    out = [None] * 4
    for p in range(2):
        even = float(0.5 * (VALUES[p, 0] + VALUES[p, 3])) * d + half
        odd = float(0.5 * (VALUES[p, 0] - VALUES[p, 3])) * oa + float(0.5 * (VALUES[p, 1] - VALUES[p, 2])) * ob
        out[p], out[3 - p] = even + odd, even - odd
    return out


def slopes_of(part):
    d, _, oa, ob = part
    out = [None] * 4
    for p in range(2):
        even = float(0.5 * (SLOPES[p, 0] + SLOPES[p, 3])) * d
        odd = float(0.5 * (SLOPES[p, 0] - SLOPES[p, 3])) * oa + float(0.5 * (SLOPES[p, 1] - SLOPES[p, 2])) * ob
        out[p], out[3 - p] = even + odd, odd - even
    return out


def slopes_back(s):
    sa, sb, ta, tb = halves(s)
    odd = float(0.5 * (SLOPES[0, 0] - SLOPES[3, 0])) * ta + float(0.5 * (SLOPES[1, 0] - SLOPES[2, 0])) * tb
    e0 = float(0.5 * (SLOPES[0, 0] + SLOPES[3, 0])) * sa + float(0.5 * (SLOPES[1, 0] + SLOPES[2, 0])) * sb
    e1 = float(0.5 * (SLOPES[0, 1] + SLOPES[3, 1])) * sa + float(0.5 * (SLOPES[1, 1] + SLOPES[2, 1])) * sb
    return [odd + e0, e1 - odd, -odd - e1, odd - e0]


def both_back(v, s):
    (va, vb, wa, wb), (sa, sb, ta, tb) = halves(v), halves(s)
    odd = float(0.5 * (SLOPES[0, 0] - SLOPES[3, 0])) * ta + float(0.5 * (SLOPES[1, 0] - SLOPES[2, 0])) * tb
    out = [None] * 4
    for k in range(2):
        first = float(0.5 * (VALUES[0, k] + VALUES[3, k])) * va + float(0.5 * (VALUES[1, k] + VALUES[2, k])) * vb
        first = first + odd if k == 0 else first - odd
        second = float(0.5 * (VALUES[0, k] - VALUES[3, k])) * wa + float(0.5 * (VALUES[1, k] - VALUES[2, k])) * wb
        second = second + float(0.5 * (SLOPES[0, k] + SLOPES[3, k])) * sa + float(0.5 * (SLOPES[1, k] + SLOPES[2, k])) * sb
        out[k], out[3 - k] = first + second, first - second
    return out


def slope_pieces(src, dst, a_s, b_s, c):
    def first(line):
        part = parts([src[c * 64 + k * 16 + line] for k in range(4)])
        v, s = values_of(part), slopes_of(part)
        for p in range(4):
            a_s[p * 16 + line] = v[p]
            a_s[64 + p * 16 + line] = s[p]

    def second(p, kz):
        pv = parts([a_s[p * 16 + k * 4 + kz] for k in range(4)])
        ps = parts([a_s[64 + p * 16 + k * 4 + kz] for k in range(4)])
        sv, vs, vv = values_of(ps), slopes_of(pv), values_of(pv)
        for r in range(4):
            b_s[p * 16 + r * 4 + kz] = sv[r]
            b_s[64 + p * 16 + r * 4 + kz] = vs[r]
            b_s[128 + p * 16 + r * 4 + kz] = vv[r]

    def third(pr, col):
        part = parts([b_s[64 * col + pr * 4 + k] for k in range(4)])
        out = slopes_of(part) if col == 2 else values_of(part)
        for t in range(4):
            dst[c * 192 + 64 * col + pr * 4 + t] = out[t]

    return (
        [partial(first, line) for line in range(16)]
        + [partial(second, p, kz) for p in range(4) for kz in range(4)]
        + [partial(third, pr, col) for pr in range(16) for col in range(3)]
    )


def points_to_corners(src, dst, a_s, b_s):
    values_t = VALUES.T

    def one(c, carry):
        at = c * 64
        for pr in range(16):
            for col in range(3):
                at_points = [src[c * 192 + 64 * col + pr * 4 + t] for t in range(4)]
                out = slopes_back(at_points) if col == 2 else apply_table(values_t, 1, halves(at_points))
                for k in range(4):
                    b_s[64 * col + pr * 4 + k] = out[k]
        for p in range(4):
            for kz in range(4):
                sv = apply_table(values_t, 1, halves([b_s[p * 16 + r * 4 + kz] for r in range(4)]))
                vs = [b_s[64 + p * 16 + r * 4 + kz] for r in range(4)]
                v = both_back([b_s[128 + p * 16 + r * 4 + kz] for r in range(4)], vs)
                for k in range(4):
                    a_s[p * 16 + k * 4 + kz] = v[k]
                    a_s[64 + p * 16 + k * 4 + kz] = sv[k]
        for line in range(16):
            out = both_back([a_s[p * 16 + line] for p in range(4)], [a_s[64 + p * 16 + line] for p in range(4)])
            for k in range(4):
                dst[at + k * 16 + line] = out[k]
        return carry

    lax.fori_loop(0, 3, one, 0)


def legendre_line(u):
    out = [None] * 4
    for p in range(2):
        even = u[0] + float(LEGENDRE[p, 2] / p2) * u[2]
        odd = float(LEGENDRE[p, 1] / p1) * u[1]
        out[p] = even + odd
        out[3 - p] = even - odd
    return out


def sample_sizes(u_s, size_s, a_s):
    for bc in range(9):
        out = legendre_line([u_s[8 * (a * 9 + bc) : 8 * (a * 9 + bc) + 8, :] for a in range(3)])
        for p in range(4):
            a_s[p * 9 + bc] = out[p]
    for p in range(4):
        grid = [[None] * 3 for _ in range(4)]
        for c in range(3):
            out = legendre_line([a_s[p * 9 + b * 3 + c] for b in range(3)])
            for r in range(4):
                grid[r][c] = out[r]
        for r in range(4):
            out = legendre_line(grid[r])
            for t in range(4):
                size_s[p * 16 + r * 4 + t] = jnp.exp(theta_size * out[t])


PAIRS = ((0, 0), (1, 1), (2, 2), (0, 1), (0, 2), (1, 2))
AT = {pair: n for n, pair in enumerate(PAIRS)} | {(b, a): n for n, (a, b) in enumerate(PAIRS)}


def dot3(x, y, at):
    return x[at] * y[at] + x[at + 1] * y[at + 1] + x[at + 2] * y[at + 2]


def dot6(x, y):
    return dot3(x, y, 0) + 2.0 * dot3(x, y, 3)


def weight_of(pr):
    def w(k):
        return jnp.where((k == 0) | (k == 3), jnp.float32(WEIGHTS[0]), jnp.float32(WEIGHTS[1]))

    return w(pr >> 2) * w(pr & 3)


def jacobian(j_s, q):
    return [[j_s[c * 192 + col * 64 + q] for col in range(3)] for c in range(3)]


def stress(j_s, size_s, g_s, p_s):
    def one(pr, energy):
        weights = [weight_of(2 * pr), weight_of(2 * pr + 1)]
        for t in range(8):
            q = pr * 8 + t
            pair_weight = weights[t // 4]
            jac = jacobian(j_s, q)
            for c in range(3):
                jac[c][c] = jac[c][c] + 1.0
                j_s[c * 192 + c * 64 + q] = jac[c][c]
            size = size_s[q]
            inverse = 1.0 / size
            inverse2 = inverse * inverse
            weighted = (pair_weight * float(WEIGHTS[t % 4])) * size
            dev = []
            for n, (a, b) in enumerate(PAIRS):
                gram = (jac[0][a] * jac[0][b] + jac[1][a] * jac[1][b] + jac[2][a] * jac[2][b]) * inverse2
                dev.append(gram - 1.0 if a == b else gram)
                g_s[n * 64 + q] = dev[n]
            energy = energy + weighted * size * size * dot6(dev, dev)
            scaled = [4.0 * weighted * d for d in dev]
            for c in range(3):
                for col in range(3):
                    p_s[c * 192 + col * 64 + q] = (
                        jac[c][0] * scaled[AT[0, col]]
                        + jac[c][1] * scaled[AT[1, col]]
                        + jac[c][2] * scaled[AT[2, col]]
                    )
        return energy

    return lax.fori_loop(0, 8, one, jnp.zeros((8, 128), jnp.float32))


def trial_terms(j_s, size_s, g_s, d_s):
    def one(pr, sums):
        e2, e3, e4 = sums
        weights = [weight_of(2 * pr), weight_of(2 * pr + 1)]
        for t in range(8):
            q = pr * 8 + t
            pair_weight = weights[t // 4]
            jac = jacobian(j_s, q)
            der = jacobian(d_s, q)
            size = size_s[q]
            point_weight = pair_weight * float(WEIGHTS[t % 4])
            dev, first, second = [], [], []
            for n, (a, b) in enumerate(PAIRS):
                dev.append(g_s[n * 64 + q])
                cross = jac[0][a] * der[0][b] + jac[1][a] * der[1][b] + jac[2][a] * der[2][b]
                if a != b:
                    cross = cross + (jac[0][b] * der[0][a] + jac[1][b] * der[1][a] + jac[2][b] * der[2][a])
                first.append(cross)
                second.append(der[0][a] * der[0][b] + der[1][a] * der[1][b] + der[2][a] * der[2][b])
            square = 2.0 * dot3(first, first, 0) + dot3(first, first, 3)
            mixed = dot3(first, second, 0) + dot3(first, second, 3)
            low, high = point_weight * size, point_weight / size
            e2 = e2 + (high * square + low * dot6(dev, second))
            e3 = e3 + high * mixed
            e4 = e4 + high * dot6(second, second)
        return e2, e3, e4

    zero = jnp.zeros((8, 128), jnp.float32)
    e2, e3, e4 = lax.fori_loop(0, 8, one, (zero, zero, zero))
    return 2.0 * e2, -4.0 * e3, e4


def remap(u_s, v_s, mid_s, face_s, time_step, pieces):
    def mode(ref, m):
        return ref[24 * m : 24 * m + 24, :].reshape(3, 8, 128)

    def put(ref, m, value):
        ref[24 * m : 24 * m + 24, :] = value.reshape(24, 128)

    for d in range(3):
        v = mode(v_s, d)
        face = 0.5 * (v + following3(v, d))
        for stage, part in ((0, time_step), (1, 0.5 * time_step)):
            at = 12 * stage + 4 * d
            put(face_s, at, part * jnp.maximum(face, 0.0))
            put(face_s, at + 1, part * jnp.minimum(face, 0.0))
            put(face_s, at + 2, 6.0 * part * v)
            put(face_s, at + 3, 10.0 * part * v)

    def terms(w, d, stage):
        at = 12 * stage + 4 * d
        even = w[0] + w[2]
        flux = mode(face_s, at) * (even + w[1]) + mode(face_s, at + 1) * following3(even - w[1], d)
        before = preceding3(flux, d)
        jump = before - flux
        return (
            jump,
            mode(face_s, at + 2) * w[0] - 3.0 * (flux + before),
            mode(face_s, at + 3) * w[1] + 5.0 * jump,
        )

    def spare(upto):
        while done[0] < upto * len(pieces):
            pieces[done[0]]()
            done[0] += 1

    done = [0]
    for n in range(SUBSTEPS):
        for stage, src, dst in ((0, u_s, mid_s), (1, mid_s, u_s)):
            at = (2 * n + stage) / (2.0 * SUBSTEPS)
            for m in range(9):
                w = [mode(src, m + 9 * k) for k in range(3)]
                for k, term in enumerate(terms(w, 0, stage)):
                    old = w[k] if stage == 0 else 0.5 * (mode(u_s, m + 9 * k) + w[k])
                    put(dst, m + 9 * k, old + term)
                spare(at + (m + 1) / 27.0 / (2.0 * SUBSTEPS))
            for a in range(3):
                w = [[mode(src, 9 * a + 3 * b + c) for c in range(3)] for b in range(3)]
                acc = [list(terms(w[b], 2, stage)) for b in range(3)]
                spare(at + (9 + 6 * a + 3) / 27.0 / (2.0 * SUBSTEPS))
                for c in range(3):
                    for b, term in enumerate(terms([w[b][c] for b in range(3)], 1, stage)):
                        acc[b][c] = acc[b][c] + term
                for b in range(3):
                    for c in range(3):
                        m = 9 * a + 3 * b + c
                        put(dst, m, mode(dst, m) + acc[b][c])
                spare(at + (9 + 6 * a + 6) / 27.0 / (2.0 * SUBSTEPS))
    spare(1.0)


def main_kernel(
    g_ref, in_ref, out_ref, in_s, outer_s, t_s, u_s, v_s, mid_s, face_s, uf_s, g3_s, x_s, a_s, b_s, j_s, p_s, g_s, size_s
):
    corners = [(n, kz, (n // 9) * 64 + ((n // 3) % 3) * 16 + (n % 3) * 4 + kz) for n in range(27) for kz in range(3)]
    in_s[0:8, :] = jnp.zeros((8, 128), jnp.float32)
    chunk = lax.div(g_ref[0], NZ)
    lane, row = iota((IN_ROWS, 128), 1), iota((IN_ROWS, 128), 0) % 20
    high = lane - 64
    layer = jnp.where(lane < 64, 4 * chunk - 8 + row, (12 * chunk - 3 + row + 384) // 3 - 128)
    upper = jnp.where(high < 54, (high >> 1) % 3, jnp.where(high < 56, 1, 0)) == 1
    layer = jnp.where((row == 19) & (lane >= 64), jnp.where(upper, 4 * chunk + 12, 4 * chunk - 9), layer)
    beyond = jnp.abs(2 * layer - 127) > 128
    for n in range(NXY):
        other = (2 * FAR_SENDER[n // 8] + (n // 4) % 2) * 4 + n % 4
        own, far = in_ref[IN_ROWS * n : IN_ROWS * n + IN_ROWS, :], in_ref[IN_ROWS * other : IN_ROWS * other + IN_ROWS, :]
        in_s[8 + IN_ROWS * n : 8 + IN_ROWS * n + IN_ROWS, :] = jnp.where(beyond, far, own)
    in_s[8 + NXY * IN_ROWS : 16 + NXY * IN_ROWS, :] = jnp.zeros((8, 128), jnp.float32)
    outer = lanes(in_s[pl.ds(8 + 19, 2 * NXY, stride=20), :], 64)
    lane = iota((2 * NXY, 128), 1)
    trace = jnp.where(lane < 54, (lane >> 1) % 3, 1) == 0
    speed = jnp.abs(2 * lane - 117) < 2
    outer_s[0:64, :] = jnp.where(trace, outer, jnp.where(speed, outer, 0.0))
    outer_s[64:128, :] = jnp.where(trace, lanes(outer, 2), jnp.where(speed, lanes(outer, -4), 0.0))
    row = iota((8, 128), 0)
    for t in range(3):
        for j in range(4):
            stacked = []
            for i in range(8):
                for a in range(2):
                    n = 2 * (4 * i + j) + a
                    block = in_s[pl.ds(8 + 20 * n + t - 1, 8, stride=3), :]
                    if t == 0:
                        block = jnp.where(row == 0, outer_s[n : n + 1, :], block)
                        block = jnp.where(row == 7, outer_s[64 + n : 65 + n, :], block)
                    stacked.append(block)
            t_s[...] = jnp.concatenate(stacked, axis=0).T
            for b in range(2):
                y = 2 * j + b
                u_s[pl.ds(8 * t + y, 27, stride=24), :] = t_s[pl.ds(b, 27, stride=2), :]
                v_s[pl.ds(8 * t + y, 3, stride=24), :] = t_s[pl.ds(54 + b, 3, stride=2), :]
                nodes = t_s[pl.ds(64 + b, 27, stride=2), :]
                if t == 0:
                    nodes = lanes(nodes, 1)
                g3_s[pl.ds(216 * ((t + 2) % 3) + y, 27, stride=8), :] = nodes
    lane = iota((8, 128), 1)
    fastest = jnp.max(in_ref[pl.ds(0, NXY, stride=IN_ROWS), :], axis=0, keepdims=True)
    fastest = jnp.where(iota((1, 128), 1) < SUM_LANE, 0.0, fastest)
    fastest = jnp.broadcast_to(jnp.max(fastest, axis=1, keepdims=True), (8, 128))
    for n, kz, at in corners:
        x_s[at] = g3_s[216 * kz + 8 * n : 216 * kz + 8 * n + 8, :]
    corner_fill(x_s)
    pieces = [piece for c in range(3) for piece in slope_pieces(x_s, j_s, a_s, b_s, c)]
    remap(u_s, v_s, mid_s, face_s, courant / jnp.maximum(fastest, 0.25), pieces)

    layer = lane & 7
    for m in range(27):
        u0, u1, u2 = (u_s[24 * m + 8 * t : 24 * m + 8 * t + 8, :] for t in range(3))
        value = jnp.where(layer == 3, u2, u0)
        value = jnp.where(layer < 2, lanes(jnp.where(layer == 2, u2, u0), 2), value)
        value = jnp.where(layer == 2, lanes(u1, 1), value)
        uf_s[8 * m : 8 * m + 8, :] = jnp.where(layer == 5, lanes(u1, -1), value)
    sample_sizes(uf_s, size_s, a_s)
    for m in range(27):
        uf_s[8 * m : 8 * m + 8, :] = (1.0 / SCALES[m]) * uf_s[8 * m : 8 * m + 8, :]
    energy = stress(j_s, size_s, g_s, p_s)
    points_to_corners(p_s, x_s, a_s, b_s)
    corner_fold(x_s)
    square = jnp.zeros((8, 128), jnp.float32)
    for n, kz, at in corners:
        grad = x_s[at]
        g3_s[216 * kz + 8 * n : 216 * kz + 8 * n + 8, :] = grad
        square = square + grad * grad
    own = jnp.abs(2 * layer - 5) < 4

    def own_sum(x):
        return jnp.sum(jnp.where(own, x, 0.0), axis=(0, 1), keepdims=True)

    square = own_sum(square)
    length = jnp.sqrt(1.0 + square * (1.0 / (512.0 * 81.0)))
    shorter = jnp.broadcast_to(1.0 / length, (8, 128))
    for n, kz, at in corners:
        x_s[at] = x_s[at] * shorter
    corner_fill(x_s)

    def pack_back(p, j):
        for b in range(2):
            y = 2 * j + b
            first = uf_s[pl.ds(y, 27, stride=8), :] if p == 0 else g3_s[pl.ds(216 + y, 27, stride=8), :]
            t_s[pl.ds(b, 27, stride=2), :] = first
            t_s[pl.ds(64 + b, 27, stride=2), :] = g3_s[pl.ds(432 * p + y, 27, stride=8), :]
        back = t_s[...].T
        for i in range(8):
            for a in range(2):
                to = (4 * i + j) * OUT_ROWS + 8 * p + 4 * a
                at = (2 * i + a) * 8 + 1
                out_ref[to : to + 4, :] = back[at : at + 4, :]

    pieces = [piece for c in range(3) for piece in slope_pieces(x_s, p_s, a_s, b_s, c)]
    for n, piece in enumerate(pieces):
        piece()
        if n % 60 == 30:
            pack_back(1, n // 60)
    e2, e3, e4 = trial_terms(j_s, size_s, g_s, p_s)
    t_s[...] = jnp.zeros((128, 128), jnp.float32)
    length = jnp.broadcast_to(length, (8, 128))
    t_s[SUM_LANE:128, :] = length
    for n, total in enumerate((own_sum(energy), square, own_sum(e2), own_sum(e3), own_sum(e4))):
        t_s[SUM_LANE + n : SUM_LANE + 1 + n, :] = jnp.where(layer[0:1] == 1, total, length[0:1])
    for j in range(4):
        pack_back(0, j)


def unpack_kernel(in_ref, u_ref, g_ref, sums_ref, u_s, g_s):
    def part(p, a, layer):
        return in_ref[pl.ds(8 * p + 4 * a + layer, NXY, stride=OUT_ROWS), :]

    low = iota((NXY, 128), 1) < 64
    for layer in range(4):
        for a in range(2):
            u_s[pl.ds(128 * a + layer, NXY, stride=4), :] = part(0, a, layer)
        for kz in range(3):
            first, second = part((kz + 1) // 2, 0, layer), part((kz + 1) // 2, 1, layer)
            if kz == 1:
                both = jnp.where(low, first, lanes(second, 64))
            else:
                both = jnp.where(low, lanes(first, 64), second)
            g_s[pl.ds(3 * layer + kz, NXY, stride=12), :] = both
    lane = iota((NXY, 128), 1)
    length = jnp.where(lane < SUM_LANE, 1.0, part(0, 0, 1))
    longest = jnp.max(length, axis=0, keepdims=True)
    ratio = length / longest
    ratio2 = ratio * ratio
    power = jnp.where(lane < SUM_LANE + 3, ratio2, jnp.where(lane < SUM_LANE + 4, ratio2 * ratio, ratio2 * ratio2))
    power = jnp.where(lane < SUM_LANE + 2, 1.0, power)
    total = jnp.sum(part(0, 0, 0) * power, axis=0, keepdims=True)
    total = jnp.where(lane[0:1] < SUM_LANE + 5, total, longest)
    sums_ref[...] = jnp.broadcast_to(total[None], (NZ, 1, 128))
    for a in range(2):
        back = u_s[128 * a : 128 * a + 128, :].T
        for m in range(27):
            u_ref[m, a] = back[2 * m : 2 * m + 2, :]
    for n in range(3):
        back = g_s[128 * n : 128 * n + 128, :].T
        for a in range(2):
            for q in range(27):
                c, kx, ky = q // 9, (q // 3) % 3, q % 3
                for b in range(2):
                    at = 64 * a + 2 * q + b
                    g_ref[c, 3 * a + kx, ky + 3 * b : ky + 3 * b + 1, 128 * n : 128 * n + 128] = back[at : at + 1, :]


def checks_kernel(sums_ref, out_ref):
    sums = jnp.concatenate([sums_ref[n] for n in range(NZ)], axis=0)
    lane = iota((NZ, 128), 1)
    e0, square, e2, e3, e4, length = (
        jnp.sum(jnp.where(lane == SUM_LANE + n, sums, 0.0), axis=1, keepdims=True) for n in range(6)
    )
    e0 = jnp.sum(e0, axis=0, keepdims=True)
    square = jnp.sum(square, axis=0, keepdims=True)
    elements = float(512 * NXY * NZ)
    entries = 81.0 * elements
    step = trial_step / jnp.sqrt(1.0 + square / entries)
    x = step * length
    trial = e0 - step * square + jnp.sum(x * x * (e2 + x * (e3 + x * e4)), axis=0, keepdims=True)
    for n, value in enumerate((e0 / elements, square / entries, trial / elements)):
        out_ref[n] = value[0, 0]


def shape(*dims):
    return jax.ShapeDtypeStruct(dims, jnp.float32)


def on_chip(*dims):
    return pltpu.VMEM(dims, jnp.float32)


def keep(x):
    return pltpu.with_memory_space_constraint(x, pltpu.VMEM)


def vmem(*dims):
    return pltpu.VMEM(dims, jnp.float32)


MAIN_SCRATCH = [
    vmem(16 + NXY * IN_ROWS, 128),
    vmem(128, 128),
    vmem(128, 128),
    vmem(27 * 24, 128),
    vmem(3 * 24, 128),
    vmem(27 * 24, 128),
    vmem(24 * 24, 128),
    vmem(27 * 8, 128),
    vmem(81 * 8, 128),
    vmem(192, 8, 128),
    vmem(128, 8, 128),
    vmem(192, 8, 128),
    vmem(576, 8, 128),
    vmem(576, 8, 128),
    vmem(384, 8, 128),
    vmem(64, 8, 128),
]
SMEM = pl.BlockSpec(memory_space=pltpu.SMEM)
VMEM = pl.BlockSpec(memory_space=pltpu.VMEM)


def near_groups(partner):
    groups = []
    for z in range(4):
        for core in range(2):
            for x in range(4):
                group = []
                for y in range(4):
                    for half in range(2):
                        at = z if half == 0 else partner[z]
                        group.append((((at * 2 + core) * 4 + x) * 4 + y) * 2 + half)
                groups.append(group)
    return groups


def on_device(displacement, size_field_modes, velocity):
    place = (lax.axis_index(XY) * NZ + lax.axis_index(GZ)).reshape(1).astype(jnp.int32)
    tuv, tx, halo = pl.pallas_call(
        transpose_kernel,
        out_shape=(on_chip(128, 128), on_chip(384, 128), on_chip(NZ, HALO_ROWS, 128)),
        in_specs=[SMEM, VMEM, VMEM, VMEM],
        out_specs=(VMEM, VMEM, VMEM),
        scratch_shapes=[vmem(128, 128), vmem(128, 384)],
        name="transpose",
    )(place, size_field_modes, velocity, displacement)
    halo = lax.all_to_all(halo, XY + GZ, 0, 0, axis_index_groups=near_groups(FAR_SENDER))
    packed = pl.pallas_call(
        pack_kernel,
        out_shape=on_chip(NXY * IN_ROWS, 128),
        in_specs=[SMEM, VMEM, VMEM, VMEM],
        out_specs=VMEM,
        scratch_shapes=[
            vmem(160, 128),
            vmem(408, 128),
            vmem(160, 128),
            vmem(408, 128),
            vmem(160, 128),
            vmem(160, 128),
        ],
        name="pack",
    )(place, keep(tuv), keep(tx), keep(halo))
    spread = lax.all_to_all(packed.reshape(NXY, IN_ROWS, 128), XY, 0, 0)
    result = pl.pallas_call(
        main_kernel,
        out_shape=on_chip(NXY * OUT_ROWS, 128),
        in_specs=[SMEM, VMEM],
        out_specs=VMEM,
        scratch_shapes=MAIN_SCRATCH,
        name="remap_and_gradient",
    )(place, keep(spread.reshape(NXY * IN_ROWS, 128)))
    result = lax.all_to_all(result.reshape(NXY, OUT_ROWS, 128), XY, 0, 0)
    advected, gradient, sums = pl.pallas_call(
        unpack_kernel,
        out_shape=(shape(27, 2, 2, 128), shape(3, 6, 6, 384), on_chip(NZ, 1, 128)),
        in_specs=[VMEM],
        out_specs=(VMEM, VMEM, VMEM),
        scratch_shapes=[vmem(256, 128), vmem(384, 128)],
        name="unpack",
    )(keep(result.reshape(NXY * OUT_ROWS, 128)))
    sums = lax.all_to_all(sums, XY + GZ, 0, 0, axis_index_groups=near_groups((3, 2, 1, 0)))
    checks = pl.pallas_call(
        checks_kernel, out_shape=shape(3), in_specs=[VMEM], out_specs=SMEM, name="checks"
    )(keep(sums))
    return advected, gradient, checks


def solution(mesh):
    finer = Mesh(
        mesh.devices.reshape(4, 2, mesh.shape["gy"], 4, 2), ("gx_0", "gx_1", "gy", "gz_0", "gz_1")
    )
    return jax.shard_map(
        on_device,
        mesh=finer,
        in_specs=(P(None, GX, "gy", GZ), P(None, GX, "gy", GZ), P(None, GX, "gy", GZ)),
        out_specs=(P(None, GX, "gy", GZ), P(None, GX, "gy", GZ), P()),
        check_vma=False,
    )
```

```python
from functools import partial

import jax
import jax.numpy as jnp
import numpy as np
from jax import lax
from jax.experimental import pallas as pl
from jax.experimental.pallas import tpu as pltpu
from jax.sharding import Mesh
from jax.sharding import PartitionSpec as P

SUBSTEPS = 4
GX = ("gx_0", "gx_1")
GZ = ("gz_0", "gz_1")
XY = ("gx_0", "gx_1", "gy")

NZ = 8
NXY = 32
HALO_ROWS = 16
IN_ROWS = 40
SUM_LANE = 120
FAR_SENDER = (2, 3, 0, 1)
OUT_ROWS = 16

p0 = 0.7071067811865476
p1 = 1.224744871391589
p2 = 1.5811388300841898
SCALES = [a * b * c for a in (p0, p1, p2) for b in (p0, p1, p2) for c in (p0, p1, p2)]
courant = 0.1
theta_size = 0.3
trial_step = 0.05


def build_tables():
    points = np.array(
        [-0.8611363115940526, -0.3399810435848563, 0.3399810435848563, 0.8611363115940526]
    )
    weights = np.array(
        [0.3478548451374538, 0.6521451548625461, 0.6521451548625461, 0.3478548451374538]
    )
    points = 0.5 * (points + 1.0)
    weights = 0.5 * weights
    node_points = np.array([0.0, 1.0 / 3.0, 2.0 / 3.0, 1.0])
    value_table = np.zeros((4, 4))
    slope_table = np.zeros((4, 4))
    for column in range(4):
        others = [node_points[member] for member in range(4) if member != column]
        denominator = np.prod([node_points[column] - member for member in others])
        for quad_row in range(4):
            gauss_point = points[quad_row]
            value_table[quad_row, column] = (
                np.prod([gauss_point - member for member in others]) / denominator
            )
            slope_table[quad_row, column] = (
                sum(
                    np.prod(
                        [gauss_point - others[position] for position in range(3) if position != skipped]
                    )
                    for skipped in range(3)
                )
                / denominator
            )
    centred = 2.0 * points - 1.0
    legendre_table = np.stack(
        [
            np.full(4, p0),
            p1 * centred,
            p2 * 0.5 * (3.0 * centred**2 - 1.0),
        ],
        axis=1,
    )
    return value_table, slope_table, legendre_table, weights


VALUES, SLOPES, LEGENDRE, WEIGHTS = build_tables()


def iota(shape, dim):
    return lax.broadcasted_iota(jnp.int32, shape, dim)


def lanes(x, by):
    return pltpu.roll(x, (-by) % 128, x.ndim - 1)


def rows(x, by):
    return pltpu.roll(x, (-by) % 8, x.ndim - 2)


def following(x, d):
    return rows(x, 1) if d == 1 else lanes(x, 8 if d == 0 else 1)


def preceding(x, d):
    return rows(x, -1) if d == 1 else lanes(x, -8 if d == 0 else -1)


def following3(x, d):
    if d < 2:
        return following(x, d)
    return jnp.stack([x[1], x[2], lanes(x[0], 1)])


def preceding3(x, d):
    if d < 2:
        return preceding(x, d)
    return jnp.stack([lanes(x[2], -1), x[0], x[1]])


def halves(x):
    return (x[0] + x[3], x[1] + x[2], x[0] - x[3], x[1] - x[2])


def apply_table(table, sign, half):
    ea, eb, oa, ob = half
    out = [None] * 4
    for p in range(2):
        even = float(0.5 * (table[p, 0] + table[p, 3])) * ea + float(0.5 * (table[p, 1] + table[p, 2])) * eb
        odd = float(0.5 * (table[p, 0] - table[p, 3])) * oa + float(0.5 * (table[p, 1] - table[p, 2])) * ob
        out[p] = even + odd
        out[3 - p] = even - odd if sign > 0 else odd - even
    return out


def transpose_kernel(g_ref, u_ref, v_ref, x_ref, tuv_ref, tx_ref, halo_ref, uv_s, x_s):
    zero = jnp.zeros((16, 384), jnp.float32)
    for a in range(2):
        for m in range(27):
            uv_s[64 * a + 2 * m : 64 * a + 2 * m + 2, :] = SCALES[m] * u_ref[m, a]
        for d in range(3):
            uv_s[64 * a + 54 + 2 * d : 64 * a + 56 + 2 * d, :] = v_ref[d, a]
        uv_s[64 * a + 60 : 64 * a + 64, :] = zero[0:4, 0:128]
        at = 64 * (1 - a)
        for n in range(27):
            c, kx, ky = n // 9, (n // 3) % 3, n % 3
            for b in range(2):
                x_s[at + 2 * n + b : at + 2 * n + b + 1, :] = x_ref[c, 3 * a + kx, ky + 3 * b : ky + 3 * b + 1, :]
        x_s[at + 54 : at + 64, :] = zero[0:10]
    tuv_ref[...] = uv_s[...].T
    for n in range(3):
        tx_ref[128 * n : 128 * n + 128, :] = x_s[:, 128 * n : 128 * n + 128].T
    speed = jnp.abs(v_ref[0]) + jnp.abs(v_ref[1]) + jnp.abs(v_ref[2])
    speed = jnp.maximum(speed[0], speed[1])
    fastest = jnp.broadcast_to(jnp.max(speed, axis=(0, 1), keepdims=True), (1, 128))
    for n in range(NZ):
        halo_ref[n, :, :] = zero[0:16, 0:128]
        halo_ref[n, 13:14, :] = fastest
    at_z = lax.rem(g_ref[0], NZ)
    up = lax.rem(at_z + 1, NZ)
    down = lax.rem(at_z + NZ - 1, NZ)
    halo_ref[up, 0:9, :] = tuv_ref[119:128, :]
    halo_ref[up, 9:12, :] = tx_ref[381:384, :]
    halo_ref[down, 0:9, :] = tuv_ref[0:9, :]
    halo_ref[down, 9:13, :] = tx_ref[0:4, :]


def pack_kernel(g_ref, tuv_ref, tx_ref, halo_ref, out_ref, uv_s, x_s, uv2_s, x2_s, plus_s, minus_s):
    at_z = lax.rem(g_ref[0], NZ)
    below = lax.rem(at_z + NZ - 1, NZ)
    above = lax.rem(at_z + 1, NZ)
    uv_s[0:16, :] = jnp.zeros((16, 128), jnp.float32)
    uv_s[144:160, :] = jnp.zeros((16, 128), jnp.float32)
    x_s[0:8, :] = jnp.zeros((8, 128), jnp.float32)
    x_s[392:408, :] = jnp.zeros((16, 128), jnp.float32)
    uv_s[16:144, :] = tuv_ref[...]
    x_s[8:392, :] = tx_ref[...]
    uv_s[7:16, :] = halo_ref[below, 0:9, :]
    uv_s[144:153, :] = halo_ref[above, 0:9, :]
    x_s[5:8, :] = halo_ref[below, 9:12, :]
    x_s[392:396, :] = halo_ref[above, 9:13, :]
    uv = uv_s[...]
    uv2_s[...] = lanes(uv, 64)
    x2_s[...] = lanes(x_s[...], 64)
    lane = iota((160, 128), 1) & 63
    along_z = (lane >> 1) % 3
    even = uv + lanes(uv, 4)
    odd = lanes(uv, 2)
    field = lane < 54
    plus_s[...] = jnp.where(field, jnp.where(along_z == 0, even + odd, 0.0), jnp.where(lane >= 58, uv, 0.0))
    minus = lanes(even - odd, -2)
    minus_s[...] = jnp.where(field, jnp.where(along_z == 1, minus, 0.0), jnp.where(lane < 56, lanes(uv, 4), 0.0))
    fastest = halo_ref[0, 13:14, :]
    for n in range(1, NZ):
        fastest = jnp.maximum(fastest, halo_ref[n, 13:14, :])
    lane, row = iota((20, 128), 1), iota((20, 128), 0)
    at_speed = jnp.where(row == 0, lane, 0) >= SUM_LANE
    for k in range(NXY):
        at = IN_ROWS * k
        uv, x = pl.ds(4 * k + 8, 20), pl.ds(12 * k + 5, 20)
        first = jnp.where(lane < 64, uv_s[uv, :], x_s[x, :])
        out_ref[at : at + 20, :] = jnp.where(at_speed, fastest, first)
        out_ref[at + 20 : at + 40, :] = jnp.where(lane < 64, uv2_s[uv, :], x2_s[x, :])
    outer = plus_s[pl.ds(7, NXY, stride=4), :] + minus_s[pl.ds(28, NXY, stride=4), :]
    low = iota((NXY, 128), 1) < 64
    last = pl.ds(27, NXY, stride=4)
    out_ref[pl.ds(19, NXY, stride=IN_ROWS), :] = jnp.where(low, uv_s[last, :], lanes(outer, 64))
    out_ref[pl.ds(39, NXY, stride=IN_ROWS), :] = jnp.where(low, uv2_s[last, :], outer)


def corner_fill(ref):
    def one(c, carry):
        at = c * 64
        for kx in range(3):
            for ky in range(3):
                ref[at + kx * 16 + ky * 4 + 3] = following(ref[at + kx * 16 + ky * 4], 2)
        for ky in range(3):
            for kz in range(4):
                ref[at + 48 + ky * 4 + kz] = following(ref[at + ky * 4 + kz], 0)
        for kx in range(4):
            for kz in range(4):
                ref[at + kx * 16 + 12 + kz] = following(ref[at + kx * 16 + kz], 1)
        return carry

    lax.fori_loop(0, 3, one, 0)


def corner_fold(ref):
    def one(c, carry):
        at = c * 64
        for kx in range(4):
            for kz in range(4):
                n = at + kx * 16 + kz
                ref[n] = ref[n] + preceding(ref[n + 12], 1)
        for ky in range(3):
            for kz in range(4):
                n = at + ky * 4 + kz
                ref[n] = ref[n] + preceding(ref[n + 48], 0)
        for kx in range(3):
            for ky in range(3):
                n = at + kx * 16 + ky * 4
                ref[n] = ref[n] + preceding(ref[n + 3], 2)
        return carry

    lax.fori_loop(0, 3, one, 0)


def parts(x):
    ea, eb = x[0] + x[3], x[1] + x[2]
    return ea - eb, 0.5 * eb, x[0] - x[3], x[1] - x[2]


def values_of(part):
    d, half, oa, ob = part
    out = [None] * 4
    for p in range(2):
        even = float(0.5 * (VALUES[p, 0] + VALUES[p, 3])) * d + half
        odd = float(0.5 * (VALUES[p, 0] - VALUES[p, 3])) * oa + float(0.5 * (VALUES[p, 1] - VALUES[p, 2])) * ob
        out[p], out[3 - p] = even + odd, even - odd
    return out


def slopes_of(part):
    d, _, oa, ob = part
    out = [None] * 4
    for p in range(2):
        even = float(0.5 * (SLOPES[p, 0] + SLOPES[p, 3])) * d
        odd = float(0.5 * (SLOPES[p, 0] - SLOPES[p, 3])) * oa + float(0.5 * (SLOPES[p, 1] - SLOPES[p, 2])) * ob
        out[p], out[3 - p] = even + odd, odd - even
    return out


def slopes_back(s):
    sa, sb, ta, tb = halves(s)
    odd = float(0.5 * (SLOPES[0, 0] - SLOPES[3, 0])) * ta + float(0.5 * (SLOPES[1, 0] - SLOPES[2, 0])) * tb
    e0 = float(0.5 * (SLOPES[0, 0] + SLOPES[3, 0])) * sa + float(0.5 * (SLOPES[1, 0] + SLOPES[2, 0])) * sb
    e1 = float(0.5 * (SLOPES[0, 1] + SLOPES[3, 1])) * sa + float(0.5 * (SLOPES[1, 1] + SLOPES[2, 1])) * sb
    return [odd + e0, e1 - odd, -odd - e1, odd - e0]


def both_back(v, s):
    (va, vb, wa, wb), (sa, sb, ta, tb) = halves(v), halves(s)
    odd = float(0.5 * (SLOPES[0, 0] - SLOPES[3, 0])) * ta + float(0.5 * (SLOPES[1, 0] - SLOPES[2, 0])) * tb
    out = [None] * 4
    for k in range(2):
        first = float(0.5 * (VALUES[0, k] + VALUES[3, k])) * va + float(0.5 * (VALUES[1, k] + VALUES[2, k])) * vb
        first = first + odd if k == 0 else first - odd
        second = float(0.5 * (VALUES[0, k] - VALUES[3, k])) * wa + float(0.5 * (VALUES[1, k] - VALUES[2, k])) * wb
        second = second + float(0.5 * (SLOPES[0, k] + SLOPES[3, k])) * sa + float(0.5 * (SLOPES[1, k] + SLOPES[2, k])) * sb
        out[k], out[3 - k] = first + second, first - second
    return out


def slope_pieces(src, dst, a_s, b_s, c):
    def first(line):
        part = parts([src[c * 64 + k * 16 + line] for k in range(4)])
        v, s = values_of(part), slopes_of(part)
        for p in range(4):
            a_s[p * 16 + line] = v[p]
            a_s[64 + p * 16 + line] = s[p]

    def second(p, kz):
        pv = parts([a_s[p * 16 + k * 4 + kz] for k in range(4)])
        ps = parts([a_s[64 + p * 16 + k * 4 + kz] for k in range(4)])
        sv, vs, vv = values_of(ps), slopes_of(pv), values_of(pv)
        for r in range(4):
            b_s[p * 16 + r * 4 + kz] = sv[r]
            b_s[64 + p * 16 + r * 4 + kz] = vs[r]
            b_s[128 + p * 16 + r * 4 + kz] = vv[r]

    def third(pr, col):
        part = parts([b_s[64 * col + pr * 4 + k] for k in range(4)])
        out = slopes_of(part) if col == 2 else values_of(part)
        for t in range(4):
            dst[c * 192 + 64 * col + pr * 4 + t] = out[t]

    return (
        [partial(first, line) for line in range(16)]
        + [partial(second, p, kz) for p in range(4) for kz in range(4)]
        + [partial(third, pr, col) for pr in range(16) for col in range(3)]
    )


def points_to_corners(src, dst, a_s, b_s):
    values_t = VALUES.T

    def one(c, carry):
        at = c * 64
        for pr in range(16):
            for col in range(3):
                at_points = [src[c * 192 + 64 * col + pr * 4 + t] for t in range(4)]
                out = slopes_back(at_points) if col == 2 else apply_table(values_t, 1, halves(at_points))
                for k in range(4):
                    b_s[64 * col + pr * 4 + k] = out[k]
        for p in range(4):
            for kz in range(4):
                sv = apply_table(values_t, 1, halves([b_s[p * 16 + r * 4 + kz] for r in range(4)]))
                vs = [b_s[64 + p * 16 + r * 4 + kz] for r in range(4)]
                v = both_back([b_s[128 + p * 16 + r * 4 + kz] for r in range(4)], vs)
                for k in range(4):
                    a_s[p * 16 + k * 4 + kz] = v[k]
                    a_s[64 + p * 16 + k * 4 + kz] = sv[k]
        for line in range(16):
            out = both_back([a_s[p * 16 + line] for p in range(4)], [a_s[64 + p * 16 + line] for p in range(4)])
            for k in range(4):
                dst[at + k * 16 + line] = out[k]
        return carry

    for c in range(3):
        one(c, 0)


def legendre_line(u):
    out = [None] * 4
    for p in range(2):
        even = u[0] + float(LEGENDRE[p, 2] / p2) * u[2]
        odd = float(LEGENDRE[p, 1] / p1) * u[1]
        out[p] = even + odd
        out[3 - p] = even - odd
    return out


def sample_sizes(u_s, size_s, a_s):
    for bc in range(9):
        out = legendre_line([u_s[8 * (a * 9 + bc) : 8 * (a * 9 + bc) + 8, :] for a in range(3)])
        for p in range(4):
            a_s[p * 9 + bc] = out[p]
    for p in range(4):
        grid = [[None] * 3 for _ in range(4)]
        for c in range(3):
            out = legendre_line([a_s[p * 9 + b * 3 + c] for b in range(3)])
            for r in range(4):
                grid[r][c] = out[r]
        for r in range(4):
            out = legendre_line(grid[r])
            for t in range(4):
                size_s[p * 16 + r * 4 + t] = jnp.exp(theta_size * out[t])


PAIRS = ((0, 0), (1, 1), (2, 2), (0, 1), (0, 2), (1, 2))
AT = {pair: n for n, pair in enumerate(PAIRS)} | {(b, a): n for n, (a, b) in enumerate(PAIRS)}


def dot3(x, y, at):
    return x[at] * y[at] + x[at + 1] * y[at + 1] + x[at + 2] * y[at + 2]


def dot6(x, y):
    return dot3(x, y, 0) + 2.0 * dot3(x, y, 3)


def weight_of(pr):
    def w(k):
        return jnp.where((k == 0) | (k == 3), jnp.float32(WEIGHTS[0]), jnp.float32(WEIGHTS[1]))

    return w(pr >> 2) * w(pr & 3)


def jacobian(j_s, q):
    return [[j_s[c * 192 + col * 64 + q] for col in range(3)] for c in range(3)]


def stress(j_s, size_s, g_s, p_s):
    def one(pr, energy):
        weights = [weight_of(4 * pr + n) for n in range(4)]
        for t in range(16):
            q = pr * 16 + t
            pair_weight = weights[t // 4]
            jac = jacobian(j_s, q)
            for c in range(3):
                jac[c][c] = jac[c][c] + 1.0
                j_s[c * 192 + c * 64 + q] = jac[c][c]
            size = size_s[q]
            inverse = 1.0 / size
            inverse2 = inverse * inverse
            weighted = (pair_weight * float(WEIGHTS[t % 4])) * size
            dev = []
            for n, (a, b) in enumerate(PAIRS):
                gram = (jac[0][a] * jac[0][b] + jac[1][a] * jac[1][b] + jac[2][a] * jac[2][b]) * inverse2
                dev.append(gram - 1.0 if a == b else gram)
                g_s[n * 64 + q] = dev[n]
            energy = energy + weighted * size * size * dot6(dev, dev)
            scaled = [4.0 * weighted * d for d in dev]
            for c in range(3):
                for col in range(3):
                    p_s[c * 192 + col * 64 + q] = (
                        jac[c][0] * scaled[AT[0, col]]
                        + jac[c][1] * scaled[AT[1, col]]
                        + jac[c][2] * scaled[AT[2, col]]
                    )
        return energy

    return lax.fori_loop(0, 4, one, jnp.zeros((8, 128), jnp.float32))


def trial_terms(j_s, size_s, g_s, d_s):
    def one(pr, sums):
        e2, e3, e4 = sums
        weights = [weight_of(4 * pr + n) for n in range(4)]
        for t in range(16):
            q = pr * 16 + t
            pair_weight = weights[t // 4]
            jac = jacobian(j_s, q)
            der = jacobian(d_s, q)
            size = size_s[q]
            point_weight = pair_weight * float(WEIGHTS[t % 4])
            dev, first, second = [], [], []
            for n, (a, b) in enumerate(PAIRS):
                dev.append(g_s[n * 64 + q])
                cross = jac[0][a] * der[0][b] + jac[1][a] * der[1][b] + jac[2][a] * der[2][b]
                if a != b:
                    cross = cross + (jac[0][b] * der[0][a] + jac[1][b] * der[1][a] + jac[2][b] * der[2][a])
                first.append(cross)
                second.append(der[0][a] * der[0][b] + der[1][a] * der[1][b] + der[2][a] * der[2][b])
            square = 2.0 * dot3(first, first, 0) + dot3(first, first, 3)
            mixed = dot3(first, second, 0) + dot3(first, second, 3)
            low, high = point_weight * size, point_weight / size
            e2 = e2 + (high * square + low * dot6(dev, second))
            e3 = e3 + high * mixed
            e4 = e4 + high * dot6(second, second)
        return e2, e3, e4

    zero = jnp.zeros((8, 128), jnp.float32)
    e2, e3, e4 = lax.fori_loop(0, 4, one, (zero, zero, zero))
    return 2.0 * e2, -4.0 * e3, e4


def remap(u_s, v_s, mid_s, face_s, time_step, pieces):
    def mode(ref, m):
        return ref[24 * m : 24 * m + 24, :].reshape(3, 8, 128)

    def put(ref, m, value):
        ref[24 * m : 24 * m + 24, :] = value.reshape(24, 128)

    for d in range(3):
        v = mode(v_s, d)
        face = 0.5 * (v + following3(v, d))
        for stage, part in ((0, time_step), (1, 0.5 * time_step)):
            at = 12 * stage + 4 * d
            put(face_s, at, part * jnp.maximum(face, 0.0))
            put(face_s, at + 1, part * jnp.minimum(face, 0.0))
            put(face_s, at + 2, 6.0 * part * v)
            put(face_s, at + 3, 10.0 * part * v)

    def terms(w, d, stage):
        at = 12 * stage + 4 * d
        even = w[0] + w[2]
        flux = mode(face_s, at) * (even + w[1]) + mode(face_s, at + 1) * following3(even - w[1], d)
        before = preceding3(flux, d)
        jump = before - flux
        return (
            jump,
            mode(face_s, at + 2) * w[0] - 3.0 * (flux + before),
            mode(face_s, at + 3) * w[1] + 5.0 * jump,
        )

    def spare(upto):
        while done[0] < upto * len(pieces):
            pieces[done[0]]()
            done[0] += 1

    done = [0]
    for n in range(SUBSTEPS):
        for stage, src, dst in ((0, u_s, mid_s), (1, mid_s, u_s)):
            at = (2 * n + stage) / (2.0 * SUBSTEPS)
            for m in range(9):
                w = [mode(src, m + 9 * k) for k in range(3)]
                for k, term in enumerate(terms(w, 0, stage)):
                    old = w[k] if stage == 0 else 0.5 * (mode(u_s, m + 9 * k) + w[k])
                    put(dst, m + 9 * k, old + term)
                spare(at + (m + 1) / 27.0 / (2.0 * SUBSTEPS))
            for a in range(3):
                w = [[mode(src, 9 * a + 3 * b + c) for c in range(3)] for b in range(3)]
                acc = [list(terms(w[b], 2, stage)) for b in range(3)]
                spare(at + (9 + 6 * a + 3) / 27.0 / (2.0 * SUBSTEPS))
                for c in range(3):
                    for b, term in enumerate(terms([w[b][c] for b in range(3)], 1, stage)):
                        acc[b][c] = acc[b][c] + term
                for b in range(3):
                    for c in range(3):
                        m = 9 * a + 3 * b + c
                        put(dst, m, mode(dst, m) + acc[b][c])
                spare(at + (9 + 6 * a + 6) / 27.0 / (2.0 * SUBSTEPS))
    spare(1.0)


def main_kernel(
    g_ref, in_ref, out_ref, in_s, outer_s, t_s, u_s, v_s, mid_s, face_s, uf_s, g3_s, x_s, a_s, b_s, j_s, p_s, g_s, size_s
):
    corners = [(n, kz, (n // 9) * 64 + ((n // 3) % 3) * 16 + (n % 3) * 4 + kz) for n in range(27) for kz in range(3)]
    in_s[0:8, :] = jnp.zeros((8, 128), jnp.float32)
    chunk = lax.div(g_ref[0], NZ)
    lane, row = iota((IN_ROWS, 128), 1), iota((IN_ROWS, 128), 0) % 20
    high = lane - 64
    layer = jnp.where(lane < 64, 4 * chunk - 8 + row, (12 * chunk - 3 + row + 384) // 3 - 128)
    upper = jnp.where(high < 54, (high >> 1) % 3, jnp.where(high < 56, 1, 0)) == 1
    layer = jnp.where((row == 19) & (lane >= 64), jnp.where(upper, 4 * chunk + 12, 4 * chunk - 9), layer)
    beyond = jnp.abs(2 * layer - 127) > 128
    for n in range(NXY):
        other = (2 * FAR_SENDER[n // 8] + (n // 4) % 2) * 4 + n % 4
        own, far = in_ref[IN_ROWS * n : IN_ROWS * n + IN_ROWS, :], in_ref[IN_ROWS * other : IN_ROWS * other + IN_ROWS, :]
        in_s[8 + IN_ROWS * n : 8 + IN_ROWS * n + IN_ROWS, :] = jnp.where(beyond, far, own)
    in_s[8 + NXY * IN_ROWS : 16 + NXY * IN_ROWS, :] = jnp.zeros((8, 128), jnp.float32)
    outer = lanes(in_s[pl.ds(8 + 19, 2 * NXY, stride=20), :], 64)
    lane = iota((2 * NXY, 128), 1)
    trace = jnp.where(lane < 54, (lane >> 1) % 3, 1) == 0
    speed = jnp.abs(2 * lane - 117) < 2
    outer_s[0:64, :] = jnp.where(trace, outer, jnp.where(speed, outer, 0.0))
    outer_s[64:128, :] = jnp.where(trace, lanes(outer, 2), jnp.where(speed, lanes(outer, -4), 0.0))
    row = iota((8, 128), 0)
    for t in range(3):
        for j in range(4):
            stacked = []
            for i in range(8):
                for a in range(2):
                    n = 2 * (4 * i + j) + a
                    block = in_s[pl.ds(8 + 20 * n + t - 1, 8, stride=3), :]
                    if t == 0:
                        block = jnp.where(row == 0, outer_s[n : n + 1, :], block)
                        block = jnp.where(row == 7, outer_s[64 + n : 65 + n, :], block)
                    stacked.append(block)
            t_s[...] = jnp.concatenate(stacked, axis=0).T
            for b in range(2):
                y = 2 * j + b
                u_s[pl.ds(8 * t + y, 27, stride=24), :] = t_s[pl.ds(b, 27, stride=2), :]
                v_s[pl.ds(8 * t + y, 3, stride=24), :] = t_s[pl.ds(54 + b, 3, stride=2), :]
                nodes = t_s[pl.ds(64 + b, 27, stride=2), :]
                if t == 0:
                    nodes = lanes(nodes, 1)
                g3_s[pl.ds(216 * ((t + 2) % 3) + y, 27, stride=8), :] = nodes
    lane = iota((8, 128), 1)
    fastest = jnp.max(in_ref[pl.ds(0, NXY, stride=IN_ROWS), :], axis=0, keepdims=True)
    fastest = jnp.where(iota((1, 128), 1) < SUM_LANE, 0.0, fastest)
    fastest = jnp.broadcast_to(jnp.max(fastest, axis=1, keepdims=True), (8, 128))
    for n, kz, at in corners:
        x_s[at] = g3_s[216 * kz + 8 * n : 216 * kz + 8 * n + 8, :]
    corner_fill(x_s)
    pieces = [piece for c in range(3) for piece in slope_pieces(x_s, j_s, a_s, b_s, c)]
    remap(u_s, v_s, mid_s, face_s, courant / jnp.maximum(fastest, 0.25), pieces)

    layer = lane & 7
    for m in range(27):
        u0, u1, u2 = (u_s[24 * m + 8 * t : 24 * m + 8 * t + 8, :] for t in range(3))
        value = jnp.where(layer == 3, u2, u0)
        value = jnp.where(layer < 2, lanes(jnp.where(layer == 2, u2, u0), 2), value)
        value = jnp.where(layer == 2, lanes(u1, 1), value)
        uf_s[8 * m : 8 * m + 8, :] = jnp.where(layer == 5, lanes(u1, -1), value)
    sample_sizes(uf_s, size_s, a_s)
    for m in range(27):
        uf_s[8 * m : 8 * m + 8, :] = (1.0 / SCALES[m]) * uf_s[8 * m : 8 * m + 8, :]
    energy = stress(j_s, size_s, g_s, p_s)
    points_to_corners(p_s, x_s, a_s, b_s)
    corner_fold(x_s)
    square = jnp.zeros((8, 128), jnp.float32)
    for n, kz, at in corners:
        grad = x_s[at]
        g3_s[216 * kz + 8 * n : 216 * kz + 8 * n + 8, :] = grad
        square = square + grad * grad
    own = jnp.abs(2 * layer - 5) < 4

    def own_sum(x):
        return jnp.sum(jnp.where(own, x, 0.0), axis=(0, 1), keepdims=True)

    square = own_sum(square)
    length = jnp.sqrt(1.0 + square * (1.0 / (512.0 * 81.0)))
    shorter = jnp.broadcast_to(1.0 / length, (8, 128))
    for n, kz, at in corners:
        x_s[at] = x_s[at] * shorter
    corner_fill(x_s)

    def pack_back(p, j):
        for b in range(2):
            y = 2 * j + b
            first = uf_s[pl.ds(y, 27, stride=8), :] if p == 0 else g3_s[pl.ds(216 + y, 27, stride=8), :]
            t_s[pl.ds(b, 27, stride=2), :] = first
            t_s[pl.ds(64 + b, 27, stride=2), :] = g3_s[pl.ds(432 * p + y, 27, stride=8), :]
        back = t_s[...].T
        for i in range(8):
            for a in range(2):
                to = (4 * i + j) * OUT_ROWS + 8 * p + 4 * a
                at = (2 * i + a) * 8 + 1
                out_ref[to : to + 4, :] = back[at : at + 4, :]

    pieces = [piece for c in range(3) for piece in slope_pieces(x_s, p_s, a_s, b_s, c)]
    for n, piece in enumerate(pieces):
        piece()
        if n % 60 == 30:
            pack_back(1, n // 60)
    e2, e3, e4 = trial_terms(j_s, size_s, g_s, p_s)
    t_s[...] = jnp.zeros((128, 128), jnp.float32)
    length = jnp.broadcast_to(length, (8, 128))
    t_s[SUM_LANE:128, :] = length
    for n, total in enumerate((own_sum(energy), square, own_sum(e2), own_sum(e3), own_sum(e4))):
        t_s[SUM_LANE + n : SUM_LANE + 1 + n, :] = jnp.where(layer[0:1] == 1, total, length[0:1])
    for j in range(4):
        pack_back(0, j)


def unpack_kernel(in_ref, u_ref, g_ref, sums_ref, u_s, g_s):
    def part(p, a, layer):
        return in_ref[pl.ds(8 * p + 4 * a + layer, NXY, stride=OUT_ROWS), :]

    low = iota((NXY, 128), 1) < 64
    for layer in range(4):
        for a in range(2):
            u_s[pl.ds(128 * a + layer, NXY, stride=4), :] = part(0, a, layer)
        for kz in range(3):
            first, second = part((kz + 1) // 2, 0, layer), part((kz + 1) // 2, 1, layer)
            if kz == 1:
                both = jnp.where(low, first, lanes(second, 64))
            else:
                both = jnp.where(low, lanes(first, 64), second)
            g_s[pl.ds(3 * layer + kz, NXY, stride=12), :] = both
    lane = iota((NXY, 128), 1)
    length = jnp.where(lane < SUM_LANE, 1.0, part(0, 0, 1))
    longest = jnp.max(length, axis=0, keepdims=True)
    ratio = length / longest
    ratio2 = ratio * ratio
    power = jnp.where(lane < SUM_LANE + 3, ratio2, jnp.where(lane < SUM_LANE + 4, ratio2 * ratio, ratio2 * ratio2))
    power = jnp.where(lane < SUM_LANE + 2, 1.0, power)
    total = jnp.sum(part(0, 0, 0) * power, axis=0, keepdims=True)
    total = jnp.where(lane[0:1] < SUM_LANE + 5, total, longest)
    sums_ref[...] = jnp.broadcast_to(total[None], (NZ, 1, 128))
    for a in range(2):
        back = u_s[128 * a : 128 * a + 128, :].T
        for m in range(27):
            u_ref[m, a] = back[2 * m : 2 * m + 2, :]
    for n in range(3):
        back = g_s[128 * n : 128 * n + 128, :].T
        for a in range(2):
            for q in range(27):
                c, kx, ky = q // 9, (q // 3) % 3, q % 3
                for b in range(2):
                    at = 64 * a + 2 * q + b
                    g_ref[c, 3 * a + kx, ky + 3 * b : ky + 3 * b + 1, 128 * n : 128 * n + 128] = back[at : at + 1, :]


def checks_kernel(sums_ref, out_ref):
    sums = jnp.concatenate([sums_ref[n] for n in range(NZ)], axis=0)
    lane = iota((NZ, 128), 1)
    e0, square, e2, e3, e4, length = (
        jnp.sum(jnp.where(lane == SUM_LANE + n, sums, 0.0), axis=1, keepdims=True) for n in range(6)
    )
    e0 = jnp.sum(e0, axis=0, keepdims=True)
    square = jnp.sum(square, axis=0, keepdims=True)
    elements = float(512 * NXY * NZ)
    entries = 81.0 * elements
    step = trial_step / jnp.sqrt(1.0 + square / entries)
    x = step * length
    trial = e0 - step * square + jnp.sum(x * x * (e2 + x * (e3 + x * e4)), axis=0, keepdims=True)
    for n, value in enumerate((e0 / elements, square / entries, trial / elements)):
        out_ref[n] = value[0, 0]


def shape(*dims):
    return jax.ShapeDtypeStruct(dims, jnp.float32)


def on_chip(*dims):
    return pltpu.VMEM(dims, jnp.float32)


def keep(x):
    return pltpu.with_memory_space_constraint(x, pltpu.VMEM)


def vmem(*dims):
    return pltpu.VMEM(dims, jnp.float32)


MAIN_SCRATCH = [
    vmem(16 + NXY * IN_ROWS, 128),
    vmem(128, 128),
    vmem(128, 128),
    vmem(27 * 24, 128),
    vmem(3 * 24, 128),
    vmem(27 * 24, 128),
    vmem(24 * 24, 128),
    vmem(27 * 8, 128),
    vmem(81 * 8, 128),
    vmem(192, 8, 128),
    vmem(128, 8, 128),
    vmem(192, 8, 128),
    vmem(576, 8, 128),
    vmem(576, 8, 128),
    vmem(384, 8, 128),
    vmem(64, 8, 128),
]
SMEM = pl.BlockSpec(memory_space=pltpu.SMEM)
VMEM = pl.BlockSpec(memory_space=pltpu.VMEM)


def near_groups(partner):
    groups = []
    for z in range(4):
        for core in range(2):
            for x in range(4):
                group = []
                for y in range(4):
                    for half in range(2):
                        at = z if half == 0 else partner[z]
                        group.append((((at * 2 + core) * 4 + x) * 4 + y) * 2 + half)
                groups.append(group)
    return groups


def on_device(displacement, size_field_modes, velocity):
    place = (lax.axis_index(XY) * NZ + lax.axis_index(GZ)).reshape(1).astype(jnp.int32)
    tuv, tx, halo = pl.pallas_call(
        transpose_kernel,
        out_shape=(on_chip(128, 128), on_chip(384, 128), on_chip(NZ, HALO_ROWS, 128)),
        in_specs=[SMEM, VMEM, VMEM, VMEM],
        out_specs=(VMEM, VMEM, VMEM),
        scratch_shapes=[vmem(128, 128), vmem(128, 384)],
        name="transpose",
    )(place, size_field_modes, velocity, displacement)
    halo = lax.all_to_all(halo, XY + GZ, 0, 0, axis_index_groups=near_groups(FAR_SENDER))
    packed = pl.pallas_call(
        pack_kernel,
        out_shape=on_chip(NXY * IN_ROWS, 128),
        in_specs=[SMEM, VMEM, VMEM, VMEM],
        out_specs=VMEM,
        scratch_shapes=[
            vmem(160, 128),
            vmem(408, 128),
            vmem(160, 128),
            vmem(408, 128),
            vmem(160, 128),
            vmem(160, 128),
        ],
        name="pack",
    )(place, keep(tuv), keep(tx), keep(halo))
    spread = lax.all_to_all(packed.reshape(NXY, IN_ROWS, 128), XY, 0, 0)
    result = pl.pallas_call(
        main_kernel,
        out_shape=on_chip(NXY * OUT_ROWS, 128),
        in_specs=[SMEM, VMEM],
        out_specs=VMEM,
        scratch_shapes=MAIN_SCRATCH,
        name="remap_and_gradient",
    )(place, keep(spread.reshape(NXY * IN_ROWS, 128)))
    result = lax.all_to_all(result.reshape(NXY, OUT_ROWS, 128), XY, 0, 0)
    advected, gradient, sums = pl.pallas_call(
        unpack_kernel,
        out_shape=(shape(27, 2, 2, 128), shape(3, 6, 6, 384), on_chip(NZ, 1, 128)),
        in_specs=[VMEM],
        out_specs=(VMEM, VMEM, VMEM),
        scratch_shapes=[vmem(256, 128), vmem(384, 128)],
        name="unpack",
    )(keep(result.reshape(NXY * OUT_ROWS, 128)))
    sums = lax.all_to_all(sums, XY + GZ, 0, 0, axis_index_groups=near_groups((3, 2, 1, 0)))
    checks = pl.pallas_call(
        checks_kernel, out_shape=shape(3), in_specs=[VMEM], out_specs=SMEM, name="checks"
    )(keep(sums))
    return advected, gradient, checks


def solution(mesh):
    finer = Mesh(
        mesh.devices.reshape(4, 2, mesh.shape["gy"], 4, 2), ("gx_0", "gx_1", "gy", "gz_0", "gz_1")
    )
    return jax.shard_map(
        on_device,
        mesh=finer,
        in_specs=(P(None, GX, "gy", GZ), P(None, GX, "gy", GZ), P(None, GX, "gy", GZ)),
        out_specs=(P(None, GX, "gy", GZ), P(None, GX, "gy", GZ), P()),
        check_vma=False,
    )
```
